32 devices in a mesh: dp: 2 (over x), tp: 4 (over z), ep: 4 (over y, core).
Axes of the slice: x: 2, y: 2, z: 4, core: 2. Of those that a mesh axis runs over, the one named last changes fastest.
Arguments:
- x: bfloat16 [256, 2048], P(('dp', 'tp', 'ep')), parts along dimension 0
- kv0: bfloat16 [256, 256, 576], P(('dp', 'tp', 'ep')), parts along dimension 0
- kv1: bfloat16 [256, 256, 576], P(('dp', 'tp', 'ep')), parts along dimension 0
- lens: int32 [256], P(('dp', 'tp', 'ep')), parts along dimension 0
- ids: int32 [256, 6], P(('dp', 'tp', 'ep')), parts along dimension 0
- wts: float32 [256, 6], P(('dp', 'tp', 'ep')), parts along dimension 0
- wq: bfloat16 [2, 2048, 3072], replicated
- wuk: bfloat16 [2, 16, 128, 512], replicated
- wuv: bfloat16 [2, 16, 512, 128], replicated
- wo: bfloat16 [2, 2048, 2048], replicated
- w_in: bfloat16 [2, 2, 2048, 11264], P(None, None, None, 'tp')
- w_out: bfloat16 [2, 11264, 2048], P(None, 'tp')
- e_in: bfloat16 [64, 2048, 2816], P(('tp', 'ep'))
- e_out: bfloat16 [64, 1408, 2048], P(('tp', 'ep'))
Outputs:
- output: bfloat16 [256, 2048], P(('dp', 'tp', 'ep')), parts along dimension 0
There are 2 independent parts. The reference program is written for one: setup_inputs(seed, part) draws one part's arguments, and reference() takes and returns one part's arrays. A program takes and returns all parts, laid end to end along the dimension named above; an argument that names none is the same for every part.
All inputs are finite; a program needn't handle non-finite values.
Results may differ from the reference program's by a relative error of at most 0.0157094.
Values are sent between devices in bfloat16 or wider.
A program may use at most 1 GiB of HBM per device.

```python
import jax
import jax.numpy as jnp
from jax import lax

TOKENS = 8
LKV = 256
H = 2048
EXPERTS = 64
ZERO = 0
TOP = 6
EFF = 1408
HEADS = 16
LAT = 512
ROPE = 64
NOPE = 128
VHEAD = 128
DFF = 11264
TP = 4
EP = 4

NDEV = TP * EP
T = NDEV * TOKENS
EL = EXPERTS // NDEV
SCALE = (NOPE + ROPE) ** -0.5


def normal_bf16(k, shape, scale):
    return (jax.random.normal(k, shape, jnp.float32) * scale).astype(jnp.bfloat16)


def cache_draw(k):
    k1, k2 = jax.random.split(k)
    seg = jax.random.normal(k1, (T, 8, LAT + ROPE), jnp.float32)
    c = seg[:, (jnp.arange(LKV) * 8) // LKV, :] + 0.5 * jax.random.normal(k2, (T, LKV, LAT + ROPE), jnp.float32)
    return c.astype(jnp.bfloat16)


def routing(k):
    ks, kq, kh, kz, ki = jax.random.split(k, 5)
    shift = jax.random.randint(ks, (NDEV, 1), 0, NDEV)
    r = ((jnp.arange(TOKENS)[None, :] * NDEV) // TOKENS + shift) % NDEV
    j = jnp.arange(TOP)[None, :]
    dst = (r.reshape(T, 1) + j) % NDEV
    hot = jax.random.uniform(kh, (T, NDEV)) < 0.6
    qt = jnp.where(hot, 0, jax.random.randint(kq, (T, NDEV), 0, EL))
    loc = (jnp.take_along_axis(qt, dst, axis=1) + j // NDEV) % EL
    zero_den = 10 * (EXPERTS + ZERO) * max(NDEV - 1, 1)
    z = jax.random.randint(kz, (T, TOP), 0, zero_den) < 18 * ZERO * dst
    zid = EXPERTS + jax.random.randint(ki, (T, TOP), 0, max(ZERO, 1))
    return jnp.where(z, zid, dst * EL + loc).astype(jnp.int32), z


def setup_inputs(seed: int = 0, part: int = 0) -> dict:
    kp = jax.random.split(jax.random.fold_in(jax.random.key(seed), part), 6)
    ks = jax.random.split(jax.random.key(seed + 1), 8)
    kd = jax.random.split(jax.random.fold_in(kp[3], 7), 4)
    x = jax.random.normal(kp[0], (T, H), jnp.float32).astype(jnp.bfloat16)
    kv0 = cache_draw(kp[1])
    kv1 = cache_draw(kp[2])
    short = jax.random.uniform(kd[0], (T,)) < 0.5
    ls = jax.random.randint(kd[1], (T,), 1, max(LKV // 16, 2))
    ll = jax.random.randint(kd[2], (T,), LKV // 2, LKV + 1)
    lens = jnp.where(short, ls, ll).astype(jnp.int32)
    ids, z = routing(kd[3])
    kw1, kw2 = jax.random.split(kp[5])
    wf = jax.random.uniform(kw1, (T, TOP), jnp.float32, 0.5, 1.5) * (1.5 / TOP ** 0.5)
    wz = jax.random.uniform(kw2, (T, TOP), jnp.float32, 0.05, 0.3) * (1.0 / TOP ** 0.5)
    wts = jnp.where(z, wz, wf).astype(jnp.float32)
    wq = normal_bf16(ks[0], (2, H, HEADS * (NOPE + ROPE)), H ** -0.5)
    wuk = normal_bf16(ks[1], (2, HEADS, NOPE, LAT), NOPE ** -0.5)
    wuv = normal_bf16(ks[2], (2, HEADS, LAT, VHEAD), LAT ** -0.5)
    wo = normal_bf16(ks[3], (2, HEADS * VHEAD, H), (HEADS * VHEAD) ** -0.5)
    w_in = normal_bf16(ks[4], (2, 2, H, DFF), H ** -0.5)
    w_out = normal_bf16(ks[5], (2, DFF, H), DFF ** -0.5)
    e_in = lax.map(lambda kk: normal_bf16(kk, (H, 2 * EFF), H ** -0.5), jax.random.split(ks[6], EXPERTS))
    e_out = lax.map(lambda kk: normal_bf16(kk, (EFF, H), EFF ** -0.5), jax.random.split(ks[7], EXPERTS))
    return dict(x=x, kv0=kv0, kv1=kv1, lens=lens, ids=ids, wts=wts, wq=wq, wuk=wuk, wuv=wuv, wo=wo,
                w_in=w_in, w_out=w_out, e_in=e_in, e_out=e_out)


def rms(v):
    vf = v.astype(jnp.float32)
    return (vf * lax.rsqrt(jnp.mean(vf * vf, axis=-1, keepdims=True) + 1e-6)).astype(jnp.bfloat16)


def rope_q(q, pos):
    half = ROPE // 2
    freq = 10000.0 ** (-2.0 * jnp.arange(half, dtype=jnp.float32) / ROPE)
    ang = pos.astype(jnp.float32)[:, None, None] * freq
    cs = jnp.cos(ang)
    sn = jnp.sin(ang)
    q1 = q[..., :half]
    q2 = q[..., half:]
    return jnp.concatenate([q1 * cs - q2 * sn, q2 * cs + q1 * sn], axis=-1)


def mla(a, cache, lens, wq, wuk, wuv, wo):
    t = a.shape[0]
    q = jnp.dot(a, wq, preferred_element_type=jnp.float32).reshape(t, HEADS, NOPE + ROPE)
    qn = q[..., :NOPE].astype(jnp.bfloat16)
    qr = rope_q(q[..., NOPE:], lens).astype(jnp.bfloat16)
    ql = jnp.einsum('thn,hnl->thl', qn.astype(jnp.float32), wuk.astype(jnp.float32)).astype(jnp.bfloat16)
    qc = jnp.concatenate([ql, qr], axis=-1)

    def one(xs):
        qt, ct, nt = xs
        s = jnp.einsum('hd,ld->hl', qt.astype(jnp.float32), ct.astype(jnp.float32)) * SCALE
        s = jnp.where(jnp.arange(LKV)[None, :] < nt, s, -1e30)
        p = jax.nn.softmax(s, axis=-1).astype(jnp.bfloat16)
        return jnp.einsum('hl,ld->hd', p.astype(jnp.float32), ct[:, :LAT].astype(jnp.float32)).astype(jnp.bfloat16)

    ol = lax.map(one, (qc, cache, lens))
    o = jnp.einsum('thl,hlv->thv', ol.astype(jnp.float32), wuv.astype(jnp.float32)).astype(jnp.bfloat16)
    return jnp.dot(o.reshape(t, HEADS * VHEAD), wo, preferred_element_type=jnp.float32)


def ffn(a, wi, wd):
    g = jnp.dot(a, wi[0], preferred_element_type=jnp.float32)
    up = jnp.dot(a, wi[1], preferred_element_type=jnp.float32)
    act = (jax.nn.silu(g) * up).astype(jnp.bfloat16)
    w = DFF // TP
    acc = jnp.zeros((a.shape[0], H), jnp.float32)
    for s in range(TP):
        pr = jnp.dot(act[:, s * w:(s + 1) * w], wd[s * w:(s + 1) * w], preferred_element_type=jnp.float32)
        acc = acc + pr.astype(jnp.bfloat16).astype(jnp.float32)
    return acc


def moe(u, ids, wts, e_in, e_out):
    t = u.shape[0]
    fid = ids.reshape(-1)
    fw = wts.reshape(-1)
    ftok = jnp.arange(t * TOP) // TOP
    isff = fid < EXPERTS
    key = jnp.where(isff, fid, EXPERTS)
    order = jnp.argsort(key)
    cnt = jnp.zeros((EXPERTS,), jnp.int32).at[key].add(1, mode='drop')
    off = jnp.cumsum(cnt) - cnt
    zw = jnp.sum(jnp.where(isff, 0.0, fw).reshape(t, TOP), axis=1)
    acc0 = zw[:, None] * u.astype(jnp.float32)
    rows = jnp.arange(64)

    def expert(acc, xs):
        wi, wd, o, n = xs

        def cond(c):
            return c[0] < n

        def body(c):
            s, a = c
            pos = s + rows
            ok = pos < n
            sl = order[jnp.minimum(o + pos, t * TOP - 1)]
            tk = ftok[sl]
            gu = jnp.dot(u[tk], wi, preferred_element_type=jnp.float32)
            act = (jax.nn.silu(gu[:, :EFF]) * gu[:, EFF:]).astype(jnp.bfloat16)
            out = jnp.dot(act, wd, preferred_element_type=jnp.float32).astype(jnp.bfloat16)
            contrib = jnp.where(ok, fw[sl], 0.0)[:, None] * out.astype(jnp.float32)
            return s + 64, a.at[tk].add(contrib)

        s0 = jnp.zeros((), jnp.int32)
        return lax.while_loop(cond, body, (s0, acc))[1], None

    return lax.scan(expert, acc0, (e_in, e_out, off, cnt))[0]


def reference(x, kv0, kv1, lens, ids, wts, wq, wuk, wuv, wo, w_in, w_out, e_in, e_out):
    h0 = (x.astype(jnp.float32) + mla(rms(x), kv0, lens, wq[0], wuk[0], wuv[0], wo[0])).astype(jnp.bfloat16)
    u = rms(h0)
    m = moe(u, ids, wts, e_in, e_out)
    f0 = (h0.astype(jnp.float32) + ffn(u, w_in[0], w_out[0])).astype(jnp.bfloat16)
    h1 = (f0.astype(jnp.float32) + mla(rms(f0), kv1, lens, wq[1], wuk[1], wuv[1], wo[1])).astype(jnp.bfloat16)
    y = h1.astype(jnp.float32) + ffn(rms(h1), w_in[1], w_out[1]) + m
    return y.astype(jnp.bfloat16)
```

```python
import functools
import types

import jax
import jax.numpy as jnp
import numpy as np
from jax import lax
from jax.experimental import pallas as pl
from jax.experimental.pallas import tpu as pltpu
from jax.sharding import PartitionSpec as P

BATCH = ('dp', 'tp', 'ep')
GROUP = ('tp', 'ep')
MESH = pl.DeviceIdType.MESH
BF = jnp.bfloat16
F32 = jnp.float32
I32 = jnp.int32

B = 8
H = 2048
HEADS = 16
NOPE = 128
ROPE = 64
LAT = 512
VH = 128
L = 256
FH = 1408
TP = 4
N = 16
R = HEADS * B
M = 64
CB = 512
SCALE = (NOPE + ROPE) ** -0.5

ALONG = (1, 3, 2)


def scratch():
    dma = pltpu.SemaphoreType.DMA
    v = pltpu.VMEM
    return dict(
        mbuf=v((8, H, CB), BF), wukb=v((HEADS, NOPE, LAT), BF), wuvb=v((HEADS, LAT, VH), BF), kvb=v((B * L, LAT + ROPE), BF),
        gu5=v((2, 5, H, CB), BF), gu1=v((2, H, CB // 2), BF), wd=v((2, 4, FH, CB), BF),
        qs=v((B, HEADS * (NOPE + ROPE)), F32), qc=v((R, LAT + ROPE), BF), sc=v((R, L), F32), pb=v((R, B * L), BF),
        ol=v((R, LAT), F32), os=v((B, HEADS * VH), BF), res=v((B, H), F32), an=v((B, H), BF),
        h0=v((B, H), BF), f0=v((B, H), BF), h1=v((B, H), BF),
        cs=v((R, ROPE), F32), sn=v((R, ROPE), F32), lm=v((R, L), F32),
        uall=v((N, B, H), BF), vall=v((N // 2, B, H), BF), fa=v((M, H), BF), ea=v((M, H), BF), act=v((M, FH), BF),
        pm=v((4, M // 2, CB), F32), ps=v((2, 4, M // 2, CB), F32), pr=v((2, 4, M // 2, CB), F32),
        bs=v((2, TP, B, H), BF), br=v((2, TP, B, H), BF),
        idall=v((N, B, 128), I32), ptk=v((N * B, M), BF), el=v((M, 128), F32), gsel=v((2 * 6 * B, 128), BF),
        racc=v((M, H), F32), rs=v((N, B, H // 2), BF), rr=v((N, B, H // 2), BF), rk=v((N * B, H // 2), BF), mm=v((B, H), F32),
        s_m=dma((8,)), s_kv=dma((B,)), s_uk=dma((2,)), s_gu=dma((2, 6, 2)), s_wd=dma((2, 4)),
        us=dma((16,)), ur=dma((N,)), vs=dma((8,)), vr=dma((N // 2,)),
        pss=dma((2, 4)), psr=dma((2, 4)), bss=dma((2, TP)), bsr=dma((2, TP)),
        ids_s=dma((N,)), ids_r=dma((N,)), ret_s=dma((N,)), ret_r=dma((N,)),
    )


def rms(v):
    vf = v.astype(F32)
    return (vf * lax.rsqrt(jnp.mean(vf * vf, axis=-1, keepdims=True) + 1e-6)).astype(BF)


def dot(a, b):
    return jnp.dot(a, b, preferred_element_type=F32)


def kernel(names, x, lens, ids, wts, table, kv0, kv1, wq, wuk, wuv, wo, w_in, w_out, e_in, e_out, y, *scr):
    s = types.SimpleNamespace(**dict(zip(names, scr)))
    z = lax.axis_index('tp')
    e = lax.axis_index('ep')
    me = z * 4 + e
    c = lax.rem(e, 2)
    pe = e + 1 - 2 * c
    ye = lax.rem(e + 2, 4)
    ype = lax.rem(pe + 2, 4)
    kvs = (kv0, kv1)
    sends = []

    barrier = pltpu.get_barrier_semaphore()
    others = []
    for i in range(1, N):
        zz, ee = lax.rem(z + i // 4, 4), lax.rem(e + i % 4, 4)
        others.append((i, zz * 4 + ee, zz, ee))
    for i, g, zz, ee in others:
        pl.semaphore_signal(barrier, inc=1, device_id=(lax.axis_index('dp'), zz, ee), device_id_type=MESH)

    def cp(src, dst, sem):
        return pltpu.make_async_copy(src, dst, sem)

    def m_q(l, j):
        k = 2 * l + j
        return cp(wq.at[l, :, pl.ds(j * CB, CB)], s.mbuf.at[k], s.s_m.at[k])

    def m_o(l, j):
        k = lax.rem(2 * l + 6 + j, 8)
        return cp(wo.at[l, :, pl.ds(j * CB, CB)], s.mbuf.at[k], s.s_m.at[k])

    def c_kv(l, t):
        return cp(kvs[l].at[t], s.kvb.at[pl.ds(t * L, L)], s.s_kv.at[t])

    def c_uk(l):
        return cp(wuk.at[l], s.wukb, s.s_uk.at[0])

    def c_uv(l):
        return cp(wuv.at[l], s.wuvb, s.s_uk.at[1])

    def u_gu(what, i, k, j, w, half):
        o = pl.multiple_of(j * 256, 128)
        if what == 'ffn':
            src = w_in.at[i, half, :, pl.ds(pl.multiple_of(c * FH + o, 128), w)]
        else:
            src = e_in.at[i, :, pl.ds(pl.multiple_of(half * FH + o, 128), w)]
        dst = s.gu5.at[k, j, :, pl.ds(half * w, w)] if w == 256 else s.gu1.at[k, :, pl.ds(half * w, w)]
        return cp(src, dst, s.s_gu.at[k, j, half])

    def u_wd(what, i, k, j):
        cols = pl.ds(pl.multiple_of(j * CB, CB), CB)
        if what == 'ffn':
            src = w_out.at[i, pl.ds(pl.multiple_of(c * FH, 128), FH), cols]
        else:
            src = e_out.at[i, :, cols]
        return cp(src, s.wd.at[k, j], s.s_wd.at[k, j])

    def u_start(what, i, k):
        def gu(j, _):
            u_gu(what, i, k, j, 256, 0).start()
            u_gu(what, i, k, j, 256, 1).start()
            return 0

        lax.fori_loop(0, 5, gu, 0)
        u_gu(what, i, k, 5, 128, 0).start()
        u_gu(what, i, k, 5, 128, 1).start()

        def dn(j, _):
            u_wd(what, i, k, j).start()
            return 0

        lax.fori_loop(0, 4, dn, 0)

    def rc(src, dst, ss, rs, tp, ep):
        return pltpu.make_async_remote_copy(src_ref=src, dst_ref=dst, send_sem=ss, recv_sem=rs,
                                            device_id=(lax.axis_index('dp'), tp, ep), device_id_type=MESH)

    def send(*a):
        d = rc(*a)
        d.start()
        sends.append(d)

    for j in range(6):
        m_q(0, j).start()
    for t in range(B):
        c_kv(0, t).start()
    c_uk(0).start()
    c_uv(0).start()
    m_o(0, 0).start()
    m_o(0, 1).start()

    diag = lax.broadcasted_iota(I32, (B, B), 0) == lax.broadcasted_iota(I32, (B, B), 1)
    lrow = jnp.broadcast_to(lens[...].astype(F32).reshape(1, B), (B, B))
    lv = jnp.broadcast_to(jnp.sum(jnp.where(diag, lrow, 0.0), axis=1, keepdims=True), (B, L))
    at = jnp.where(lax.broadcasted_iota(I32, (B, L), 1).astype(F32) == lv - 1.0, 1.0, 0.0).astype(BF)
    tb = dot(at, table[...])
    tb = tb[:, :128] + tb[:, 128:256] + tb[:, 256:]
    s.cs[...] = jnp.concatenate([tb[:, :ROPE]] * HEADS, axis=0)
    s.sn[...] = jnp.concatenate([tb[:, ROPE:]] * HEADS, axis=0)
    rowt = lax.broadcasted_iota(I32, (R, L), 0) & (B - 1)
    s.lm[...] = jnp.concatenate([lv] * HEADS, axis=0)

    def q_steps(l, lo, hi):
        def step(j, _):
            m_q(l, j).wait()
            s.qs[:, pl.ds(pl.multiple_of(j * CB, CB), CB)] = dot(s.an[...], s.mbuf[2 * l + j])
            return 0

        lax.fori_loop(lo, hi, step, 0)

    def mla(l, after_two, after_q, after_uk, after_kv, after_uv):
        q_steps(l, 0, 2)
        after_two()
        q_steps(l, 2, 6)
        after_q()
        c_uk(l).wait()
        D = NOPE + ROPE
        rope = []
        for hp in range(HEADS // 2):
            pair = []
            for k in range(2):
                h = 2 * hp + k
                qn = s.qs[:, h * D:h * D + NOPE].astype(BF)
                pair.append(dot(qn, s.wukb[h]))
                rope.append(s.qs[:, h * D + NOPE:(h + 1) * D])
            s.qc[hp * 16:(hp + 1) * 16, :LAT] = jnp.concatenate(pair, axis=0).astype(BF)
        after_uk()
        r = jnp.concatenate(rope, axis=0)
        rot = jnp.concatenate([r[:, ROPE // 2:], r[:, :ROPE // 2]], axis=1)
        s.qc[:, LAT:] = (r * s.cs[...] + rot * s.sn[...]).astype(BF)
        for t in range(B):
            c_kv(l, t).wait()
            st = lax.dot_general(s.qc[...], s.kvb[t * L:(t + 1) * L, :], (((1,), (1,)), ((), ())), preferred_element_type=F32)
            if t == 0:
                s.sc[...] = st
            else:
                s.sc[...] = jnp.where(rowt == t, st, s.sc[...])
        sc = jnp.where(lax.broadcasted_iota(I32, (R, L), 1).astype(F32) < s.lm[...], s.sc[...] * SCALE, -1e30)
        ex = jnp.exp(sc - jnp.max(sc, axis=-1, keepdims=True))
        p = ex / jnp.sum(ex, axis=-1, keepdims=True)
        for t in range(B):
            s.pb[:, t * L:(t + 1) * L] = jnp.where(rowt == t, p, 0.0).astype(BF)
        s.ol[...] = dot(s.pb[...], s.kvb[:, :LAT])
        after_kv()
        c_uv(l).wait()
        for h in range(HEADS):
            o = dot(s.ol[h * B:(h + 1) * B, :].astype(BF), s.wuvb[h])
            s.os[:, h * VH:(h + 1) * VH] = o.astype(BF)
        after_uv()

        def step(j, _):
            m_o(l, j).wait()
            s.res[:, pl.ds(pl.multiple_of(j * CB, CB), CB)] = dot(s.os[...], s.mbuf[lax.rem(2 * l + 6 + j, 8)])
            return 0

        lax.fori_loop(0, 4, step, 0)

    def unit(what, i, k, lhs, down):
        def silu(g, u):
            return (g / (1.0 + jnp.exp(-g)) * u).astype(BF)

        def gu(j, _):
            u_gu(what, i, k, j, 256, 0).wait()
            u_gu(what, i, k, j, 256, 1).wait()
            r = dot(lhs[...], s.gu5[k, j])
            s.act[:, pl.ds(pl.multiple_of(j * 256, 256), 256)] = silu(r[:, :256], r[:, 256:])
            return 0

        lax.fori_loop(0, 5, gu, 0)
        u_gu(what, i, k, 5, 128, 0).wait()
        u_gu(what, i, k, 5, 128, 1).wait()
        r = dot(lhs[...], s.gu1[k])
        s.act[:, 1280:] = silu(r[:, :128], r[:, 128:])

        def dn(j, _):
            u_wd(what, i, k, j).wait()
            down(j, dot(s.act[...], s.wd[k, j]))
            return 0

        lax.fori_loop(0, 4, dn, 0)

    def gather(buf, ss, rs, at, on_y):
        own = at(z, e)
        for k in ALONG:
            send(buf.at[own], buf.at[own], ss.at[k - 1], rs.at[own], lax.rem(z + k, TP), e)
        send(buf.at[own], buf.at[own], ss.at[3], rs.at[own], z, pe)
        if on_y:
            send(buf.at[own], buf.at[own], ss.at[8], rs.at[own], z, ye)
        for k in ALONG:
            g = at(lax.rem(z + k, TP), e)
            rc(buf.at[g], buf.at[g], ss.at[3 + k], rs.at[g], z, pe).wait_recv()
            send(buf.at[g], buf.at[g], ss.at[3 + k], rs.at[g], z, pe)
            if on_y:
                send(buf.at[g], buf.at[g], ss.at[8 + k], rs.at[g], z, ye)
        for zz in range(TP):
            g = at(zz, pe)
            rc(buf.at[g], buf.at[g], ss.at[0], rs.at[g], z, pe).wait_recv()

    def stack(buf, at):
        for i, ee in enumerate((e, pe)):
            for q in range(2):
                s.fa[i * 32 + q * 16:i * 32 + q * 16 + 16, :] = jnp.concatenate([buf[at(2 * q, ee)], buf[at(2 * q + 1, ee)]], axis=0)

    def ffn(l, k):
        def down(j, r):
            s.pm[j] = r[:M // 2]
            s.ps[l, j] = r[M // 2:]
            rc(s.ps.at[l, j], s.pr.at[l, j], s.pss.at[l, j], s.psr.at[l, j], z, pe).start()

        unit('ffn', l, k, s.fa, down)

    def ffn_send(l):
        for j in range(4):
            rc(s.ps.at[l, j], s.pr.at[l, j], s.pss.at[l, j], s.psr.at[l, j], z, pe).wait()
            tot = s.pm[j] + s.pr[l, j]
            for q in range(TP):
                s.bs[l, q, :, j * CB:(j + 1) * CB] = tot[q * B:(q + 1) * B].astype(BF)
        for k in ALONG:
            zz = lax.rem(z + k, TP)
            send(s.bs.at[l, zz], s.br.at[l, z], s.bss.at[l, k], s.bsr.at[l, z], zz, e)
        s.br[l, z] = s.bs[l, z]

    def ffn_recv(l):
        for k in ALONG:
            zz = lax.rem(z + k, TP)
            rc(s.bs.at[l, zz], s.br.at[l, zz], s.bss.at[l, k], s.bsr.at[l, zz], zz, e).wait_recv()
        acc = s.br[l, 0].astype(F32)
        for q in range(1, TP):
            acc = acc + s.br[l, q].astype(F32)
        return acc

    def at16(zz, ee):
        return zz * 4 + ee

    def at8(zz, ee):
        return zz * 2 + lax.rem(ee, 2)

    def send_ids():
        s.idall[me] = jnp.full((B, 128), -1, I32)
        s.idall[me, :, 0:6] = ids[...]
        pl.semaphore_wait(barrier, N - 1)
        for i, g, zz, ee in others:
            send(s.idall.at[me], s.idall.at[me], s.ids_s.at[i], s.ids_r.at[me], zz, ee)

    def slots_here():
        lane = lax.broadcasted_iota(I32, (B, 128), 1)
        mine = s.idall[me]
        dst = [jnp.broadcast_to(mine[:, j:j + 1], (B, 128)) >> 2 for j in range(6)]
        hot = [jnp.where(d == lane, 1.0, 0.0) for d in dst]
        cnt = functools.reduce(jnp.add, hot)
        row = lax.broadcasted_iota(I32, (B, 128), 0)
        run = jnp.zeros((B, 128), F32)
        for t in range(B - 1):
            run = run + jnp.where(row > t, jnp.broadcast_to(cnt[t:t + 1], (B, 128)), 0.0)
        left, right = [], []
        for j in range(6):
            pos = jnp.sum(hot[j] * run, axis=1, keepdims=True)
            run = run + hot[j]
            col = dst[j].astype(F32) * B + pos
            left.append(jnp.where(col == lane.astype(F32), 1.0, 0.0))
            right.append(jnp.where(col + 4.0 == lane.astype(F32), 1.0, 0.0))
        s.gsel[...] = jnp.concatenate(left + right, axis=0).astype(BF)

    def slots_there():
        for i, g, zz, ee in others:
            rc(s.idall.at[g], s.idall.at[g], s.ids_s.at[i], s.ids_r.at[g], z, pe).wait_recv()
        T = N * B
        idt = jnp.concatenate([s.idall[d] for d in range(N)], axis=0)
        lane = lax.broadcasted_iota(I32, (T, 128), 1)
        tok = lax.broadcasted_iota(I32, (T, 128), 0)
        col = [jnp.broadcast_to(idt[:, j:j + 1], (T, 128)) for j in range(6)]
        hit = [jnp.where((v >> 2) == me, 1.0, 0.0) for v in col]
        before = jnp.where((tok >> 3 == lane >> 3) & (lane < tok), 1.0, 0.0)
        run = dot(before.astype(BF), functools.reduce(jnp.add, hit).astype(BF)) + ((tok >> 3) * 4).astype(F32)
        pt = jnp.zeros((T, 128), F32)
        ex = jnp.zeros((T, 128), F32)
        for j in range(6):
            at = jnp.where(run == lane.astype(F32), hit[j], 0.0)
            pt = pt + at
            ex = ex + at * (col[j] & 3).astype(F32)
            run = run + hit[j]
        s.ptk[...] = pt[:, :M].astype(BF)
        s.el[...] = lax.dot_general(ex[:, :M].astype(BF), jnp.ones((T, 128), BF), (((0,), (0,)), ((), ())),
                                    preferred_element_type=F32)

    def expert(i, k):
        def down(j, r):
            cols = pl.ds(pl.multiple_of(j * CB, CB), CB)
            r = r.astype(BF).astype(F32)
            if i == 0:
                s.racc[:, cols] = r
            else:
                keep = jnp.broadcast_to(s.el[:, 0:1], (M, CB)) == float(i)
                s.racc[:, cols] = jnp.where(keep, r, s.racc[:, cols])

        unit('moe', i, k, s.ea, down)

    def give_back():
        for d in range(N):
            a = s.racc[4 * d:4 * d + 4, :]
            s.rs[d] = jnp.concatenate([a[:, :H // 2], a[:, H // 2:]], axis=0).astype(BF)
        for i, g, zz, ee in others:
            send(s.rs.at[g], s.rr.at[me], s.ret_s.at[i], s.ret_r.at[me], zz, ee)
        s.rr[me] = s.rs[me]

    def take_back():
        for i, g, zz, ee in others:
            rc(s.rs.at[g], s.rr.at[g], s.ret_s.at[i], s.ret_r.at[g], z, pe).wait_recv()
        for d in range(N // 2):
            s.rk[d * 16:(d + 1) * 16, :] = jnp.concatenate([s.rr[2 * d], s.rr[2 * d + 1]], axis=0)
        got = dot(s.gsel[...], s.rk[...])
        for half in range(2):
            acc = None
            for j in range(6):
                o = (half * 6 + j) * B
                term = wts[:, j:j + 1] * got[o:o + B]
                acc = term if acc is None else acc + term
            s.mm[:, half * (H // 2):(half + 1) * (H // 2)] = acc

    nothing = lambda: None

    s.an[...] = rms(x[...])

    def two0():
        m_o(0, 2).start()
        m_o(0, 3).start()
        u_start('ffn', 0, 0)
        u_start('moe', 0, 1)
        send_ids()

    def q0():
        for j in range(4):
            m_q(1, j).start()

    def kv0_done():
        for t in range(B):
            c_kv(1, t).start()

    mla(0, two0, q0, lambda: c_uk(1).start(), kv0_done, lambda: c_uv(1).start())
    for j in (4, 5):
        m_q(1, j).start()
    for j in (0, 1):
        m_o(1, j).start()
    h0 = (x[...].astype(F32) + s.res[...]).astype(BF)
    s.h0[...] = h0
    s.uall[me] = rms(h0)
    slots_here()
    gather(s.uall, s.us, s.ur, at16, True)
    slots_there()
    stack(s.uall, at16)
    ffn(0, 0)
    u_start('moe', 1, 0)
    for zz in range(TP):
        g = at16(zz, ye)
        rc(s.uall.at[g], s.uall.at[g], s.us.at[12 + zz], s.ur.at[g], z, pe).wait_recv()
        send(s.uall.at[g], s.uall.at[g], s.us.at[12 + zz], s.ur.at[g], z, pe)
    ffn_send(0)
    for zz in range(TP):
        g = at16(zz, ype)
        rc(s.uall.at[g], s.uall.at[g], s.us.at[12 + zz], s.ur.at[g], z, pe).wait_recv()
    for half in range(2):
        cols = pl.ds(half * (H // 2), H // 2)
        for d in range(N // 2):
            s.rk[d * 16:(d + 1) * 16, :] = jnp.concatenate([s.uall[2 * d, :, cols], s.uall[2 * d + 1, :, cols]], axis=0)
        s.ea[:, cols] = lax.dot_general(s.ptk[...], s.rk[...], (((0,), (0,)), ((), ())),
                                        preferred_element_type=F32).astype(BF)
    expert(0, 1)
    u_start('moe', 2, 1)
    f0 = (s.h0[...].astype(F32) + ffn_recv(0)).astype(BF)
    s.f0[...] = f0
    s.an[...] = rms(f0)

    def q1():
        m_o(1, 2).start()
        m_o(1, 3).start()

    mla(1, nothing, q1, nothing, nothing, nothing)
    h1 = (s.f0[...].astype(F32) + s.res[...]).astype(BF)
    s.h1[...] = h1
    s.vall[at8(z, e)] = rms(h1)
    gather(s.vall, s.vs, s.vr, at8, False)
    stack(s.vall, at8)
    expert(1, 0)
    u_start('moe', 3, 0)
    expert(2, 1)
    u_start('ffn', 1, 1)
    expert(3, 0)
    give_back()
    ffn(1, 1)
    ffn_send(1)
    take_back()
    y[...] = (s.h1[...].astype(F32) + ffn_recv(1) + s.mm[...]).astype(BF)
    for d in sends:
        d.wait_send()


def rope_table():
    half = ROPE // 2
    f = np.float32(10000.0) ** (np.float32(-2.0) * np.arange(half, dtype=np.float32) / np.float32(ROPE))
    ang = np.arange(1, L + 1, dtype=np.float32)[:, None] * f.astype(np.float32)
    cs, sn = np.cos(ang.astype(np.float64)), np.sin(ang.astype(np.float64))
    left = np.concatenate([cs, cs, -sn, sn], axis=1).astype(np.float32)
    parts = []
    for _ in range(3):
        part = left.astype(jnp.bfloat16)
        parts.append(part)
        left = left - part.astype(np.float32)
    return jnp.asarray(np.concatenate(parts, axis=1))


def layer(x, kv0, kv1, lens, ids, wts, wq, wuk, wuv, wo, w_in, w_out, e_in, e_out):
    table = rope_table()
    sc = scratch()
    vm = pl.BlockSpec(memory_space=pltpu.VMEM)
    hbm = pl.BlockSpec(memory_space=pl.ANY)
    return pl.pallas_call(
        functools.partial(kernel, tuple(sc)),
        out_shape=jax.ShapeDtypeStruct((B, H), BF),
        in_specs=[vm] * 5 + [hbm] * 10,
        out_specs=vm,
        scratch_shapes=list(sc.values()),
        compiler_params=pltpu.CompilerParams(collective_id=0, has_side_effects=True, vmem_limit_bytes=67043328),
    )(x, lens, ids, wts, table, kv0, kv1, wq, wuk, wuv, wo, w_in, w_out, e_in, e_out)


def solution(mesh):
    in_specs = (P(BATCH, None), P(BATCH, None, None), P(BATCH, None, None), P(BATCH), P(BATCH, None), P(BATCH, None),
                P(), P(), P(), P(), P(None, None, None, 'tp'), P(None, 'tp', None), P(GROUP, None, None), P(GROUP, None, None))
    return jax.shard_map(layer, mesh=mesh, in_specs=in_specs, out_specs=P(BATCH, None), check_vma=False)
```

```python
import functools
import types

import jax
import jax.numpy as jnp
import numpy as np
from jax import lax
from jax.experimental import pallas as pl
from jax.experimental.pallas import tpu as pltpu
from jax.sharding import PartitionSpec as P

BATCH = ('dp', 'tp', 'ep')
GROUP = ('tp', 'ep')
MESH = pl.DeviceIdType.MESH
BF = jnp.bfloat16
F32 = jnp.float32
I32 = jnp.int32

B = 8
H = 2048
HEADS = 16
NOPE = 128
ROPE = 64
LAT = 512
VH = 128
L = 256
FH = 1408
TP = 4
N = 16
R = HEADS * B
M = 64
CB = 512
SCALE = (NOPE + ROPE) ** -0.5

ALONG = (1, 3, 2)


def scratch():
    dma = pltpu.SemaphoreType.DMA
    v = pltpu.VMEM
    return dict(
        mbuf=v((8, H, CB), BF), wukb=v((HEADS, NOPE, LAT), BF), wuvb=v((HEADS, LAT, VH), BF), kvb=v((B, LAT + ROPE, L), BF),
        gu5=v((2, 5, H, CB), BF), gu1=v((2, H, CB // 2), BF), wd=v((2, 4, FH, CB), BF),
        qs=v((B, HEADS * (NOPE + ROPE)), F32), qc=v((R, LAT + ROPE), BF), sc=v((R, L), F32),
        ol=v((R, LAT), F32), os=v((B, HEADS * VH), BF), res=v((B, H), F32), an=v((B, H), BF),
        h0=v((B, H), BF), f0=v((B, H), BF), h1=v((B, H), BF),
        cs=v((R, ROPE), F32), sn=v((R, ROPE), F32), lm=v((R, L), F32),
        uall=v((N, B, H), BF), vall=v((N // 2, B, H), BF), fa=v((M, H), BF), ea=v((M, H), BF), act=v((M, FH), BF),
        pm=v((4, M // 2, CB), F32), ps=v((2, 4, M // 2, CB), F32), pr=v((2, 4, M // 2, CB), F32),
        bs=v((2, TP, B, H), BF), br=v((2, TP, B, H), BF),
        idall=v((N, B, 128), I32), ptk=v((N * B, M), BF), el=v((M, 128), F32), gsel=v((2 * 6 * B, 128), BF),
        racc=v((M, H), F32), rs=v((N, B, H // 2), BF), rr=v((N, B, H // 2), BF), rk=v((N * B, H // 2), BF), mm=v((B, H), F32),
        s_m=dma((8,)), s_kv=dma((B,)), s_uk=dma((2,)), s_gu=dma((2, 6, 2)), s_wd=dma((2, 4)),
        us=dma((16,)), ur=dma((N,)), vs=dma((8,)), vr=dma((N // 2,)),
        pss=dma((2, 4)), psr=dma((2, 4)), bss=dma((2, TP)), bsr=dma((2, TP)),
        ids_s=dma((N,)), ids_r=dma((N,)), ret_s=dma((N,)), ret_r=dma((N,)),
    )


def rms(v):
    vf = v.astype(F32)
    return (vf * lax.rsqrt(jnp.mean(vf * vf, axis=-1, keepdims=True) + 1e-6)).astype(BF)


def dot(a, b):
    return jnp.dot(a, b, preferred_element_type=F32)


def kernel(names, x, lens, ids, wts, table, kv0, kv1, wq, wuk, wuv, wo, w_in, w_out, e_in, e_out, y, *scr):
    s = types.SimpleNamespace(**dict(zip(names, scr)))
    z = lax.axis_index('tp')
    e = lax.axis_index('ep')
    me = z * 4 + e
    c = lax.rem(e, 2)
    pe = e + 1 - 2 * c
    ye = lax.rem(e + 2, 4)
    ype = lax.rem(pe + 2, 4)
    kvs = (kv0, kv1)
    sends = []

    barrier = pltpu.get_barrier_semaphore()
    others = []
    for i in range(1, N):
        zz, ee = lax.rem(z + i // 4, 4), lax.rem(e + i % 4, 4)
        others.append((i, zz * 4 + ee, zz, ee))
    for i, g, zz, ee in others:
        pl.semaphore_signal(barrier, inc=1, device_id=(lax.axis_index('dp'), zz, ee), device_id_type=MESH)

    def cp(src, dst, sem):
        return pltpu.make_async_copy(src, dst, sem)

    def m_q(l, j):
        k = 2 * l + j
        return cp(wq.at[l, :, pl.ds(j * CB, CB)], s.mbuf.at[k], s.s_m.at[k])

    def m_o(l, j):
        k = lax.rem(2 * l + 6 + j, 8)
        return cp(wo.at[l, :, pl.ds(j * CB, CB)], s.mbuf.at[k], s.s_m.at[k])

    def c_kv(l, t):
        return cp(kvs[l].at[t], s.kvb.at[t], s.s_kv.at[t])

    def c_uk(l):
        return cp(wuk.at[l], s.wukb, s.s_uk.at[0])

    def c_uv(l):
        return cp(wuv.at[l], s.wuvb, s.s_uk.at[1])

    def u_gu(what, i, k, j, w, half):
        o = pl.multiple_of(j * 256, 128)
        if what == 'ffn':
            src = w_in.at[i, half, :, pl.ds(pl.multiple_of(c * FH + o, 128), w)]
        else:
            src = e_in.at[i, :, pl.ds(pl.multiple_of(half * FH + o, 128), w)]
        dst = s.gu5.at[k, j, :, pl.ds(half * w, w)] if w == 256 else s.gu1.at[k, :, pl.ds(half * w, w)]
        return cp(src, dst, s.s_gu.at[k, j, half])

    def u_wd(what, i, k, j):
        cols = pl.ds(pl.multiple_of(j * CB, CB), CB)
        if what == 'ffn':
            src = w_out.at[i, pl.ds(pl.multiple_of(c * FH, 128), FH), cols]
        else:
            src = e_out.at[i, :, cols]
        return cp(src, s.wd.at[k, j], s.s_wd.at[k, j])

    def u_start(what, i, k):
        def gu(j, _):
            u_gu(what, i, k, j, 256, 0).start()
            u_gu(what, i, k, j, 256, 1).start()
            return 0

        lax.fori_loop(0, 5, gu, 0)
        u_gu(what, i, k, 5, 128, 0).start()
        u_gu(what, i, k, 5, 128, 1).start()

        def dn(j, _):
            u_wd(what, i, k, j).start()
            return 0

        lax.fori_loop(0, 4, dn, 0)

    def rc(src, dst, ss, rs, tp, ep):
        return pltpu.make_async_remote_copy(src_ref=src, dst_ref=dst, send_sem=ss, recv_sem=rs,
                                            device_id=(lax.axis_index('dp'), tp, ep), device_id_type=MESH)

    def send(*a):
        d = rc(*a)
        d.start()
        sends.append(d)

    for j in range(6):
        m_q(0, j).start()
    for t in range(B):
        c_kv(0, t).start()
    c_uk(0).start()
    c_uv(0).start()
    m_o(0, 0).start()
    m_o(0, 1).start()

    diag = lax.broadcasted_iota(I32, (B, B), 0) == lax.broadcasted_iota(I32, (B, B), 1)
    lrow = jnp.broadcast_to(lens[...].astype(F32).reshape(1, B), (B, B))
    lv = jnp.broadcast_to(jnp.sum(jnp.where(diag, lrow, 0.0), axis=1, keepdims=True), (B, L))
    at = jnp.where(lax.broadcasted_iota(I32, (B, L), 1).astype(F32) == lv - 1.0, 1.0, 0.0).astype(BF)
    tb = dot(at, table[...])
    tb = tb[:, :128] + tb[:, 128:256] + tb[:, 256:]
    s.cs[...] = jnp.concatenate([tb[:, :ROPE]] * HEADS, axis=0)
    s.sn[...] = jnp.concatenate([tb[:, ROPE:]] * HEADS, axis=0)
    rowt = lax.broadcasted_iota(I32, (R, L), 0) & (B - 1)
    s.lm[...] = jnp.concatenate([lv] * HEADS, axis=0)

    def q_steps(l, lo, hi):
        def step(j, _):
            m_q(l, j).wait()
            s.qs[:, pl.ds(pl.multiple_of(j * CB, CB), CB)] = dot(s.an[...], s.mbuf[2 * l + j])
            return 0

        lax.fori_loop(lo, hi, step, 0)

    def mla(l, after_two, after_q, after_uk, after_kv, after_uv):
        q_steps(l, 0, 2)
        after_two()
        q_steps(l, 2, 6)
        after_q()
        c_uk(l).wait()
        D = NOPE + ROPE
        rope = []
        for hp in range(HEADS // 2):
            pair = []
            for k in range(2):
                h = 2 * hp + k
                qn = s.qs[:, h * D:h * D + NOPE].astype(BF)
                pair.append(dot(qn, s.wukb[h]))
                rope.append(s.qs[:, h * D + NOPE:(h + 1) * D])
            s.qc[hp * 16:(hp + 1) * 16, :LAT] = jnp.concatenate(pair, axis=0).astype(BF)
        after_uk()
        r = jnp.concatenate(rope, axis=0)
        rot = jnp.concatenate([r[:, ROPE // 2:], r[:, :ROPE // 2]], axis=1)
        s.qc[:, LAT:] = (r * s.cs[...] + rot * s.sn[...]).astype(BF)
        for t in range(B):
            c_kv(l, t).wait()
            st = dot(s.qc[...], s.kvb[t])
            if t == 0:
                s.sc[...] = st
            else:
                s.sc[...] = jnp.where(rowt == t, st, s.sc[...])
        sc = jnp.where(lax.broadcasted_iota(I32, (R, L), 1).astype(F32) < s.lm[...], s.sc[...] * SCALE, -1e30)
        ex = jnp.exp(sc - jnp.max(sc, axis=-1, keepdims=True))
        p = ex / jnp.sum(ex, axis=-1, keepdims=True)
        ol = None
        for t in range(B):
            pt = jnp.where(rowt == t, p, 0.0).astype(BF)
            ot = lax.dot_general(pt, s.kvb[t, :LAT, :], (((1,), (1,)), ((), ())), preferred_element_type=F32)
            ol = ot if ol is None else ol + ot
        s.ol[...] = ol
        after_kv()
        c_uv(l).wait()
        for h in range(HEADS):
            o = dot(s.ol[h * B:(h + 1) * B, :].astype(BF), s.wuvb[h])
            s.os[:, h * VH:(h + 1) * VH] = o.astype(BF)
        after_uv()

        def step(j, _):
            m_o(l, j).wait()
            s.res[:, pl.ds(pl.multiple_of(j * CB, CB), CB)] = dot(s.os[...], s.mbuf[lax.rem(2 * l + 6 + j, 8)])
            return 0

        lax.fori_loop(0, 4, step, 0)

    def unit(what, i, k, lhs, down):
        def silu(g, u):
            return (g / (1.0 + jnp.exp(-g)) * u).astype(BF)

        def gu(j, _):
            u_gu(what, i, k, j, 256, 0).wait()
            u_gu(what, i, k, j, 256, 1).wait()
            r = dot(lhs[...], s.gu5[k, j])
            s.act[:, pl.ds(pl.multiple_of(j * 256, 256), 256)] = silu(r[:, :256], r[:, 256:])
            return 0

        lax.fori_loop(0, 5, gu, 0)
        u_gu(what, i, k, 5, 128, 0).wait()
        u_gu(what, i, k, 5, 128, 1).wait()
        r = dot(lhs[...], s.gu1[k])
        s.act[:, 1280:] = silu(r[:, :128], r[:, 128:])

        def dn(j, _):
            u_wd(what, i, k, j).wait()
            down(j, dot(s.act[...], s.wd[k, j]))
            return 0

        lax.fori_loop(0, 4, dn, 0)

    def gather(buf, ss, rs, at, on_y):
        own = at(z, e)
        for k in ALONG:
            send(buf.at[own], buf.at[own], ss.at[k - 1], rs.at[own], lax.rem(z + k, TP), e)
        send(buf.at[own], buf.at[own], ss.at[3], rs.at[own], z, pe)
        if on_y:
            send(buf.at[own], buf.at[own], ss.at[8], rs.at[own], z, ye)
        for k in ALONG:
            g = at(lax.rem(z + k, TP), e)
            rc(buf.at[g], buf.at[g], ss.at[3 + k], rs.at[g], z, pe).wait_recv()
            send(buf.at[g], buf.at[g], ss.at[3 + k], rs.at[g], z, pe)
            if on_y:
                send(buf.at[g], buf.at[g], ss.at[8 + k], rs.at[g], z, ye)
        for zz in range(TP):
            g = at(zz, pe)
            rc(buf.at[g], buf.at[g], ss.at[0], rs.at[g], z, pe).wait_recv()

    def stack(buf, at):
        for i, ee in enumerate((e, pe)):
            for q in range(2):
                s.fa[i * 32 + q * 16:i * 32 + q * 16 + 16, :] = jnp.concatenate([buf[at(2 * q, ee)], buf[at(2 * q + 1, ee)]], axis=0)

    def ffn(l, k):
        def down(j, r):
            s.pm[j] = r[:M // 2]
            s.ps[l, j] = r[M // 2:]
            rc(s.ps.at[l, j], s.pr.at[l, j], s.pss.at[l, j], s.psr.at[l, j], z, pe).start()

        unit('ffn', l, k, s.fa, down)

    def ffn_send(l):
        for j in range(4):
            rc(s.ps.at[l, j], s.pr.at[l, j], s.pss.at[l, j], s.psr.at[l, j], z, pe).wait()
            tot = s.pm[j] + s.pr[l, j]
            for q in range(TP):
                s.bs[l, q, :, j * CB:(j + 1) * CB] = tot[q * B:(q + 1) * B].astype(BF)
        for k in ALONG:
            zz = lax.rem(z + k, TP)
            send(s.bs.at[l, zz], s.br.at[l, z], s.bss.at[l, k], s.bsr.at[l, z], zz, e)
        s.br[l, z] = s.bs[l, z]

    def ffn_recv(l):
        for k in ALONG:
            zz = lax.rem(z + k, TP)
            rc(s.bs.at[l, zz], s.br.at[l, zz], s.bss.at[l, k], s.bsr.at[l, zz], zz, e).wait_recv()
        acc = s.br[l, 0].astype(F32)
        for q in range(1, TP):
            acc = acc + s.br[l, q].astype(F32)
        return acc

    def at16(zz, ee):
        return zz * 4 + ee

    def at8(zz, ee):
        return zz * 2 + lax.rem(ee, 2)

    def send_ids():
        s.idall[me] = jnp.full((B, 128), -1, I32)
        s.idall[me, :, 0:6] = ids[...]
        pl.semaphore_wait(barrier, N - 1)
        for i, g, zz, ee in others:
            send(s.idall.at[me], s.idall.at[me], s.ids_s.at[i], s.ids_r.at[me], zz, ee)

    def slots_here():
        lane = lax.broadcasted_iota(I32, (B, 128), 1)
        mine = s.idall[me]
        dst = [jnp.broadcast_to(mine[:, j:j + 1], (B, 128)) >> 2 for j in range(6)]
        hot = [jnp.where(d == lane, 1.0, 0.0) for d in dst]
        cnt = functools.reduce(jnp.add, hot)
        row = lax.broadcasted_iota(I32, (B, 128), 0)
        run = jnp.zeros((B, 128), F32)
        for t in range(B - 1):
            run = run + jnp.where(row > t, jnp.broadcast_to(cnt[t:t + 1], (B, 128)), 0.0)
        left, right = [], []
        for j in range(6):
            pos = jnp.sum(hot[j] * run, axis=1, keepdims=True)
            run = run + hot[j]
            col = dst[j].astype(F32) * B + pos
            left.append(jnp.where(col == lane.astype(F32), 1.0, 0.0))
            right.append(jnp.where(col + 4.0 == lane.astype(F32), 1.0, 0.0))
        s.gsel[...] = jnp.concatenate(left + right, axis=0).astype(BF)

    def slots_there():
        for i, g, zz, ee in others:
            rc(s.idall.at[g], s.idall.at[g], s.ids_s.at[i], s.ids_r.at[g], z, pe).wait_recv()
        T = N * B
        idt = jnp.concatenate([s.idall[d] for d in range(N)], axis=0)
        lane = lax.broadcasted_iota(I32, (T, 128), 1)
        tok = lax.broadcasted_iota(I32, (T, 128), 0)
        col = [jnp.broadcast_to(idt[:, j:j + 1], (T, 128)) for j in range(6)]
        hit = [jnp.where((v >> 2) == me, 1.0, 0.0) for v in col]
        before = jnp.where((tok >> 3 == lane >> 3) & (lane < tok), 1.0, 0.0)
        run = dot(before.astype(BF), functools.reduce(jnp.add, hit).astype(BF)) + ((tok >> 3) * 4).astype(F32)
        pt = jnp.zeros((T, 128), F32)
        ex = jnp.zeros((T, 128), F32)
        for j in range(6):
            at = jnp.where(run == lane.astype(F32), hit[j], 0.0)
            pt = pt + at
            ex = ex + at * (col[j] & 3).astype(F32)
            run = run + hit[j]
        s.ptk[...] = pt[:, :M].astype(BF)
        s.el[...] = lax.dot_general(ex[:, :M].astype(BF), jnp.ones((T, 128), BF), (((0,), (0,)), ((), ())),
                                    preferred_element_type=F32)

    def expert(i, k):
        def down(j, r):
            cols = pl.ds(pl.multiple_of(j * CB, CB), CB)
            r = r.astype(BF).astype(F32)
            if i == 0:
                s.racc[:, cols] = r
            else:
                keep = jnp.broadcast_to(s.el[:, 0:1], (M, CB)) == float(i)
                s.racc[:, cols] = jnp.where(keep, r, s.racc[:, cols])

        unit('moe', i, k, s.ea, down)

    def give_back():
        for d in range(N):
            a = s.racc[4 * d:4 * d + 4, :]
            s.rs[d] = jnp.concatenate([a[:, :H // 2], a[:, H // 2:]], axis=0).astype(BF)
        for i, g, zz, ee in others:
            send(s.rs.at[g], s.rr.at[me], s.ret_s.at[i], s.ret_r.at[me], zz, ee)
        s.rr[me] = s.rs[me]

    def take_back():
        for i, g, zz, ee in others:
            rc(s.rs.at[g], s.rr.at[g], s.ret_s.at[i], s.ret_r.at[g], z, pe).wait_recv()
        for d in range(N // 2):
            s.rk[d * 16:(d + 1) * 16, :] = jnp.concatenate([s.rr[2 * d], s.rr[2 * d + 1]], axis=0)
        got = dot(s.gsel[...], s.rk[...])
        for half in range(2):
            acc = None
            for j in range(6):
                o = (half * 6 + j) * B
                term = wts[:, j:j + 1] * got[o:o + B]
                acc = term if acc is None else acc + term
            s.mm[:, half * (H // 2):(half + 1) * (H // 2)] = acc

    nothing = lambda: None

    s.an[...] = rms(x[...])

    def two0():
        m_o(0, 2).start()
        m_o(0, 3).start()
        u_start('ffn', 0, 0)
        u_start('moe', 0, 1)
        send_ids()

    def q0():
        for j in range(4):
            m_q(1, j).start()

    def kv0_done():
        for t in range(B):
            c_kv(1, t).start()

    mla(0, two0, q0, lambda: c_uk(1).start(), kv0_done, lambda: c_uv(1).start())
    for j in (4, 5):
        m_q(1, j).start()
    for j in (0, 1):
        m_o(1, j).start()
    h0 = (x[...].astype(F32) + s.res[...]).astype(BF)
    s.h0[...] = h0
    s.uall[me] = rms(h0)
    slots_here()
    gather(s.uall, s.us, s.ur, at16, True)
    slots_there()
    stack(s.uall, at16)
    ffn(0, 0)
    u_start('moe', 1, 0)
    for zz in range(TP):
        g = at16(zz, ye)
        rc(s.uall.at[g], s.uall.at[g], s.us.at[12 + zz], s.ur.at[g], z, pe).wait_recv()
        send(s.uall.at[g], s.uall.at[g], s.us.at[12 + zz], s.ur.at[g], z, pe)
    ffn_send(0)
    for zz in range(TP):
        g = at16(zz, ype)
        rc(s.uall.at[g], s.uall.at[g], s.us.at[12 + zz], s.ur.at[g], z, pe).wait_recv()
    for half in range(2):
        cols = pl.ds(half * (H // 2), H // 2)
        for d in range(N // 2):
            s.rk[d * 16:(d + 1) * 16, :] = jnp.concatenate([s.uall[2 * d, :, cols], s.uall[2 * d + 1, :, cols]], axis=0)
        s.ea[:, cols] = lax.dot_general(s.ptk[...], s.rk[...], (((0,), (0,)), ((), ())),
                                        preferred_element_type=F32).astype(BF)
    expert(0, 1)
    u_start('moe', 2, 1)
    f0 = (s.h0[...].astype(F32) + ffn_recv(0)).astype(BF)
    s.f0[...] = f0
    s.an[...] = rms(f0)

    def q1():
        m_o(1, 2).start()
        m_o(1, 3).start()

    mla(1, nothing, q1, nothing, nothing, nothing)
    h1 = (s.f0[...].astype(F32) + s.res[...]).astype(BF)
    s.h1[...] = h1
    s.vall[at8(z, e)] = rms(h1)
    gather(s.vall, s.vs, s.vr, at8, False)
    stack(s.vall, at8)
    expert(1, 0)
    u_start('moe', 3, 0)
    expert(2, 1)
    u_start('ffn', 1, 1)
    expert(3, 0)
    give_back()
    ffn(1, 1)
    ffn_send(1)
    take_back()
    y[...] = (s.h1[...].astype(F32) + ffn_recv(1) + s.mm[...]).astype(BF)
    for d in sends:
        d.wait_send()


def rope_table():
    half = ROPE // 2
    f = np.float32(10000.0) ** (np.float32(-2.0) * np.arange(half, dtype=np.float32) / np.float32(ROPE))
    ang = np.arange(1, L + 1, dtype=np.float32)[:, None] * f.astype(np.float32)
    cs, sn = np.cos(ang.astype(np.float64)), np.sin(ang.astype(np.float64))
    left = np.concatenate([cs, cs, -sn, sn], axis=1).astype(np.float32)
    parts = []
    for _ in range(3):
        part = left.astype(jnp.bfloat16)
        parts.append(part)
        left = left - part.astype(np.float32)
    return jnp.asarray(np.concatenate(parts, axis=1))


def layer(x, kv0, kv1, lens, ids, wts, wq, wuk, wuv, wo, w_in, w_out, e_in, e_out):
    table = rope_table()
    sc = scratch()
    vm = pl.BlockSpec(memory_space=pltpu.VMEM)
    hbm = pl.BlockSpec(memory_space=pl.ANY)
    return pl.pallas_call(
        functools.partial(kernel, tuple(sc)),
        out_shape=jax.ShapeDtypeStruct((B, H), BF),
        in_specs=[vm] * 5 + [hbm] * 10,
        out_specs=vm,
        scratch_shapes=list(sc.values()),
        compiler_params=pltpu.CompilerParams(collective_id=0, has_side_effects=True, vmem_limit_bytes=67043328),
    )(x, lens, ids, wts, table, jnp.swapaxes(kv0, 1, 2), jnp.swapaxes(kv1, 1, 2), wq, wuk, wuv, wo, w_in, w_out, e_in, e_out)


def solution(mesh):
    in_specs = (P(BATCH, None), P(BATCH, None, None), P(BATCH, None, None), P(BATCH), P(BATCH, None), P(BATCH, None),
                P(), P(), P(), P(), P(None, None, None, 'tp'), P(None, 'tp', None), P(GROUP, None, None), P(GROUP, None, None))
    return jax.shard_map(layer, mesh=mesh, in_specs=in_specs, out_specs=P(BATCH, None), check_vma=False)
```

```python
import functools
import types

import jax
import jax.numpy as jnp
import numpy as np
from jax import lax
from jax.experimental import pallas as pl
from jax.experimental.pallas import tpu as pltpu
from jax.sharding import PartitionSpec as P

BATCH = ('dp', 'tp', 'ep')
GROUP = ('tp', 'ep')
MESH = pl.DeviceIdType.MESH
BF = jnp.bfloat16
F32 = jnp.float32
I32 = jnp.int32

B = 8
H = 2048
HEADS = 16
NOPE = 128
ROPE = 64
LAT = 512
VH = 128
L = 256
FH = 1408
TP = 4
N = 16
R = HEADS * B
M = 64
CB = 512
SCALE = (NOPE + ROPE) ** -0.5

ALONG = (1, 3, 2)


def scratch():
    dma = pltpu.SemaphoreType.DMA
    v = pltpu.VMEM
    return dict(
        x=v((B, H), BF), lens=v((B,), I32), ids=v((B, 6), I32), wts=v((B, 6), F32), table=v((L, 384), BF), s_in=dma((5,)),
        mbuf=v((8, H, CB), BF), wukb=v((HEADS, NOPE, LAT), BF), wuvb=v((HEADS, LAT, VH), BF), kvb=v((B, LAT + ROPE, L), BF),
        gu5=v((2, 5, H, CB), BF), gu1=v((2, H, CB // 2), BF), wd=v((2, 4, FH, CB), BF),
        qs=v((B, HEADS * (NOPE + ROPE)), F32), qc=v((R, LAT + ROPE), BF), sc=v((R, L), F32),
        ol=v((R, LAT), F32), os=v((B, HEADS * VH), BF), res=v((B, H), F32), an=v((B, H), BF),
        h0=v((B, H), BF), f0=v((B, H), BF), h1=v((B, H), BF),
        cs=v((R, ROPE), F32), sn=v((R, ROPE), F32), lm=v((R, L), F32),
        uall=v((N, B, H), BF), vall=v((N // 2, B, H), BF), fa=v((M, H), BF), ea=v((M, H), BF), act=v((M, FH), BF),
        pm=v((4, M // 2, CB), F32), ps=v((2, 4, M // 2, CB), F32), pr=v((2, 4, M // 2, CB), F32),
        bs=v((2, TP, 4, B, CB), BF), br=v((2, TP, 4, B, CB), BF),
        idall=v((N, B, 128), I32), ptk=v((N * B, M), BF), el=v((M, 128), F32), gsel=v((2 * 6 * B, 128), BF),
        racc=v((M, H), F32), rs=v((N, B, H // 2), BF), rr=v((N, B, H // 2), BF), rk=v((N * B, H // 2), BF), mm=v((B, H), F32),
        s_m=dma((8,)), s_kv=dma((B,)), s_uk=dma((2,)), s_gu=dma((2, 6, 2)), s_wd=dma((2, 4)),
        us=dma((16,)), ur=dma((N,)), vs=dma((8,)), vr=dma((N // 2,)),
        pss=dma((2, 4)), psr=dma((2, 4)), bss=dma((2, TP, 4)), bsr=dma((2, TP, 4)),
        ids_s=dma((N,)), ids_r=dma((N,)), ret_s=dma((N,)), ret_r=dma((N,)),
    )


def rms(v):
    vf = v.astype(F32)
    return (vf * lax.rsqrt(jnp.mean(vf * vf, axis=-1, keepdims=True) + 1e-6)).astype(BF)


def dot(a, b):
    return jnp.dot(a, b, preferred_element_type=F32)


def kernel(names, x_in, lens_in, ids_in, wts_in, table_in, kv0, kv1, wq, wuk, wuv, wo, w_in, w_out, e_in, e_out, y, *scr):
    s = types.SimpleNamespace(**dict(zip(names, scr)))
    z = lax.axis_index('tp')
    e = lax.axis_index('ep')
    me = z * 4 + e
    c = lax.rem(e, 2)
    pe = e + 1 - 2 * c
    ye = lax.rem(e + 2, 4)
    ype = lax.rem(pe + 2, 4)
    kvs = (kv0, kv1)
    x, lens, ids, wts, table = s.x, s.lens, s.ids, s.wts, s.table
    small = [pltpu.make_async_copy(a, b, s.s_in.at[i]) for i, (a, b) in enumerate(
        ((x_in, x), (lens_in, lens), (table_in, table), (ids_in, ids), (wts_in, wts)))]
    sends = []

    barrier = pltpu.get_barrier_semaphore()
    others = []
    for i in range(1, N):
        zz, ee = lax.rem(z + i // 4, 4), lax.rem(e + i % 4, 4)
        others.append((i, zz * 4 + ee, zz, ee))
    for i, g, zz, ee in others:
        pl.semaphore_signal(barrier, inc=1, device_id=(lax.axis_index('dp'), zz, ee), device_id_type=MESH)

    def cp(src, dst, sem):
        return pltpu.make_async_copy(src, dst, sem)

    def m_q(l, j):
        k = 2 * l + j
        return cp(wq.at[l, :, pl.ds(j * CB, CB)], s.mbuf.at[k], s.s_m.at[k])

    def m_o(l, j):
        k = lax.rem(2 * l + 6 + j, 8)
        return cp(wo.at[l, :, pl.ds(j * CB, CB)], s.mbuf.at[k], s.s_m.at[k])

    def c_kv(l, t):
        return cp(kvs[l].at[t], s.kvb.at[t], s.s_kv.at[t])

    def c_uk(l):
        return cp(wuk.at[l], s.wukb, s.s_uk.at[0])

    def c_uv(l):
        return cp(wuv.at[l], s.wuvb, s.s_uk.at[1])

    def u_gu(what, i, k, j, w, half):
        o = pl.multiple_of(j * 256, 128)
        if what == 'ffn':
            src = w_in.at[i, half, :, pl.ds(pl.multiple_of(c * FH + o, 128), w)]
        else:
            src = e_in.at[i, :, pl.ds(pl.multiple_of(half * FH + o, 128), w)]
        dst = s.gu5.at[k, j, :, pl.ds(half * w, w)] if w == 256 else s.gu1.at[k, :, pl.ds(half * w, w)]
        return cp(src, dst, s.s_gu.at[k, j, half])

    def u_wd(what, i, k, j):
        cols = pl.ds(pl.multiple_of(j * CB, CB), CB)
        if what == 'ffn':
            src = w_out.at[i, pl.ds(pl.multiple_of(c * FH, 128), FH), cols]
        else:
            src = e_out.at[i, :, cols]
        return cp(src, s.wd.at[k, j], s.s_wd.at[k, j])

    def u_start(what, i, k):
        def gu(j, _):
            u_gu(what, i, k, j, 256, 0).start()
            u_gu(what, i, k, j, 256, 1).start()
            return 0

        lax.fori_loop(0, 5, gu, 0)
        u_gu(what, i, k, 5, 128, 0).start()
        u_gu(what, i, k, 5, 128, 1).start()

        def dn(j, _):
            u_wd(what, i, k, j).start()
            return 0

        lax.fori_loop(0, 4, dn, 0)

    def rc(src, dst, ss, rs, tp, ep):
        return pltpu.make_async_remote_copy(src_ref=src, dst_ref=dst, send_sem=ss, recv_sem=rs,
                                            device_id=(lax.axis_index('dp'), tp, ep), device_id_type=MESH)

    def send(*a):
        d = rc(*a)
        d.start()
        sends.append(d)

    small[0].start()
    m_q(0, 0).start()
    for d in small[1:]:
        d.start()
    for j in range(1, 6):
        m_q(0, j).start()
    for t in range(B):
        c_kv(0, t).start()
    c_uk(0).start()
    c_uv(0).start()
    m_o(0, 0).start()
    m_o(0, 1).start()

    def positions():
        with jax.named_scope('positions'):
            return positions_()

    def positions_():
        for d in small[1:]:
            d.wait()
        diag = lax.broadcasted_iota(I32, (B, B), 0) == lax.broadcasted_iota(I32, (B, B), 1)
        lrow = jnp.broadcast_to(lens[...].astype(F32).reshape(1, B), (B, B))
        lv = jnp.broadcast_to(jnp.sum(jnp.where(diag, lrow, 0.0), axis=1, keepdims=True), (B, L))
        at = jnp.where(lax.broadcasted_iota(I32, (B, L), 1).astype(F32) == lv - 1.0, 1.0, 0.0).astype(BF)
        tb = dot(at, table[...])
        tb = tb[:, :128] + tb[:, 128:256] + tb[:, 256:]
        s.cs[...] = jnp.concatenate([tb[:, :ROPE]] * HEADS, axis=0)
        s.sn[...] = jnp.concatenate([tb[:, ROPE:]] * HEADS, axis=0)
        s.lm[...] = jnp.concatenate([lv] * HEADS, axis=0)

    rowt = lax.broadcasted_iota(I32, (R, L), 0) & (B - 1)

    def q_steps(l, lo, hi):
        with jax.named_scope(f'q_steps{l}'):
            return q_steps_(l, lo, hi)

    def q_steps_(l, lo, hi):
        def step(j, _):
            m_q(l, j).wait()
            s.qs[:, pl.ds(pl.multiple_of(j * CB, CB), CB)] = dot(s.an[...], s.mbuf[2 * l + j])
            return 0

        lax.fori_loop(lo, hi, step, 0)

    def mla(l, after_two, after_q, after_uk, after_kv, after_uv):
        q_steps(l, 0, 2)
        after_two()
        q_steps(l, 2, 6)
        after_q()
        latent_q(l)
        after_uk()
        attend(l)
        after_kv()
        values(l)
        after_uv()
        project(l)

    def latent_q(l):
        with jax.named_scope(f'latent_q{l}'):
            return latent_q_(l)

    def latent_q_(l):
        c_uk(l).wait()
        D = NOPE + ROPE
        rope = []
        for hp in range(HEADS // 2):
            pair = []
            for k in range(2):
                h = 2 * hp + k
                qn = s.qs[:, h * D:h * D + NOPE].astype(BF)
                pair.append(dot(qn, s.wukb[h]))
                rope.append(s.qs[:, h * D + NOPE:(h + 1) * D])
            s.qc[hp * 16:(hp + 1) * 16, :LAT] = jnp.concatenate(pair, axis=0).astype(BF)
        r = jnp.concatenate(rope, axis=0)
        rot = jnp.concatenate([r[:, ROPE // 2:], r[:, :ROPE // 2]], axis=1)
        s.qc[:, LAT:] = (r * s.cs[...] + rot * s.sn[...]).astype(BF)

    def attend(l):
        with jax.named_scope(f'attend{l}'):
            return attend_(l)

    def attend_(l):
        for t in range(B):
            c_kv(l, t).wait()
            st = dot(s.qc[...], s.kvb[t])
            if t == 0:
                s.sc[...] = st
            else:
                s.sc[...] = jnp.where(rowt == t, st, s.sc[...])
        sc = jnp.where(lax.broadcasted_iota(I32, (R, L), 1).astype(F32) < s.lm[...], s.sc[...] * SCALE, -1e30)
        ex = jnp.exp(sc - jnp.max(sc, axis=-1, keepdims=True))
        p = ex / jnp.sum(ex, axis=-1, keepdims=True)
        ol = None
        for t in range(B):
            pt = jnp.where(rowt == t, p, 0.0).astype(BF)
            ot = lax.dot_general(pt, s.kvb[t, :LAT, :], (((1,), (1,)), ((), ())), preferred_element_type=F32)
            ol = ot if ol is None else ol + ot
        s.ol[...] = ol

    def values(l):
        with jax.named_scope(f'values{l}'):
            return values_(l)

    def values_(l):
        c_uv(l).wait()
        for h in range(HEADS):
            o = dot(s.ol[h * B:(h + 1) * B, :].astype(BF), s.wuvb[h])
            s.os[:, h * VH:(h + 1) * VH] = o.astype(BF)

    def project(l):
        with jax.named_scope(f'project{l}'):
            return project_(l)

    def project_(l):
        def step(j, _):
            m_o(l, j).wait()
            s.res[:, pl.ds(pl.multiple_of(j * CB, CB), CB)] = dot(s.os[...], s.mbuf[lax.rem(2 * l + 6 + j, 8)])
            return 0

        lax.fori_loop(0, 4, step, 0)

    def unit(what, i, k, lhs, down_groups, down, between):
        def silu(g, u):
            return (g / (1.0 + jnp.exp(-g)) * u).astype(BF)

        for group in ((0, 1, 2), (3, 4, 5)):
            for j in group:
                w = 256 if j < 5 else 128
                u_gu(what, i, k, j, w, 0).wait()
                u_gu(what, i, k, j, w, 1).wait()
            for j in group:
                w = 256 if j < 5 else 128
                r = dot(lhs[...], s.gu5[k, j] if j < 5 else s.gu1[k])
                s.act[:, j * 256:j * 256 + w] = silu(r[:, :w], r[:, w:])
        between()
        for group in down_groups:
            for j in group:
                u_wd(what, i, k, j).wait()
            down(group, lambda j: dot(s.act[...], s.wd[k, j]))

    def gather_start(buf, ss, rs, at, on_y):
        with jax.named_scope('gather_start'):
            return gather_start_(buf, ss, rs, at, on_y)

    def gather_start_(buf, ss, rs, at, on_y):
        own = at(z, e)
        for k in ALONG:
            send(buf.at[own], buf.at[own], ss.at[k - 1], rs.at[own], lax.rem(z + k, TP), e)
        send(buf.at[own], buf.at[own], ss.at[3], rs.at[own], z, pe)
        if on_y:
            send(buf.at[own], buf.at[own], ss.at[8], rs.at[own], z, ye)

    def gather_pass(buf, ss, rs, at, on_y):
        with jax.named_scope('gather_pass'):
            return gather_pass_(buf, ss, rs, at, on_y)

    def gather_pass_(buf, ss, rs, at, on_y):
        for k in ALONG:
            g = at(lax.rem(z + k, TP), e)
            rc(buf.at[g], buf.at[g], ss.at[3 + k], rs.at[g], z, pe).wait_recv()
            send(buf.at[g], buf.at[g], ss.at[3 + k], rs.at[g], z, pe)
            if on_y:
                send(buf.at[g], buf.at[g], ss.at[8 + k], rs.at[g], z, ye)

    def gather_wait(buf, ss, rs, at):
        with jax.named_scope('gather_wait'):
            return gather_wait_(buf, ss, rs, at)

    def gather_wait_(buf, ss, rs, at):
        for zz in range(TP):
            g = at(zz, pe)
            rc(buf.at[g], buf.at[g], ss.at[0], rs.at[g], z, pe).wait_recv()

    def stack(buf, at):
        with jax.named_scope('stack'):
            return stack_(buf, at)

    def stack_(buf, at):
        for i, ee in enumerate((e, pe)):
            for q in range(2):
                s.fa[i * 32 + q * 16:i * 32 + q * 16 + 16, :] = jnp.concatenate([buf[at(2 * q, ee)], buf[at(2 * q + 1, ee)]], axis=0)

    def ffn(l, k, between):
        with jax.named_scope(f'ffn{l}'):
            return ffn_(l, k, between)

    def ffn_(l, k, between):
        def down(group, product):
            for j in group:
                r = product(j)
                s.pm[j] = r[:M // 2]
                s.ps[l, j] = r[M // 2:]
            for j in group:
                rc(s.ps.at[l, j], s.pr.at[l, j], s.pss.at[l, j], s.psr.at[l, j], z, pe).start()

        unit('ffn', l, k, s.fa, ((0, 1), (2, 3)), down, between)

    def ffn_send(l):
        with jax.named_scope(f'ffn_send{l}'):
            return ffn_send_(l)

    def ffn_send_(l):
        for j in range(4):
            rc(s.ps.at[l, j], s.pr.at[l, j], s.pss.at[l, j], s.psr.at[l, j], z, pe).wait()
            tot = s.pm[j] + s.pr[l, j]
            for q in range(TP):
                s.bs[l, q, j] = tot[q * B:(q + 1) * B].astype(BF)
            for k in ALONG:
                zz = lax.rem(z + k, TP)
                send(s.bs.at[l, zz, j], s.br.at[l, z, j], s.bss.at[l, k, j], s.bsr.at[l, z, j], zz, e)
            s.br[l, z, j] = s.bs[l, z, j]

    def ffn_recv(l):
        with jax.named_scope(f'ffn_recv{l}'):
            return ffn_recv_(l)

    def ffn_recv_(l):
        for j in range(4):
            for k in ALONG:
                zz = lax.rem(z + k, TP)
                rc(s.bs.at[l, zz, j], s.br.at[l, zz, j], s.bss.at[l, k, j], s.bsr.at[l, zz, j], zz, e).wait_recv()
            acc = s.br[l, 0, j].astype(F32)
            for q in range(1, TP):
                acc = acc + s.br[l, q, j].astype(F32)
            s.res[:, j * CB:(j + 1) * CB] = acc
        return s.res[...]

    def at16(zz, ee):
        return zz * 4 + ee

    def at8(zz, ee):
        return zz * 2 + lax.rem(ee, 2)

    def send_ids():
        with jax.named_scope('send_ids'):
            return send_ids_()

    def send_ids_():
        s.idall[me] = jnp.full((B, 128), -1, I32)
        s.idall[me, :, 0:6] = ids[...]
        pl.semaphore_wait(barrier, N - 1)
        for i, g, zz, ee in others:
            send(s.idall.at[me], s.idall.at[me], s.ids_s.at[i], s.ids_r.at[me], zz, ee)

    def slots_here():
        with jax.named_scope('slots_here'):
            return slots_here_()

    def slots_here_():
        lane = lax.broadcasted_iota(I32, (B, 128), 1)
        mine = s.idall[me]
        dst = [jnp.broadcast_to(mine[:, j:j + 1], (B, 128)) >> 2 for j in range(6)]
        hot = [jnp.where(d == lane, 1.0, 0.0) for d in dst]
        cnt = functools.reduce(jnp.add, hot)
        row = lax.broadcasted_iota(I32, (B, 128), 0)
        run = jnp.zeros((B, 128), F32)
        for t in range(B - 1):
            run = run + jnp.where(row > t, jnp.broadcast_to(cnt[t:t + 1], (B, 128)), 0.0)
        left, right = [], []
        for j in range(6):
            pos = jnp.sum(hot[j] * run, axis=1, keepdims=True)
            run = run + hot[j]
            col = dst[j].astype(F32) * B + pos
            left.append(jnp.where(col == lane.astype(F32), 1.0, 0.0))
            right.append(jnp.where(col + 4.0 == lane.astype(F32), 1.0, 0.0))
        s.gsel[...] = jnp.concatenate(left + right, axis=0).astype(BF)

    def slots_there():
        with jax.named_scope('slots_there'):
            return slots_there_()

    def slots_there_():
        for i, g, zz, ee in others:
            rc(s.idall.at[g], s.idall.at[g], s.ids_s.at[i], s.ids_r.at[g], z, pe).wait_recv()
        T = N * B
        idt = jnp.concatenate([s.idall[d] for d in range(N)], axis=0)
        lane = lax.broadcasted_iota(I32, (T, 128), 1)
        tok = lax.broadcasted_iota(I32, (T, 128), 0)
        col = [jnp.broadcast_to(idt[:, j:j + 1], (T, 128)) for j in range(6)]
        hit = [jnp.where((v >> 2) == me, 1.0, 0.0) for v in col]
        before = jnp.where((tok >> 3 == lane >> 3) & (lane < tok), 1.0, 0.0)
        run = dot(before.astype(BF), functools.reduce(jnp.add, hit).astype(BF)) + ((tok >> 3) * 4).astype(F32)
        pt = jnp.zeros((T, 128), F32)
        ex = jnp.zeros((T, 128), F32)
        for j in range(6):
            at = jnp.where(run == lane.astype(F32), hit[j], 0.0)
            pt = pt + at
            ex = ex + at * (col[j] & 3).astype(F32)
            run = run + hit[j]
        s.ptk[...] = pt[:, :M].astype(BF)
        s.el[...] = lax.dot_general(ex[:, :M].astype(BF), jnp.ones((T, 128), BF), (((0,), (0,)), ((), ())),
                                    preferred_element_type=F32)

    def expert(i, k, between):
        with jax.named_scope(f'expert{i}'):
            return expert_(i, k, between)

    def expert_(i, k, between):
        def down(group, product):
            for j in group:
                cols = pl.ds(j * CB, CB)
                r = product(j).astype(BF).astype(F32)
                if i == 0:
                    s.racc[:, cols] = r
                else:
                    keep = jnp.broadcast_to(s.el[:, 0:1], (M, CB)) == float(i)
                    s.racc[:, cols] = jnp.where(keep, r, s.racc[:, cols])

        unit('moe', i, k, s.ea, ((0, 1, 2, 3),), down, between)

    def give_back():
        with jax.named_scope('give_back'):
            return give_back_()

    def give_back_():
        for d in range(N):
            a = s.racc[4 * d:4 * d + 4, :]
            s.rs[d] = jnp.concatenate([a[:, :H // 2], a[:, H // 2:]], axis=0).astype(BF)
        for i, g, zz, ee in others:
            send(s.rs.at[g], s.rr.at[me], s.ret_s.at[i], s.ret_r.at[me], zz, ee)
        s.rr[me] = s.rs[me]

    def take_back():
        with jax.named_scope('take_back'):
            return take_back_()

    def take_back_():
        for i, g, zz, ee in others:
            rc(s.rs.at[g], s.rr.at[g], s.ret_s.at[i], s.ret_r.at[g], z, pe).wait_recv()
        for d in range(N // 2):
            s.rk[d * 16:(d + 1) * 16, :] = jnp.concatenate([s.rr[2 * d], s.rr[2 * d + 1]], axis=0)
        got = dot(s.gsel[...], s.rk[...])
        for half in range(2):
            acc = None
            for j in range(6):
                o = (half * 6 + j) * B
                term = wts[:, j:j + 1] * got[o:o + B]
                acc = term if acc is None else acc + term
            s.mm[:, half * (H // 2):(half + 1) * (H // 2)] = acc

    nothing = lambda: None

    small[0].wait()
    s.an[...] = rms(x[...])

    def two0():
        m_o(0, 2).start()
        m_o(0, 3).start()
        u_start('ffn', 0, 0)
        u_start('moe', 0, 1)
        positions()

    def q0():
        for j in range(4):
            m_q(1, j).start()

    def kv0_done():
        for t in range(B):
            c_kv(1, t).start()

    def uk0():
        c_uk(1).start()
        send_ids()

    mla(0, two0, q0, uk0, kv0_done, lambda: c_uv(1).start())
    for j in (4, 5):
        m_q(1, j).start()
    for j in (0, 1):
        m_o(1, j).start()
    h0 = (x[...].astype(F32) + s.res[...]).astype(BF)
    s.h0[...] = h0
    s.uall[me] = rms(h0)
    gather_start(s.uall, s.us, s.ur, at16, True)
    slots_here()
    slots_there()
    gather_pass(s.uall, s.us, s.ur, at16, True)
    gather_wait(s.uall, s.us, s.ur, at16)
    stack(s.uall, at16)
    ffn(0, 0, nothing)
    u_start('moe', 1, 0)
    for zz in range(TP):
        g = at16(zz, ye)
        rc(s.uall.at[g], s.uall.at[g], s.us.at[12 + zz], s.ur.at[g], z, pe).wait_recv()
        send(s.uall.at[g], s.uall.at[g], s.us.at[12 + zz], s.ur.at[g], z, pe)
    ffn_send(0)
    for zz in range(TP):
        g = at16(zz, ype)
        rc(s.uall.at[g], s.uall.at[g], s.us.at[12 + zz], s.ur.at[g], z, pe).wait_recv()
    for half in range(2):
        cols = pl.ds(half * (H // 2), H // 2)
        for d in range(N // 2):
            s.rk[d * 16:(d + 1) * 16, :] = jnp.concatenate([s.uall[2 * d, :, cols], s.uall[2 * d + 1, :, cols]], axis=0)
        s.ea[:, cols] = lax.dot_general(s.ptk[...], s.rk[...], (((0,), (0,)), ((), ())),
                                        preferred_element_type=F32).astype(BF)
    expert(0, 1, nothing)
    f0 = (s.h0[...].astype(F32) + ffn_recv(0)).astype(BF)
    s.f0[...] = f0
    s.an[...] = rms(f0)

    def two1():
        m_o(1, 2).start()
        m_o(1, 3).start()
        u_start('moe', 2, 1)

    mla(1, two1, nothing, nothing, nothing, nothing)
    h1 = (s.f0[...].astype(F32) + s.res[...]).astype(BF)
    s.h1[...] = h1
    s.vall[at8(z, e)] = rms(h1)
    gather_start(s.vall, s.vs, s.vr, at8, False)
    expert(1, 0, lambda: gather_pass(s.vall, s.vs, s.vr, at8, False))
    u_start('moe', 3, 0)
    expert(2, 1, nothing)
    u_start('ffn', 1, 1)
    expert(3, 0, nothing)
    give_back()
    gather_wait(s.vall, s.vs, s.vr, at8)
    stack(s.vall, at8)
    ffn(1, 1, nothing)
    ffn_send(1)
    take_back()
    y[...] = (s.h1[...].astype(F32) + ffn_recv(1) + s.mm[...]).astype(BF)
    for d in sends:
        d.wait_send()


def rope_table():
    half = ROPE // 2
    f = np.float32(10000.0) ** (np.float32(-2.0) * np.arange(half, dtype=np.float32) / np.float32(ROPE))
    ang = np.arange(1, L + 1, dtype=np.float32)[:, None] * f.astype(np.float32)
    cs, sn = np.cos(ang.astype(np.float64)), np.sin(ang.astype(np.float64))
    left = np.concatenate([cs, cs, -sn, sn], axis=1).astype(np.float32)
    parts = []
    for _ in range(3):
        part = left.astype(jnp.bfloat16)
        parts.append(part)
        left = left - part.astype(np.float32)
    return jnp.asarray(np.concatenate(parts, axis=1))


def layer(x, kv0, kv1, lens, ids, wts, wq, wuk, wuv, wo, w_in, w_out, e_in, e_out):
    table = rope_table()
    sc = scratch()
    vm = pl.BlockSpec(memory_space=pltpu.VMEM)
    hbm = pl.BlockSpec(memory_space=pl.ANY)
    return pl.pallas_call(
        functools.partial(kernel, tuple(sc)),
        out_shape=jax.ShapeDtypeStruct((B, H), BF),
        in_specs=[hbm] * 15,
        out_specs=vm,
        scratch_shapes=list(sc.values()),
        compiler_params=pltpu.CompilerParams(collective_id=0, has_side_effects=True, vmem_limit_bytes=67043328),
    )(x, lens, ids, wts, table, jnp.swapaxes(kv0, 1, 2), jnp.swapaxes(kv1, 1, 2), wq, wuk, wuv, wo, w_in, w_out, e_in, e_out)


def solution(mesh):
    in_specs = (P(BATCH, None), P(BATCH, None, None), P(BATCH, None, None), P(BATCH), P(BATCH, None), P(BATCH, None),
                P(), P(), P(), P(), P(None, None, None, 'tp'), P(None, 'tp', None), P(GROUP, None, None), P(GROUP, None, None))
    return jax.shard_map(layer, mesh=mesh, in_specs=in_specs, out_specs=P(BATCH, None), check_vma=False)
```

```python
import functools
import types

import jax
import jax.numpy as jnp
import numpy as np
from jax import lax
from jax.experimental import pallas as pl
from jax.experimental.pallas import tpu as pltpu
from jax.sharding import PartitionSpec as P

BATCH = ('dp', 'tp', 'ep')
GROUP = ('tp', 'ep')
MESH = pl.DeviceIdType.MESH
BF = jnp.bfloat16
F32 = jnp.float32
I32 = jnp.int32

B = 8
H = 2048
HEADS = 16
NOPE = 128
ROPE = 64
LAT = 512
VH = 128
L = 256
FH = 1408
TP = 4
N = 16
R = HEADS * B
M = 64
CB = 512
SCALE = (NOPE + ROPE) ** -0.5

ALONG = (1, 3, 2)


def scratch():
    dma = pltpu.SemaphoreType.DMA
    v = pltpu.VMEM
    return dict(
        x=v((B, H), BF), lens=v((B,), I32), ids=v((B, 6), I32), wts=v((B, 6), F32), table=v((L, 384), BF), s_in=dma((5,)),
        mbuf=v((8, H, CB), BF), wukb=v((HEADS, NOPE, LAT), BF), wuvb=v((HEADS, LAT, VH), BF), kvb=v((B, LAT + ROPE, L), BF),
        gu5=v((2, 5, H, CB), BF), gu1=v((2, H, CB // 2), BF), wd=v((2, 4, FH, CB), BF),
        qs=v((B, HEADS * (NOPE + ROPE)), F32), qc=v((R, LAT + ROPE), BF), sc=v((R, L), F32),
        ol=v((R, LAT), F32), os=v((B, HEADS * VH), BF), res=v((B, H), F32), an=v((B, H), BF),
        h0=v((B, H), BF), f0=v((B, H), BF), h1=v((B, H), BF),
        cs=v((R, ROPE), F32), sn=v((R, ROPE), F32), lm=v((R, L), F32),
        uall=v((N, B, H), BF), vall=v((N // 2, B, H), BF), fa=v((M, H), BF), ea=v((M, H), BF), act=v((M, FH), BF),
        pm=v((4, M // 2, CB), F32), ps=v((2, 4, M // 2, CB), F32), pr=v((2, 4, M // 2, CB), F32),
        bs=v((2, TP, 4, B, CB), BF), br=v((2, TP, 4, B, CB), BF),
        idall=v((N, B, 128), I32), ptk=v((N * B, M), BF), el=v((M, 128), F32), gsel=v((2 * 6 * B, 128), BF),
        racc=v((M, H), F32), rs=v((N, B, H // 2), BF), rr=v((N, B, H // 2), BF), rk=v((N * B, H // 2), BF), mm=v((B, H), F32),
        s_m=dma((8,)), s_kv=dma((B,)), s_uk=dma((2,)), s_gu=dma((2, 6, 2)), s_wd=dma((2, 4)),
        us=dma((16,)), ur=dma((N,)), vs=dma((8,)), vr=dma((N // 2,)),
        pss=dma((2, 4)), psr=dma((2, 4)), bss=dma((2, TP, 4)), bsr=dma((2, TP, 4)),
        ids_s=dma((N,)), ids_r=dma((N,)), ret_s=dma((N,)), ret_r=dma((N,)),
    )


def rms(v):
    vf = v.astype(F32)
    return (vf * lax.rsqrt(jnp.mean(vf * vf, axis=-1, keepdims=True) + 1e-6)).astype(BF)


def dot(a, b):
    return jnp.dot(a, b, preferred_element_type=F32)


def kernel(names, x_in, lens_in, ids_in, wts_in, table_in, kv0, kv1, wq, wuk, wuv, wo, w_in, w_out, e_in, e_out, y, *scr):
    s = types.SimpleNamespace(**dict(zip(names, scr)))
    z = lax.axis_index('tp')
    e = lax.axis_index('ep')
    me = z * 4 + e
    c = lax.rem(e, 2)
    pe = e + 1 - 2 * c
    ye = lax.rem(e + 2, 4)
    ype = lax.rem(pe + 2, 4)
    kvs = (kv0, kv1)
    x, lens, ids, wts, table = s.x, s.lens, s.ids, s.wts, s.table
    small = [pltpu.make_async_copy(a, b, s.s_in.at[i]) for i, (a, b) in enumerate(
        ((x_in, x), (lens_in, lens), (table_in, table), (ids_in, ids), (wts_in, wts)))]
    sends = []

    barrier = pltpu.get_barrier_semaphore()
    others = []
    for i in range(1, N):
        zz, ee = lax.rem(z + i // 4, 4), lax.rem(e + i % 4, 4)
        others.append((i, zz * 4 + ee, zz, ee))
    for i, g, zz, ee in others:
        pl.semaphore_signal(barrier, inc=1, device_id=(lax.axis_index('dp'), zz, ee), device_id_type=MESH)

    def cp(src, dst, sem):
        return pltpu.make_async_copy(src, dst, sem)

    def m_q(l, j):
        k = 2 * l + j
        return cp(wq.at[l, :, pl.ds(j * CB, CB)], s.mbuf.at[k], s.s_m.at[k])

    def m_o(l, j):
        k = (2 * l + 6 + j) % 8
        return cp(wo.at[l, :, pl.ds(j * CB, CB)], s.mbuf.at[k], s.s_m.at[k])

    def c_kv(l, t):
        return cp(kvs[l].at[t], s.kvb.at[t], s.s_kv.at[t])

    def c_uk(l):
        return cp(wuk.at[l], s.wukb, s.s_uk.at[0])

    def c_uv(l):
        return cp(wuv.at[l], s.wuvb, s.s_uk.at[1])

    def u_gu(what, i, k, j, w, half):
        o = pl.multiple_of(j * 256, 128)
        if what == 'ffn':
            src = w_in.at[i, half, :, pl.ds(pl.multiple_of(c * FH + o, 128), w)]
        else:
            src = e_in.at[i, :, pl.ds(pl.multiple_of(half * FH + o, 128), w)]
        dst = s.gu5.at[k, j, :, pl.ds(half * w, w)] if w == 256 else s.gu1.at[k, :, pl.ds(half * w, w)]
        return cp(src, dst, s.s_gu.at[k, j, half])

    def u_wd(what, i, k, j):
        cols = pl.ds(pl.multiple_of(j * CB, CB), CB)
        if what == 'ffn':
            src = w_out.at[i, pl.ds(pl.multiple_of(c * FH, 128), FH), cols]
        else:
            src = e_out.at[i, :, cols]
        return cp(src, s.wd.at[k, j], s.s_wd.at[k, j])

    def u_start(what, i, k):
        def gu(j, _):
            u_gu(what, i, k, j, 256, 0).start()
            u_gu(what, i, k, j, 256, 1).start()
            return 0

        lax.fori_loop(0, 5, gu, 0)
        u_gu(what, i, k, 5, 128, 0).start()
        u_gu(what, i, k, 5, 128, 1).start()

        def dn(j, _):
            u_wd(what, i, k, j).start()
            return 0

        lax.fori_loop(0, 4, dn, 0)

    def rc(src, dst, ss, rs, tp, ep):
        return pltpu.make_async_remote_copy(src_ref=src, dst_ref=dst, send_sem=ss, recv_sem=rs,
                                            device_id=(lax.axis_index('dp'), tp, ep), device_id_type=MESH)

    def send(*a):
        d = rc(*a)
        d.start()
        sends.append(d)

    for d in small:
        d.start()
    m_q(0, 0).start()
    m_q(0, 1).start()
    for d in small:
        d.wait()
    for j in range(2, 6):
        m_q(0, j).start()
    for t in range(B):
        c_kv(0, t).start()
    c_uk(0).start()
    c_uv(0).start()
    m_o(0, 0).start()
    m_o(0, 1).start()

    def positions():
        with jax.named_scope('positions'):
            return positions_()

    def positions_():
        diag = lax.broadcasted_iota(I32, (B, B), 0) == lax.broadcasted_iota(I32, (B, B), 1)
        lrow = jnp.broadcast_to(lens[...].astype(F32).reshape(1, B), (B, B))
        lv = jnp.broadcast_to(jnp.sum(jnp.where(diag, lrow, 0.0), axis=1, keepdims=True), (B, L))
        at = jnp.where(lax.broadcasted_iota(I32, (B, L), 1).astype(F32) == lv - 1.0, 1.0, 0.0).astype(BF)
        tb = dot(at, table[...])
        tb = tb[:, :128] + tb[:, 128:256] + tb[:, 256:]
        s.cs[...] = jnp.concatenate([tb[:, :ROPE]] * HEADS, axis=0)
        s.sn[...] = jnp.concatenate([tb[:, ROPE:]] * HEADS, axis=0)
        s.lm[...] = jnp.concatenate([lv] * HEADS, axis=0)

    rowt = lax.broadcasted_iota(I32, (R, L), 0) & (B - 1)

    def q_steps(l, lo, hi):
        with jax.named_scope(f'q_steps{l}'):
            return q_steps_(l, lo, hi)

    def q_steps_(l, lo, hi):
        for j in range(lo, hi):
            m_q(l, j).wait()
        for j in range(lo, hi):
            s.qs[:, j * CB:(j + 1) * CB] = dot(s.an[...], s.mbuf[2 * l + j])

    def mla(l, after_two, after_q, after_uk, after_kv, after_uv):
        q_steps(l, 0, 2)
        after_two()
        if l == 0:
            q_steps(l, 2, 4)
            q_steps(l, 4, 6)
        else:
            q_steps(l, 2, 6)
        after_q()
        latent_q(l)
        after_uk()
        attend(l)
        after_kv()
        values(l)
        after_uv()
        project(l)

    def latent_q(l):
        with jax.named_scope(f'latent_q{l}'):
            return latent_q_(l)

    def latent_q_(l):
        c_uk(l).wait()
        D = NOPE + ROPE
        rope = []
        for hp in range(HEADS // 2):
            pair = []
            for k in range(2):
                h = 2 * hp + k
                qn = s.qs[:, h * D:h * D + NOPE].astype(BF)
                pair.append(dot(qn, s.wukb[h]))
                rope.append(s.qs[:, h * D + NOPE:(h + 1) * D])
            s.qc[hp * 16:(hp + 1) * 16, :LAT] = jnp.concatenate(pair, axis=0).astype(BF)
        r = jnp.concatenate(rope, axis=0)
        rot = jnp.concatenate([r[:, ROPE // 2:], r[:, :ROPE // 2]], axis=1)
        s.qc[:, LAT:] = (r * s.cs[...] + rot * s.sn[...]).astype(BF)

    def attend(l):
        with jax.named_scope(f'attend{l}'):
            return attend_(l)

    def attend_(l):
        for t in range(B):
            c_kv(l, t).wait()
        for t in range(B):
            st = dot(s.qc[...], s.kvb[t])
            if t == 0:
                s.sc[...] = st
            else:
                s.sc[...] = jnp.where(rowt == t, st, s.sc[...])
        sc = jnp.where(lax.broadcasted_iota(I32, (R, L), 1).astype(F32) < s.lm[...], s.sc[...] * SCALE, -1e30)
        ex = jnp.exp(sc - jnp.max(sc, axis=-1, keepdims=True))
        p = ex / jnp.sum(ex, axis=-1, keepdims=True)
        ol = None
        for t in range(B):
            pt = jnp.where(rowt == t, p, 0.0).astype(BF)
            ot = lax.dot_general(pt, s.kvb[t, :LAT, :], (((1,), (1,)), ((), ())), preferred_element_type=F32)
            ol = ot if ol is None else ol + ot
        s.ol[...] = ol

    def values(l):
        with jax.named_scope(f'values{l}'):
            return values_(l)

    def values_(l):
        c_uv(l).wait()
        for h in range(HEADS):
            o = dot(s.ol[h * B:(h + 1) * B, :].astype(BF), s.wuvb[h])
            s.os[:, h * VH:(h + 1) * VH] = o.astype(BF)

    def project(l):
        with jax.named_scope(f'project{l}'):
            return project_(l)

    def project_(l):
        for j in range(4):
            m_o(l, j).wait()
        for j in range(4):
            s.res[:, j * CB:(j + 1) * CB] = dot(s.os[...], s.mbuf[(2 * l + 6 + j) % 8])

    def unit(what, i, k, lhs, down_groups, down, between):
        def silu(g, u):
            return (g / (1.0 + jnp.exp(-g)) * u).astype(BF)

        for group in ((0, 1, 2), (3, 4, 5)):
            for j in group:
                w = 256 if j < 5 else 128
                u_gu(what, i, k, j, w, 0).wait()
                u_gu(what, i, k, j, w, 1).wait()
            for j in group:
                w = 256 if j < 5 else 128
                r = dot(lhs[...], s.gu5[k, j] if j < 5 else s.gu1[k])
                s.act[:, j * 256:j * 256 + w] = silu(r[:, :w], r[:, w:])
        between()
        for group in down_groups:
            for j in group:
                u_wd(what, i, k, j).wait()
            down(group, lambda j: dot(s.act[...], s.wd[k, j]))

    def gather_start(buf, ss, rs, at, on_y):
        with jax.named_scope('gather_start'):
            return gather_start_(buf, ss, rs, at, on_y)

    def gather_start_(buf, ss, rs, at, on_y):
        own = at(z, e)
        for k in ALONG:
            send(buf.at[own], buf.at[own], ss.at[k - 1], rs.at[own], lax.rem(z + k, TP), e)
        send(buf.at[own], buf.at[own], ss.at[3], rs.at[own], z, pe)
        if on_y:
            send(buf.at[own], buf.at[own], ss.at[8], rs.at[own], z, ye)

    def gather_pass(buf, ss, rs, at, on_y):
        with jax.named_scope('gather_pass'):
            return gather_pass_(buf, ss, rs, at, on_y)

    def gather_pass_(buf, ss, rs, at, on_y):
        for k in ALONG:
            g = at(lax.rem(z + k, TP), e)
            rc(buf.at[g], buf.at[g], ss.at[3 + k], rs.at[g], z, pe).wait_recv()
            send(buf.at[g], buf.at[g], ss.at[3 + k], rs.at[g], z, pe)
            if on_y:
                send(buf.at[g], buf.at[g], ss.at[8 + k], rs.at[g], z, ye)

    def gather_wait(buf, ss, rs, at):
        with jax.named_scope('gather_wait'):
            return gather_wait_(buf, ss, rs, at)

    def gather_wait_(buf, ss, rs, at):
        for zz in range(TP):
            g = at(zz, pe)
            rc(buf.at[g], buf.at[g], ss.at[0], rs.at[g], z, pe).wait_recv()

    def stack(buf, at):
        with jax.named_scope('stack'):
            return stack_(buf, at)

    def stack_(buf, at):
        for i, ee in enumerate((e, pe)):
            for q in range(2):
                s.fa[i * 32 + q * 16:i * 32 + q * 16 + 16, :] = jnp.concatenate([buf[at(2 * q, ee)], buf[at(2 * q + 1, ee)]], axis=0)

    def ffn(l, k, between):
        with jax.named_scope(f'ffn{l}'):
            return ffn_(l, k, between)

    def ffn_(l, k, between):
        def down(group, product):
            for j in group:
                r = product(j)
                s.pm[j] = r[:M // 2]
                s.ps[l, j] = r[M // 2:]
            for j in group:
                rc(s.ps.at[l, j], s.pr.at[l, j], s.pss.at[l, j], s.psr.at[l, j], z, pe).start()

        unit('ffn', l, k, s.fa, ((0, 1), (2, 3)), down, between)

    def ffn_send(l):
        with jax.named_scope(f'ffn_send{l}'):
            return ffn_send_(l)

    def ffn_send_(l):
        for j in range(4):
            rc(s.ps.at[l, j], s.pr.at[l, j], s.pss.at[l, j], s.psr.at[l, j], z, pe).wait()
            tot = s.pm[j] + s.pr[l, j]
            for q in range(TP):
                s.bs[l, q, j] = tot[q * B:(q + 1) * B].astype(BF)
            for k in ALONG:
                zz = lax.rem(z + k, TP)
                send(s.bs.at[l, zz, j], s.br.at[l, z, j], s.bss.at[l, k, j], s.bsr.at[l, z, j], zz, e)
            s.br[l, z, j] = s.bs[l, z, j]

    def ffn_recv(l):
        with jax.named_scope(f'ffn_recv{l}'):
            return ffn_recv_(l)

    def ffn_recv_(l):
        for j in range(4):
            for k in ALONG:
                zz = lax.rem(z + k, TP)
                rc(s.bs.at[l, zz, j], s.br.at[l, zz, j], s.bss.at[l, k, j], s.bsr.at[l, zz, j], zz, e).wait_recv()
            acc = s.br[l, 0, j].astype(F32)
            for q in range(1, TP):
                acc = acc + s.br[l, q, j].astype(F32)
            s.res[:, j * CB:(j + 1) * CB] = acc
        return s.res[...]

    def at16(zz, ee):
        return zz * 4 + ee

    def at8(zz, ee):
        return zz * 2 + lax.rem(ee, 2)

    def send_ids():
        with jax.named_scope('send_ids'):
            return send_ids_()

    def send_ids_():
        s.idall[me] = jnp.full((B, 128), -1, I32)
        s.idall[me, :, 0:6] = ids[...]
        pl.semaphore_wait(barrier, N - 1)
        for i, g, zz, ee in others:
            send(s.idall.at[me], s.idall.at[me], s.ids_s.at[i], s.ids_r.at[me], zz, ee)

    def slots_here():
        with jax.named_scope('slots_here'):
            return slots_here_()

    def slots_here_():
        lane = lax.broadcasted_iota(I32, (B, 128), 1)
        mine = s.idall[me]
        dst = [jnp.broadcast_to(mine[:, j:j + 1], (B, 128)) >> 2 for j in range(6)]
        hot = [jnp.where(d == lane, 1.0, 0.0) for d in dst]
        cnt = functools.reduce(jnp.add, hot)
        row = lax.broadcasted_iota(I32, (B, 128), 0)
        run = jnp.zeros((B, 128), F32)
        for t in range(B - 1):
            run = run + jnp.where(row > t, jnp.broadcast_to(cnt[t:t + 1], (B, 128)), 0.0)
        left, right = [], []
        for j in range(6):
            pos = jnp.sum(hot[j] * run, axis=1, keepdims=True)
            run = run + hot[j]
            col = dst[j].astype(F32) * B + pos
            left.append(jnp.where(col == lane.astype(F32), 1.0, 0.0))
            right.append(jnp.where(col + 4.0 == lane.astype(F32), 1.0, 0.0))
        s.gsel[...] = jnp.concatenate(left + right, axis=0).astype(BF)

    def slots_there():
        with jax.named_scope('slots_there'):
            return slots_there_()

    def slots_there_():
        for i, g, zz, ee in others:
            rc(s.idall.at[g], s.idall.at[g], s.ids_s.at[i], s.ids_r.at[g], z, pe).wait_recv()
        T = N * B
        idt = jnp.concatenate([s.idall[d] for d in range(N)], axis=0)
        lane = lax.broadcasted_iota(I32, (T, 128), 1)
        tok = lax.broadcasted_iota(I32, (T, 128), 0)
        col = [jnp.broadcast_to(idt[:, j:j + 1], (T, 128)) for j in range(6)]
        hit = [jnp.where((v >> 2) == me, 1.0, 0.0) for v in col]
        before = jnp.where((tok >> 3 == lane >> 3) & (lane < tok), 1.0, 0.0)
        run = dot(before.astype(BF), functools.reduce(jnp.add, hit).astype(BF)) + ((tok >> 3) * 4).astype(F32)
        pt = jnp.zeros((T, 128), F32)
        ex = jnp.zeros((T, 128), F32)
        for j in range(6):
            at = jnp.where(run == lane.astype(F32), hit[j], 0.0)
            pt = pt + at
            ex = ex + at * (col[j] & 3).astype(F32)
            run = run + hit[j]
        s.ptk[...] = pt[:, :M].astype(BF)
        s.el[...] = lax.dot_general(ex[:, :M].astype(BF), jnp.ones((T, 128), BF), (((0,), (0,)), ((), ())),
                                    preferred_element_type=F32)

    def expert(i, k, between):
        with jax.named_scope(f'expert{i}'):
            return expert_(i, k, between)

    def expert_(i, k, between):
        def down(group, product):
            for j in group:
                cols = pl.ds(j * CB, CB)
                r = product(j).astype(BF).astype(F32)
                if i == 0:
                    s.racc[:, cols] = r
                else:
                    keep = jnp.broadcast_to(s.el[:, 0:1], (M, CB)) == float(i)
                    s.racc[:, cols] = jnp.where(keep, r, s.racc[:, cols])

        unit('moe', i, k, s.ea, ((0, 1, 2, 3),), down, between)

    def give_back():
        with jax.named_scope('give_back'):
            return give_back_()

    def give_back_():
        for d in range(N):
            a = s.racc[4 * d:4 * d + 4, :]
            s.rs[d] = jnp.concatenate([a[:, :H // 2], a[:, H // 2:]], axis=0).astype(BF)
        for i, g, zz, ee in others:
            send(s.rs.at[g], s.rr.at[me], s.ret_s.at[i], s.ret_r.at[me], zz, ee)
        s.rr[me] = s.rs[me]

    def take_back():
        with jax.named_scope('take_back'):
            return take_back_()

    def take_back_():
        for i, g, zz, ee in others:
            rc(s.rs.at[g], s.rr.at[g], s.ret_s.at[i], s.ret_r.at[g], z, pe).wait_recv()
        for d in range(N // 2):
            s.rk[d * 16:(d + 1) * 16, :] = jnp.concatenate([s.rr[2 * d], s.rr[2 * d + 1]], axis=0)
        got = dot(s.gsel[...], s.rk[...])
        for half in range(2):
            acc = None
            for j in range(6):
                o = (half * 6 + j) * B
                term = wts[:, j:j + 1] * got[o:o + B]
                acc = term if acc is None else acc + term
            s.mm[:, half * (H // 2):(half + 1) * (H // 2)] = acc

    nothing = lambda: None

    s.an[...] = rms(x[...])

    def two0():
        m_o(0, 2).start()
        m_o(0, 3).start()
        u_start('ffn', 0, 0)
        u_start('moe', 0, 1)
        positions()

    def q0():
        for j in range(4):
            m_q(1, j).start()

    def kv0_done():
        for t in range(B):
            c_kv(1, t).start()

    def uk0():
        c_uk(1).start()
        send_ids()

    mla(0, two0, q0, uk0, kv0_done, lambda: c_uv(1).start())
    for j in (4, 5):
        m_q(1, j).start()
    for j in (0, 1):
        m_o(1, j).start()
    h0 = (x[...].astype(F32) + s.res[...]).astype(BF)
    s.h0[...] = h0
    s.uall[me] = rms(h0)
    gather_start(s.uall, s.us, s.ur, at16, True)
    slots_here()
    gather_pass(s.uall, s.us, s.ur, at16, True)
    gather_wait(s.uall, s.us, s.ur, at16)
    stack(s.uall, at16)
    ffn(0, 0, nothing)
    u_start('moe', 1, 0)
    slots_there()
    for zz in range(TP):
        g = at16(zz, ye)
        rc(s.uall.at[g], s.uall.at[g], s.us.at[12 + zz], s.ur.at[g], z, pe).wait_recv()
        send(s.uall.at[g], s.uall.at[g], s.us.at[12 + zz], s.ur.at[g], z, pe)
    ffn_send(0)
    for zz in range(TP):
        g = at16(zz, ype)
        rc(s.uall.at[g], s.uall.at[g], s.us.at[12 + zz], s.ur.at[g], z, pe).wait_recv()
    for half in range(2):
        cols = pl.ds(half * (H // 2), H // 2)
        for d in range(N // 2):
            s.rk[d * 16:(d + 1) * 16, :] = jnp.concatenate([s.uall[2 * d, :, cols], s.uall[2 * d + 1, :, cols]], axis=0)
        s.ea[:, cols] = lax.dot_general(s.ptk[...], s.rk[...], (((0,), (0,)), ((), ())),
                                        preferred_element_type=F32).astype(BF)
    expert(0, 1, nothing)
    f0 = (s.h0[...].astype(F32) + ffn_recv(0)).astype(BF)
    s.f0[...] = f0
    s.an[...] = rms(f0)

    def two1():
        m_o(1, 2).start()
        m_o(1, 3).start()
        u_start('moe', 2, 1)

    mla(1, two1, nothing, nothing, nothing, nothing)
    h1 = (s.f0[...].astype(F32) + s.res[...]).astype(BF)
    s.h1[...] = h1
    s.vall[at8(z, e)] = rms(h1)
    gather_start(s.vall, s.vs, s.vr, at8, False)
    expert(1, 0, lambda: gather_pass(s.vall, s.vs, s.vr, at8, False))
    u_start('moe', 3, 0)
    expert(2, 1, nothing)
    u_start('ffn', 1, 1)
    expert(3, 0, nothing)
    give_back()
    gather_wait(s.vall, s.vs, s.vr, at8)
    stack(s.vall, at8)
    ffn(1, 1, nothing)
    ffn_send(1)
    take_back()
    y[...] = (s.h1[...].astype(F32) + ffn_recv(1) + s.mm[...]).astype(BF)
    for d in sends:
        d.wait_send()


def rope_table():
    half = ROPE // 2
    f = np.float32(10000.0) ** (np.float32(-2.0) * np.arange(half, dtype=np.float32) / np.float32(ROPE))
    ang = np.arange(1, L + 1, dtype=np.float32)[:, None] * f.astype(np.float32)
    cs, sn = np.cos(ang.astype(np.float64)), np.sin(ang.astype(np.float64))
    left = np.concatenate([cs, cs, -sn, sn], axis=1).astype(np.float32)
    parts = []
    for _ in range(3):
        part = left.astype(jnp.bfloat16)
        parts.append(part)
        left = left - part.astype(np.float32)
    return jnp.asarray(np.concatenate(parts, axis=1))


def layer(x, kv0, kv1, lens, ids, wts, wq, wuk, wuv, wo, w_in, w_out, e_in, e_out):
    table = rope_table()
    sc = scratch()
    vm = pl.BlockSpec(memory_space=pltpu.VMEM)
    hbm = pl.BlockSpec(memory_space=pl.ANY)
    return pl.pallas_call(
        functools.partial(kernel, tuple(sc)),
        out_shape=jax.ShapeDtypeStruct((B, H), BF),
        in_specs=[hbm] * 15,
        out_specs=vm,
        scratch_shapes=list(sc.values()),
        compiler_params=pltpu.CompilerParams(collective_id=0, has_side_effects=True, vmem_limit_bytes=67043328),
    )(x, lens, ids, wts, table, jnp.swapaxes(kv0, 1, 2), jnp.swapaxes(kv1, 1, 2), wq, wuk, wuv, wo, w_in, w_out, e_in, e_out)


def solution(mesh):
    in_specs = (P(BATCH, None), P(BATCH, None, None), P(BATCH, None, None), P(BATCH), P(BATCH, None), P(BATCH, None),
                P(), P(), P(), P(), P(None, None, None, 'tp'), P(None, 'tp', None), P(GROUP, None, None), P(GROUP, None, None))
    return jax.shard_map(layer, mesh=mesh, in_specs=in_specs, out_specs=P(BATCH, None), check_vma=False)
```

```python
import functools
import types

import jax
import jax.numpy as jnp
import numpy as np
from jax import lax
from jax.experimental import pallas as pl
from jax.experimental.pallas import tpu as pltpu
from jax.sharding import PartitionSpec as P

BATCH = ('dp', 'tp', 'ep')
GROUP = ('tp', 'ep')
MESH = pl.DeviceIdType.MESH
BF = jnp.bfloat16
F32 = jnp.float32
I32 = jnp.int32

B = 8
H = 2048
HEADS = 16
NOPE = 128
ROPE = 64
LAT = 512
VH = 128
L = 256
FH = 1408
TP = 4
N = 16
R = HEADS * B
M = 64
CB = 512
SCALE = (NOPE + ROPE) ** -0.5

ALONG = (1, 3, 2)


def scratch():
    dma = pltpu.SemaphoreType.DMA
    v = pltpu.VMEM
    return dict(
        x=v((B, H), BF), lens=v((B,), I32), ids=v((B, 6), I32), wts=v((B, 6), F32), table=v((L, 384), BF), s_in=dma((5,)),
        mbuf=v((8, H, CB), BF), wukb=v((HEADS, NOPE, LAT), BF), wuvb=v((HEADS, LAT, VH), BF), kvb=v((B, LAT + ROPE, L), BF),
        gu5=v((2, 5, H, CB), BF), gu1=v((2, H, CB // 2), BF), wd=v((2, 4, FH, CB), BF),
        qs=v((B, HEADS * (NOPE + ROPE)), F32), qc=v((R, LAT + ROPE), BF), sc=v((R, L), F32),
        ol=v((R, LAT), F32), os=v((B, HEADS * VH), BF), res=v((B, H), F32), an=v((B, H), BF),
        h0=v((B, H), BF), f0=v((B, H), BF), h1=v((B, H), BF),
        cs=v((R, ROPE), F32), sn=v((R, ROPE), F32), lm=v((R, L), F32),
        uall=v((N, B, H), BF), vall=v((N // 2, B, H), BF), fa=v((M, H), BF), ea=v((M, H), BF), act=v((M, FH), BF),
        pm=v((4, M // 2, CB), F32), ps=v((2, 4, M // 2, CB), F32), pr=v((2, 4, M // 2, CB), F32),
        bs=v((2, TP, 4, B, CB), BF), br=v((2, TP, 4, B, CB), BF),
        idall=v((N, B, 128), I32), ptk=v((N * B, M), BF), el=v((M, 128), F32), gsel=v((2 * 6 * B, 128), BF),
        racc=v((M, H), F32), rs=v((N, B, H // 2), BF), rr=v((N, B, H // 2), BF), rk=v((N * B, H // 2), BF), mm=v((B, H), F32),
        s_m=dma((8,)), s_kv=dma((B,)), s_uk=dma((2,)), s_gu=dma((2, 6, 2)), s_wd=dma((2, 4)),
        us=dma((16,)), ur=dma((N,)), vs=dma((8,)), vr=dma((N // 2,)),
        pss=dma((2, 4)), psr=dma((2, 4)), bss=dma((2, TP, 4)), bsr=dma((2, TP, 4)),
        ids_s=dma((N,)), ids_r=dma((N,)), ret_s=dma((N,)), ret_r=dma((N,)),
    )


def rms(v):
    vf = v.astype(F32)
    return (vf * lax.rsqrt(jnp.mean(vf * vf, axis=-1, keepdims=True) + 1e-6)).astype(BF)


def dot(a, b):
    return jnp.dot(a, b, preferred_element_type=F32)


def kernel(names, x_in, lens_in, ids_in, wts_in, table_in, kv0, kv1, wq, wuk, wuv, wo, w_in, w_out, e_in, e_out, y, *scr):
    s = types.SimpleNamespace(**dict(zip(names, scr)))
    z = lax.axis_index('tp')
    e = lax.axis_index('ep')
    me = z * 4 + e
    c = lax.rem(e, 2)
    pe = e + 1 - 2 * c
    ye = lax.rem(e + 2, 4)
    ype = lax.rem(pe + 2, 4)
    kvs = (kv0, kv1)
    x, lens, ids, wts, table = s.x, s.lens, s.ids, s.wts, s.table
    small = [pltpu.make_async_copy(a, b, s.s_in.at[i]) for i, (a, b) in enumerate(
        ((x_in, x), (lens_in, lens), (table_in, table), (ids_in, ids), (wts_in, wts)))]
    sends = []

    barrier = pltpu.get_barrier_semaphore()
    others = []
    for i in range(1, N):
        zz, ee = lax.rem(z + i // 4, 4), lax.rem(e + i % 4, 4)
        others.append((i, zz * 4 + ee, zz, ee))
    for i, g, zz, ee in others:
        pl.semaphore_signal(barrier, inc=1, device_id=(lax.axis_index('dp'), zz, ee), device_id_type=MESH)

    def cp(src, dst, sem):
        return pltpu.make_async_copy(src, dst, sem)

    def m_q(l, j):
        k = 2 * l + j
        return cp(wq.at[l, :, pl.ds(j * CB, CB)], s.mbuf.at[k], s.s_m.at[k])

    def m_o(l, j):
        k = (2 * l + 6 + j) % 8
        return cp(wo.at[l, :, pl.ds(j * CB, CB)], s.mbuf.at[k], s.s_m.at[k])

    def c_kv(l, t):
        return cp(kvs[l].at[t], s.kvb.at[t], s.s_kv.at[t])

    def c_uk(l):
        return cp(wuk.at[l], s.wukb, s.s_uk.at[0])

    def c_uv(l):
        return cp(wuv.at[l], s.wuvb, s.s_uk.at[1])

    def u_gu(what, i, k, j, w, half):
        o = pl.multiple_of(j * 256, 128)
        if what == 'ffn':
            src = w_in.at[i, half, :, pl.ds(pl.multiple_of(c * FH + o, 128), w)]
        else:
            src = e_in.at[i, :, pl.ds(pl.multiple_of(half * FH + o, 128), w)]
        dst = s.gu5.at[k, j, :, pl.ds(half * w, w)] if w == 256 else s.gu1.at[k, :, pl.ds(half * w, w)]
        return cp(src, dst, s.s_gu.at[k, j, half])

    def u_wd(what, i, k, j):
        cols = pl.ds(pl.multiple_of(j * CB, CB), CB)
        if what == 'ffn':
            src = w_out.at[i, pl.ds(pl.multiple_of(c * FH, 128), FH), cols]
        else:
            src = e_out.at[i, :, cols]
        return cp(src, s.wd.at[k, j], s.s_wd.at[k, j])

    def u_start(what, i, k):
        def gu(j, _):
            u_gu(what, i, k, j, 256, 0).start()
            u_gu(what, i, k, j, 256, 1).start()
            return 0

        lax.fori_loop(0, 5, gu, 0)
        u_gu(what, i, k, 5, 128, 0).start()
        u_gu(what, i, k, 5, 128, 1).start()

        def dn(j, _):
            u_wd(what, i, k, j).start()
            return 0

        lax.fori_loop(0, 4, dn, 0)

    def rc(src, dst, ss, rs, tp, ep):
        return pltpu.make_async_remote_copy(src_ref=src, dst_ref=dst, send_sem=ss, recv_sem=rs,
                                            device_id=(lax.axis_index('dp'), tp, ep), device_id_type=MESH)

    def send(*a):
        d = rc(*a)
        d.start()
        sends.append(d)

    for d in small:
        d.start()
    m_q(0, 0).start()
    m_q(0, 1).start()
    for d in small:
        d.wait()
    for j in range(2, 6):
        m_q(0, j).start()
    for t in range(B):
        c_kv(0, t).start()
    c_uk(0).start()
    c_uv(0).start()
    m_o(0, 0).start()
    m_o(0, 1).start()

    def positions():
        with jax.named_scope('positions'):
            return positions_()

    def positions_():
        diag = lax.broadcasted_iota(I32, (B, B), 0) == lax.broadcasted_iota(I32, (B, B), 1)
        lrow = jnp.broadcast_to(lens[...].astype(F32).reshape(1, B), (B, B))
        lv = jnp.broadcast_to(jnp.sum(jnp.where(diag, lrow, 0.0), axis=1, keepdims=True), (B, L))
        at = jnp.where(lax.broadcasted_iota(I32, (B, L), 1).astype(F32) == lv - 1.0, 1.0, 0.0).astype(BF)
        tb = dot(at, table[...])
        tb = tb[:, :128] + tb[:, 128:256] + tb[:, 256:]
        s.cs[...] = jnp.concatenate([tb[:, :ROPE]] * HEADS, axis=0)
        s.sn[...] = jnp.concatenate([tb[:, ROPE:]] * HEADS, axis=0)
        s.lm[...] = jnp.concatenate([lv] * HEADS, axis=0)

    rowt = lax.broadcasted_iota(I32, (R, L), 0) & (B - 1)

    def q_steps(l, lo, hi):
        with jax.named_scope(f'q_steps{l}'):
            return q_steps_(l, lo, hi)

    def q_steps_(l, lo, hi):
        for j in range(lo, hi):
            m_q(l, j).wait()
        for j in range(lo, hi):
            s.qs[:, j * CB:(j + 1) * CB] = dot(s.an[...], s.mbuf[2 * l + j])

    def mla(l, after_two, after_q, after_uk, after_kv, after_uv):
        q_steps(l, 0, 2)
        after_two()
        if l == 0:
            q_steps(l, 2, 4)
            q_steps(l, 4, 6)
        else:
            q_steps(l, 2, 6)
        after_q()
        latent_q(l)
        after_uk()
        attend(l)
        after_kv()
        values(l)
        after_uv()
        project(l)

    def latent_q(l):
        with jax.named_scope(f'latent_q{l}'):
            return latent_q_(l)

    def latent_q_(l):
        c_uk(l).wait()
        D = NOPE + ROPE
        rope = []
        for hp in range(HEADS // 2):
            pair = []
            for k in range(2):
                h = 2 * hp + k
                qn = s.qs[:, h * D:h * D + NOPE].astype(BF)
                pair.append(dot(qn, s.wukb[h]))
                rope.append(s.qs[:, h * D + NOPE:(h + 1) * D])
            s.qc[hp * 16:(hp + 1) * 16, :LAT] = jnp.concatenate(pair, axis=0).astype(BF)
        r = jnp.concatenate(rope, axis=0)
        rot = jnp.concatenate([r[:, ROPE // 2:], r[:, :ROPE // 2]], axis=1)
        s.qc[:, LAT:] = (r * s.cs[...] + rot * s.sn[...]).astype(BF)

    def attend(l):
        with jax.named_scope(f'attend{l}'):
            return attend_(l)

    def attend_(l):
        for t in range(B):
            c_kv(l, t).wait()
        for t in range(B):
            st = dot(s.qc[...], s.kvb[t])
            if t == 0:
                s.sc[...] = st
            else:
                s.sc[...] = jnp.where(rowt == t, st, s.sc[...])
        sc = jnp.where(lax.broadcasted_iota(I32, (R, L), 1).astype(F32) < s.lm[...], s.sc[...] * SCALE, -1e30)
        ex = jnp.exp(sc - jnp.max(sc, axis=-1, keepdims=True))
        p = ex / jnp.sum(ex, axis=-1, keepdims=True)
        ol = None
        for t in range(B):
            pt = jnp.where(rowt == t, p, 0.0).astype(BF)
            ot = lax.dot_general(pt, s.kvb[t, :LAT, :], (((1,), (1,)), ((), ())), preferred_element_type=F32)
            ol = ot if ol is None else ol + ot
        s.ol[...] = ol

    def values(l):
        with jax.named_scope(f'values{l}'):
            return values_(l)

    def values_(l):
        c_uv(l).wait()
        for h in range(HEADS):
            o = dot(s.ol[h * B:(h + 1) * B, :].astype(BF), s.wuvb[h])
            s.os[:, h * VH:(h + 1) * VH] = o.astype(BF)

    def project(l):
        with jax.named_scope(f'project{l}'):
            return project_(l)

    def project_(l):
        for j in range(4):
            m_o(l, j).wait()
        for j in range(4):
            s.res[:, j * CB:(j + 1) * CB] = dot(s.os[...], s.mbuf[(2 * l + 6 + j) % 8])

    def unit(what, i, k, lhs, down_groups, down, between):
        def silu(g, u):
            return (g / (1.0 + jnp.exp(-g)) * u).astype(BF)

        early = (what, i) in (('ffn', 0), ('moe', 0), ('moe', 1))
        for group in ((0, 1, 2, 3, 4, 5),) if early else ((0, 1, 2), (3, 4, 5)):
            for j in group:
                w = 256 if j < 5 else 128
                u_gu(what, i, k, j, w, 0).wait()
                u_gu(what, i, k, j, w, 1).wait()
            if early:
                for j in range(4):
                    u_wd(what, i, k, j).wait()
            for j in group:
                w = 256 if j < 5 else 128
                r = dot(lhs[...], s.gu5[k, j] if j < 5 else s.gu1[k])
                s.act[:, j * 256:j * 256 + w] = silu(r[:, :w], r[:, w:])
        between()
        for group in down_groups:
            for j in group if not early else ():
                u_wd(what, i, k, j).wait()
            down(group, lambda j: dot(s.act[...], s.wd[k, j]))

    def gather_start(buf, ss, rs, at, on_y):
        with jax.named_scope('gather_start'):
            return gather_start_(buf, ss, rs, at, on_y)

    def gather_start_(buf, ss, rs, at, on_y):
        own = at(z, e)
        for k in ALONG:
            send(buf.at[own], buf.at[own], ss.at[k - 1], rs.at[own], lax.rem(z + k, TP), e)
        send(buf.at[own], buf.at[own], ss.at[3], rs.at[own], z, pe)
        if on_y:
            send(buf.at[own], buf.at[own], ss.at[8], rs.at[own], z, ye)

    def gather_pass(buf, ss, rs, at, on_y, before_last):
        with jax.named_scope('gather_pass'):
            return gather_pass_(buf, ss, rs, at, on_y, before_last)

    def gather_pass_(buf, ss, rs, at, on_y, before_last):
        for k in ALONG:
            if k == ALONG[-1]:
                before_last()
            g = at(lax.rem(z + k, TP), e)
            rc(buf.at[g], buf.at[g], ss.at[3 + k], rs.at[g], z, pe).wait_recv()
            send(buf.at[g], buf.at[g], ss.at[3 + k], rs.at[g], z, pe)
            if on_y:
                send(buf.at[g], buf.at[g], ss.at[8 + k], rs.at[g], z, ye)

    def gather_wait(buf, ss, rs, at):
        with jax.named_scope('gather_wait'):
            return gather_wait_(buf, ss, rs, at)

    def gather_wait_(buf, ss, rs, at):
        for zz in range(TP):
            g = at(zz, pe)
            rc(buf.at[g], buf.at[g], ss.at[0], rs.at[g], z, pe).wait_recv()

    def stack(buf, at):
        with jax.named_scope('stack'):
            return stack_(buf, at)

    def stack_(buf, at):
        for i, ee in enumerate((e, pe)):
            for q in range(2):
                s.fa[i * 32 + q * 16:i * 32 + q * 16 + 16, :] = jnp.concatenate([buf[at(2 * q, ee)], buf[at(2 * q + 1, ee)]], axis=0)

    def ffn(l, k, between):
        with jax.named_scope(f'ffn{l}'):
            return ffn_(l, k, between)

    def ffn_(l, k, between):
        def down(group, product):
            for j in group:
                r = product(j)
                s.pm[j] = r[:M // 2]
                s.ps[l, j] = r[M // 2:]
            for j in group:
                rc(s.ps.at[l, j], s.pr.at[l, j], s.pss.at[l, j], s.psr.at[l, j], z, pe).start()

        unit('ffn', l, k, s.fa, ((0, 1), (2, 3)), down, between)

    def ffn_send(l):
        with jax.named_scope(f'ffn_send{l}'):
            return ffn_send_(l)

    def ffn_send_(l):
        for j in range(4):
            rc(s.ps.at[l, j], s.pr.at[l, j], s.pss.at[l, j], s.psr.at[l, j], z, pe).wait()
            tot = s.pm[j] + s.pr[l, j]
            for q in range(TP):
                s.bs[l, q, j] = tot[q * B:(q + 1) * B].astype(BF)
            for k in ALONG:
                zz = lax.rem(z + k, TP)
                send(s.bs.at[l, zz, j], s.br.at[l, z, j], s.bss.at[l, k, j], s.bsr.at[l, z, j], zz, e)
            s.br[l, z, j] = s.bs[l, z, j]

    def ffn_recv(l):
        with jax.named_scope(f'ffn_recv{l}'):
            return ffn_recv_(l)

    def ffn_recv_(l):
        for j in range(4):
            for k in ALONG:
                zz = lax.rem(z + k, TP)
                rc(s.bs.at[l, zz, j], s.br.at[l, zz, j], s.bss.at[l, k, j], s.bsr.at[l, zz, j], zz, e).wait_recv()
            acc = s.br[l, 0, j].astype(F32)
            for q in range(1, TP):
                acc = acc + s.br[l, q, j].astype(F32)
            s.res[:, j * CB:(j + 1) * CB] = acc
        return s.res[...]

    def at16(zz, ee):
        return zz * 4 + ee

    def at8(zz, ee):
        return zz * 2 + lax.rem(ee, 2)

    def send_ids():
        with jax.named_scope('send_ids'):
            return send_ids_()

    def send_ids_():
        s.idall[me] = jnp.full((B, 128), -1, I32)
        s.idall[me, :, 0:6] = ids[...]
        pl.semaphore_wait(barrier, N - 1)
        for i, g, zz, ee in others:
            send(s.idall.at[me], s.idall.at[me], s.ids_s.at[i], s.ids_r.at[me], zz, ee)

    def slots_here():
        with jax.named_scope('slots_here'):
            return slots_here_()

    def slots_here_():
        lane = lax.broadcasted_iota(I32, (B, 128), 1)
        mine = s.idall[me]
        dst = [jnp.broadcast_to(mine[:, j:j + 1], (B, 128)) >> 2 for j in range(6)]
        hot = [jnp.where(d == lane, 1.0, 0.0) for d in dst]
        cnt = functools.reduce(jnp.add, hot)
        row = lax.broadcasted_iota(I32, (B, 128), 0)
        run = jnp.zeros((B, 128), F32)
        for t in range(B - 1):
            run = run + jnp.where(row > t, jnp.broadcast_to(cnt[t:t + 1], (B, 128)), 0.0)
        left, right = [], []
        for j in range(6):
            pos = jnp.sum(hot[j] * run, axis=1, keepdims=True)
            run = run + hot[j]
            col = dst[j].astype(F32) * B + pos
            left.append(jnp.where(col == lane.astype(F32), 1.0, 0.0))
            right.append(jnp.where(col + 4.0 == lane.astype(F32), 1.0, 0.0))
        s.gsel[...] = jnp.concatenate(left + right, axis=0).astype(BF)

    def slots_there():
        with jax.named_scope('slots_there'):
            return slots_there_()

    def slots_there_():
        for i, g, zz, ee in others:
            rc(s.idall.at[g], s.idall.at[g], s.ids_s.at[i], s.ids_r.at[g], z, pe).wait_recv()
        T = N * B
        idt = jnp.concatenate([s.idall[d] for d in range(N)], axis=0)
        lane = lax.broadcasted_iota(I32, (T, 128), 1)
        tok = lax.broadcasted_iota(I32, (T, 128), 0)
        col = [jnp.broadcast_to(idt[:, j:j + 1], (T, 128)) for j in range(6)]
        hit = [jnp.where((v >> 2) == me, 1.0, 0.0) for v in col]
        before = jnp.where((tok >> 3 == lane >> 3) & (lane < tok), 1.0, 0.0)
        run = dot(before.astype(BF), functools.reduce(jnp.add, hit).astype(BF)) + ((tok >> 3) * 4).astype(F32)
        pt = jnp.zeros((T, 128), F32)
        ex = jnp.zeros((T, 128), F32)
        for j in range(6):
            at = jnp.where(run == lane.astype(F32), hit[j], 0.0)
            pt = pt + at
            ex = ex + at * (col[j] & 3).astype(F32)
            run = run + hit[j]
        s.ptk[...] = pt[:, :M].astype(BF)
        s.el[...] = lax.dot_general(ex[:, :M].astype(BF), jnp.ones((T, 128), BF), (((0,), (0,)), ((), ())),
                                    preferred_element_type=F32)

    def expert(i, k, between):
        with jax.named_scope(f'expert{i}'):
            return expert_(i, k, between)

    def expert_(i, k, between):
        def down(group, product):
            for j in group:
                cols = pl.ds(j * CB, CB)
                r = product(j).astype(BF).astype(F32)
                if i == 0:
                    s.racc[:, cols] = r
                else:
                    keep = jnp.broadcast_to(s.el[:, 0:1], (M, CB)) == float(i)
                    s.racc[:, cols] = jnp.where(keep, r, s.racc[:, cols])

        unit('moe', i, k, s.ea, ((0, 1, 2, 3),), down, between)

    def give_back():
        with jax.named_scope('give_back'):
            return give_back_()

    def give_back_():
        for d in range(N):
            a = s.racc[4 * d:4 * d + 4, :]
            s.rs[d] = jnp.concatenate([a[:, :H // 2], a[:, H // 2:]], axis=0).astype(BF)
        for i, g, zz, ee in others:
            send(s.rs.at[g], s.rr.at[me], s.ret_s.at[i], s.ret_r.at[me], zz, ee)
        s.rr[me] = s.rs[me]

    def take_back():
        with jax.named_scope('take_back'):
            return take_back_()

    def take_back_():
        for i, g, zz, ee in others:
            rc(s.rs.at[g], s.rr.at[g], s.ret_s.at[i], s.ret_r.at[g], z, pe).wait_recv()
        for d in range(N // 2):
            s.rk[d * 16:(d + 1) * 16, :] = jnp.concatenate([s.rr[2 * d], s.rr[2 * d + 1]], axis=0)
        got = dot(s.gsel[...], s.rk[...])
        for half in range(2):
            acc = None
            for j in range(6):
                o = (half * 6 + j) * B
                term = wts[:, j:j + 1] * got[o:o + B]
                acc = term if acc is None else acc + term
            s.mm[:, half * (H // 2):(half + 1) * (H // 2)] = acc

    nothing = lambda: None

    s.an[...] = rms(x[...])

    def two0():
        m_o(0, 2).start()
        m_o(0, 3).start()
        positions()

    def q0():
        u_start('ffn', 0, 0)

    def kv0_done():
        u_start('moe', 0, 1)
        for j in range(4):
            m_q(1, j).start()
        c_uk(1).start()
        for t in range(B):
            c_kv(1, t).start()

    def uk0():
        send_ids()

    mla(0, two0, q0, uk0, kv0_done, lambda: c_uv(1).start())
    for j in (4, 5):
        m_q(1, j).start()
    for j in (0, 1):
        m_o(1, j).start()
    h0 = (x[...].astype(F32) + s.res[...]).astype(BF)
    s.h0[...] = h0
    s.uall[me] = rms(h0)
    gather_start(s.uall, s.us, s.ur, at16, True)
    slots_here()
    gather_pass(s.uall, s.us, s.ur, at16, True, slots_there)
    gather_wait(s.uall, s.us, s.ur, at16)
    stack(s.uall, at16)
    ffn(0, 0, nothing)
    u_start('moe', 1, 0)
    for zz in range(TP):
        g = at16(zz, ye)
        rc(s.uall.at[g], s.uall.at[g], s.us.at[12 + zz], s.ur.at[g], z, pe).wait_recv()
        send(s.uall.at[g], s.uall.at[g], s.us.at[12 + zz], s.ur.at[g], z, pe)
    ffn_send(0)
    for zz in range(TP):
        g = at16(zz, ype)
        rc(s.uall.at[g], s.uall.at[g], s.us.at[12 + zz], s.ur.at[g], z, pe).wait_recv()
    for half in range(2):
        cols = pl.ds(half * (H // 2), H // 2)
        for d in range(N // 2):
            s.rk[d * 16:(d + 1) * 16, :] = jnp.concatenate([s.uall[2 * d, :, cols], s.uall[2 * d + 1, :, cols]], axis=0)
        s.ea[:, cols] = lax.dot_general(s.ptk[...], s.rk[...], (((0,), (0,)), ((), ())),
                                        preferred_element_type=F32).astype(BF)
    expert(0, 1, nothing)
    f0 = (s.h0[...].astype(F32) + ffn_recv(0)).astype(BF)
    s.f0[...] = f0
    s.an[...] = rms(f0)

    def two1():
        m_o(1, 2).start()
        m_o(1, 3).start()
        u_start('moe', 2, 1)

    mla(1, two1, nothing, nothing, nothing, nothing)
    h1 = (s.f0[...].astype(F32) + s.res[...]).astype(BF)
    s.h1[...] = h1
    s.vall[at8(z, e)] = rms(h1)
    gather_start(s.vall, s.vs, s.vr, at8, False)
    expert(1, 0, nothing)
    u_start('moe', 3, 0)
    expert(2, 1, lambda: gather_pass(s.vall, s.vs, s.vr, at8, False, nothing))
    u_start('ffn', 1, 1)
    expert(3, 0, nothing)
    give_back()
    gather_wait(s.vall, s.vs, s.vr, at8)
    stack(s.vall, at8)
    ffn(1, 1, nothing)
    ffn_send(1)
    take_back()
    y[...] = (s.h1[...].astype(F32) + ffn_recv(1) + s.mm[...]).astype(BF)
    for d in sends:
        d.wait_send()


def rope_table():
    half = ROPE // 2
    f = np.float32(10000.0) ** (np.float32(-2.0) * np.arange(half, dtype=np.float32) / np.float32(ROPE))
    ang = np.arange(1, L + 1, dtype=np.float32)[:, None] * f.astype(np.float32)
    cs, sn = np.cos(ang.astype(np.float64)), np.sin(ang.astype(np.float64))
    left = np.concatenate([cs, cs, -sn, sn], axis=1).astype(np.float32)
    parts = []
    for _ in range(3):
        part = left.astype(jnp.bfloat16)
        parts.append(part)
        left = left - part.astype(np.float32)
    return jnp.asarray(np.concatenate(parts, axis=1))


def layer(x, kv0, kv1, lens, ids, wts, wq, wuk, wuv, wo, w_in, w_out, e_in, e_out):
    table = rope_table()
    sc = scratch()
    vm = pl.BlockSpec(memory_space=pltpu.VMEM)
    hbm = pl.BlockSpec(memory_space=pl.ANY)
    return pl.pallas_call(
        functools.partial(kernel, tuple(sc)),
        out_shape=jax.ShapeDtypeStruct((B, H), BF),
        in_specs=[hbm] * 15,
        out_specs=vm,
        scratch_shapes=list(sc.values()),
        compiler_params=pltpu.CompilerParams(collective_id=0, has_side_effects=True, vmem_limit_bytes=67043328),
    )(x, lens, ids, wts, table, jnp.swapaxes(kv0, 1, 2), jnp.swapaxes(kv1, 1, 2), wq, wuk, wuv, wo, w_in, w_out, e_in, e_out)


def solution(mesh):
    in_specs = (P(BATCH, None), P(BATCH, None, None), P(BATCH, None, None), P(BATCH), P(BATCH, None), P(BATCH, None),
                P(), P(), P(), P(), P(None, None, None, 'tp'), P(None, 'tp', None), P(GROUP, None, None), P(GROUP, None, None))
    return jax.shard_map(layer, mesh=mesh, in_specs=in_specs, out_specs=P(BATCH, None), check_vma=False)
```

```python
import functools
import types

import jax
import jax.numpy as jnp
import numpy as np
from jax import lax
from jax.experimental import pallas as pl
from jax.experimental.pallas import tpu as pltpu
from jax.sharding import PartitionSpec as P

BATCH = ('dp', 'tp', 'ep')
GROUP = ('tp', 'ep')
MESH = pl.DeviceIdType.MESH
BF = jnp.bfloat16
F32 = jnp.float32
I32 = jnp.int32

B = 8
H = 2048
HEADS = 16
NOPE = 128
ROPE = 64
LAT = 512
VH = 128
L = 256
FH = 1408
TP = 4
N = 16
R = HEADS * B
M = 64
CB = 512
SCALE = (NOPE + ROPE) ** -0.5

ALONG = (1, 3, 2)


def scratch():
    dma = pltpu.SemaphoreType.DMA
    v = pltpu.VMEM
    return dict(
        x=v((B, H), BF), lens=v((B,), I32), ids=v((B, 6), I32), wts=v((B, 6), F32), table=v((L, 384), BF), s_in=dma((5,)),
        mbuf=v((8, H, CB), BF), wukb=v((HEADS, NOPE, LAT), BF), wuvb=v((HEADS, LAT, VH), BF), kvb=v((B, LAT + ROPE, L), BF),
        gu5=v((2, 5, H, CB), BF), gu1=v((2, H, CB // 2), BF), wd=v((2, 4, FH, CB), BF),
        qs=v((B, HEADS * (NOPE + ROPE)), F32), qc=v((R, LAT + ROPE), BF), sc=v((R, L), F32),
        ol=v((R, LAT), F32), os=v((B, HEADS * VH), BF), res=v((B, H), F32), an=v((B, H), BF),
        an2=v((2, B, H), BF), q2=v((2 * B, HEADS // 2 * (NOPE + ROPE)), F32), qown=v((2, R // 2, LAT), BF), qout=v((R // 2, LAT), BF),
        rown=v((2, R // 2, 128), F32), rout=v((R // 2, 128), F32), oout=v((R // 2, LAT), BF), oin=v((R // 2, LAT), BF),
        os2=v((2 * B, HEADS // 2 * VH), BF), pout=v((B, H), F32), pin=v((B, H), F32), xs=dma((5,)), xr=dma((5,)),
        h0=v((B, H), BF), f0=v((B, H), BF), h1=v((B, H), BF),
        cs=v((R, ROPE), F32), sn=v((R, ROPE), F32), lm=v((R, L), F32),
        uall=v((N, B, H), BF), vall=v((N // 2, B, H), BF), fa=v((M, H), BF), ea=v((M, H), BF), act=v((M, FH), BF),
        pm=v((4, M // 2, CB), F32), ps=v((2, 4, M // 2, CB), F32), pr=v((2, 4, M // 2, CB), F32),
        bs=v((2, TP, 4, B, CB), BF), br=v((2, TP, 4, B, CB), BF),
        idall=v((N, B, 128), I32), ptk=v((N * B, M), BF), el=v((M, 128), F32), gsel=v((2 * 6 * B, 128), BF),
        racc=v((M, H), F32), rs=v((N, B, H // 2), BF), rr=v((N, B, H // 2), BF), rk=v((N * B, H // 2), BF), mm=v((B, H), F32),
        s_m=dma((8,)), s_h=dma((4,)), s_kv=dma((B,)), s_uk=dma((2,)), s_gu=dma((2, 6, 2)), s_wd=dma((2, 4)),
        us=dma((16,)), ur=dma((N,)), vs=dma((8,)), vr=dma((N // 2,)),
        pss=dma((2, 4)), psr=dma((2, 4)), bss=dma((2, TP, 4)), bsr=dma((2, TP, 4)),
        ids_s=dma((N,)), ids_r=dma((N,)), ret_s=dma((N,)), ret_r=dma((N,)),
    )


def rms(v):
    vf = v.astype(F32)
    return (vf * lax.rsqrt(jnp.mean(vf * vf, axis=-1, keepdims=True) + 1e-6)).astype(BF)


def dot(a, b):
    return jnp.dot(a, b, preferred_element_type=F32)


def kernel(names, x_in, lens_in, ids_in, wts_in, table_in, kv0, kv1, wq, wuk, wuv, wo, w_in, w_out, e_in, e_out, y, *scr):
    s = types.SimpleNamespace(**dict(zip(names, scr)))
    z = lax.axis_index('tp')
    e = lax.axis_index('ep')
    me = z * 4 + e
    c = lax.rem(e, 2)
    pe = e + 1 - 2 * c
    ye = lax.rem(e + 2, 4)
    ype = lax.rem(pe + 2, 4)
    kvs = (kv0, kv1)
    x, lens, ids, wts, table = s.x, s.lens, s.ids, s.wts, s.table
    small = [pltpu.make_async_copy(a, b, s.s_in.at[i]) for i, (a, b) in enumerate(
        ((x_in, x), (lens_in, lens), (table_in, table), (ids_in, ids), (wts_in, wts)))]
    sends = []

    barrier = pltpu.get_barrier_semaphore()
    others = []
    for i in range(1, N):
        zz, ee = lax.rem(z + i // 4, 4), lax.rem(e + i % 4, 4)
        others.append((i, zz * 4 + ee, zz, ee))
    for i, g, zz, ee in others:
        pl.semaphore_signal(barrier, inc=1, device_id=(lax.axis_index('dp'), zz, ee), device_id_type=MESH)

    def cp(src, dst, sem):
        return pltpu.make_async_copy(src, dst, sem)

    def m_q(l, j):
        k = 2 * l + j
        return cp(wq.at[l, :, pl.ds(j * CB, CB)], s.mbuf.at[k], s.s_m.at[k])

    def m_o(l, j):
        k = (2 * l + 6 + j) % 8
        return cp(wo.at[l, :, pl.ds(j * CB, CB)], s.mbuf.at[k], s.s_m.at[k])

    def c_kv(l, t):
        return cp(kvs[l].at[t], s.kvb.at[t], s.s_kv.at[t])

    def c_uk(l):
        if l:
            return cp(wuk.at[1, pl.ds(c * 8, 8)], s.wukb.at[pl.ds(0, 8)], s.s_uk.at[0])
        return cp(wuk.at[0], s.wukb, s.s_uk.at[0])

    def c_uv(l):
        if l:
            return cp(wuv.at[1, pl.ds(c * 8, 8)], s.wuvb.at[pl.ds(0, 8)], s.s_uk.at[1])
        return cp(wuv.at[0], s.wuvb, s.s_uk.at[1])

    def h_q(j):
        cols = pl.ds(pl.multiple_of(c * 1536 + j * CB, CB), CB)
        return cp(wq.at[1, :, cols], s.mbuf.at[2 + j], s.s_m.at[2 + j])

    def h_o(j):
        rows = pl.ds(pl.multiple_of(c * 1024, 1024), 1024)
        return cp(wo.at[1, rows, pl.ds(j * CB, CB)], s.mbuf.at[5 + j // 2, pl.ds(j % 2 * 1024, 1024)], s.s_h.at[j])

    def u_gu(what, i, k, j, w, half):
        o = pl.multiple_of(j * 256, 128)
        if what == 'ffn':
            src = w_in.at[i, half, :, pl.ds(pl.multiple_of(c * FH + o, 128), w)]
        else:
            src = e_in.at[i, :, pl.ds(pl.multiple_of(half * FH + o, 128), w)]
        dst = s.gu5.at[k, j, :, pl.ds(half * w, w)] if w == 256 else s.gu1.at[k, :, pl.ds(half * w, w)]
        return cp(src, dst, s.s_gu.at[k, j, half])

    def u_wd(what, i, k, j):
        cols = pl.ds(pl.multiple_of(j * CB, CB), CB)
        if what == 'ffn':
            src = w_out.at[i, pl.ds(pl.multiple_of(c * FH, 128), FH), cols]
        else:
            src = e_out.at[i, :, cols]
        return cp(src, s.wd.at[k, j], s.s_wd.at[k, j])

    def u_start(what, i, k):
        def gu(j, _):
            u_gu(what, i, k, j, 256, 0).start()
            u_gu(what, i, k, j, 256, 1).start()
            return 0

        lax.fori_loop(0, 5, gu, 0)
        u_gu(what, i, k, 5, 128, 0).start()
        u_gu(what, i, k, 5, 128, 1).start()

        def dn(j, _):
            u_wd(what, i, k, j).start()
            return 0

        lax.fori_loop(0, 4, dn, 0)

    def rc(src, dst, ss, rs, tp, ep):
        return pltpu.make_async_remote_copy(src_ref=src, dst_ref=dst, send_sem=ss, recv_sem=rs,
                                            device_id=(lax.axis_index('dp'), tp, ep), device_id_type=MESH)

    def send(*a):
        d = rc(*a)
        d.start()
        sends.append(d)

    for d in small:
        d.start()
    m_q(0, 0).start()
    m_q(0, 1).start()
    for d in small:
        d.wait()
    for j in range(2, 6):
        m_q(0, j).start()
    for t in range(B):
        c_kv(0, t).start()
    c_uk(0).start()
    c_uv(0).start()
    m_o(0, 0).start()
    m_o(0, 1).start()

    def positions():
        with jax.named_scope('positions'):
            return positions_()

    def positions_():
        diag = lax.broadcasted_iota(I32, (B, B), 0) == lax.broadcasted_iota(I32, (B, B), 1)
        lrow = jnp.broadcast_to(lens[...].astype(F32).reshape(1, B), (B, B))
        lv = jnp.broadcast_to(jnp.sum(jnp.where(diag, lrow, 0.0), axis=1, keepdims=True), (B, L))
        at = jnp.where(lax.broadcasted_iota(I32, (B, L), 1).astype(F32) == lv - 1.0, 1.0, 0.0).astype(BF)
        tb = dot(at, table[...])
        tb = tb[:, :128] + tb[:, 128:256] + tb[:, 256:]
        s.cs[...] = jnp.concatenate([tb[:, :ROPE]] * HEADS, axis=0)
        s.sn[...] = jnp.concatenate([tb[:, ROPE:]] * HEADS, axis=0)
        s.lm[...] = jnp.concatenate([lv] * HEADS, axis=0)

    rowt = lax.broadcasted_iota(I32, (R, L), 0) & (B - 1)

    def q_steps(l, lo, hi):
        with jax.named_scope(f'q_steps{l}'):
            return q_steps_(l, lo, hi)

    def q_steps_(l, lo, hi):
        for j in range(lo, hi):
            m_q(l, j).wait()
        for j in range(lo, hi):
            s.qs[:, j * CB:(j + 1) * CB] = dot(s.an[...], s.mbuf[2 * l + j])

    def mla(l, after_two, after_q, after_uk, after_kv, after_uv):
        q_steps(l, 0, 2)
        after_two()
        if l == 0:
            q_steps(l, 2, 4)
            q_steps(l, 4, 6)
        else:
            q_steps(l, 2, 6)
        after_q()
        latent_q(l)
        after_uk()
        attend(l)
        after_kv()
        values(l)
        after_uv()
        project(l)

    def latent_q(l):
        with jax.named_scope(f'latent_q{l}'):
            return latent_q_(l)

    def latent_q_(l):
        c_uk(l).wait()
        D = NOPE + ROPE
        rope = []
        for hp in range(HEADS // 2):
            pair = []
            for k in range(2):
                h = 2 * hp + k
                qn = s.qs[:, h * D:h * D + NOPE].astype(BF)
                pair.append(dot(qn, s.wukb[h]))
                rope.append(s.qs[:, h * D + NOPE:(h + 1) * D])
            s.qc[hp * 16:(hp + 1) * 16, :LAT] = jnp.concatenate(pair, axis=0).astype(BF)
        rotate(jnp.concatenate(rope, axis=0))

    def rotate(r):
        rot = jnp.concatenate([r[:, ROPE // 2:], r[:, :ROPE // 2]], axis=1)
        s.qc[:, LAT:] = (r * s.cs[...] + rot * s.sn[...]).astype(BF)

    def attend(l):
        with jax.named_scope(f'attend{l}'):
            return attend_(l)

    def attend_(l):
        for t in range(B):
            c_kv(l, t).wait()
        for t in range(B):
            st = dot(s.qc[...], s.kvb[t])
            if t == 0:
                s.sc[...] = st
            else:
                s.sc[...] = jnp.where(rowt == t, st, s.sc[...])
        sc = jnp.where(lax.broadcasted_iota(I32, (R, L), 1).astype(F32) < s.lm[...], s.sc[...] * SCALE, -1e30)
        ex = jnp.exp(sc - jnp.max(sc, axis=-1, keepdims=True))
        p = ex / jnp.sum(ex, axis=-1, keepdims=True)
        ol = None
        for t in range(B):
            pt = jnp.where(rowt == t, p, 0.0).astype(BF)
            ot = lax.dot_general(pt, s.kvb[t, :LAT, :], (((1,), (1,)), ((), ())), preferred_element_type=F32)
            ol = ot if ol is None else ol + ot
        s.ol[...] = ol

    def values(l):
        with jax.named_scope(f'values{l}'):
            return values_(l)

    def values_(l):
        c_uv(l).wait()
        for h in range(HEADS):
            o = dot(s.ol[h * B:(h + 1) * B, :].astype(BF), s.wuvb[h])
            s.os[:, h * VH:(h + 1) * VH] = o.astype(BF)

    def project(l):
        with jax.named_scope(f'project{l}'):
            return project_(l)

    def project_(l):
        for j in range(4):
            m_o(l, j).wait()
        for j in range(4):
            s.res[:, j * CB:(j + 1) * CB] = dot(s.os[...], s.mbuf[(2 * l + 6 + j) % 8])

    def swap(i, src, dst):
        send(src, dst, s.xs.at[i], s.xr.at[i], z, pe)

    def swapped(i, src, dst):
        rc(src, dst, s.xs.at[i], s.xr.at[i], z, pe).wait_recv()

    def half_q():
        with jax.named_scope('half_q'):
            return half_q_()

    def half_q_():
        swap(0, s.an2.at[c], s.an2.at[c])
        swapped(0, s.an2.at[1 - c], s.an2.at[1 - c])
        a = jnp.concatenate([s.an2[c], s.an2[1 - c]], axis=0)
        for j in range(3):
            h_q(j).wait()
        for j in range(3):
            s.q2[:, j * CB:(j + 1) * CB] = dot(a, s.mbuf[2 + j])
        c_uk(1).wait()
        D = NOPE + ROPE
        zero = jnp.zeros((B, 128 - ROPE), F32)
        for hp in range(HEADS // 4):
            pair = []
            for h in (2 * hp, 2 * hp + 1):
                pair.append(dot(s.q2[:, h * D:h * D + NOPE].astype(BF), s.wukb[h]))
                r = s.q2[:, h * D + NOPE:(h + 1) * D]
                s.rown[c, h * B:(h + 1) * B, :] = jnp.concatenate([r[:B], zero], axis=1)
                s.rout[h * B:(h + 1) * B, :] = jnp.concatenate([r[B:], zero], axis=1)
            s.qown[c, hp * 16:(hp + 1) * 16, :] = jnp.concatenate([pair[0][:B], pair[1][:B]], axis=0).astype(BF)
            s.qout[hp * 16:(hp + 1) * 16, :] = jnp.concatenate([pair[0][B:], pair[1][B:]], axis=0).astype(BF)
        swap(1, s.qout, s.qown.at[c])
        swap(2, s.rout, s.rown.at[c])
        swapped(1, s.qout, s.qown.at[1 - c])
        swapped(2, s.rout, s.rown.at[1 - c])
        for i in range(2):
            s.qc[i * 64:(i + 1) * 64, :LAT] = s.qown[i]
        rotate(jnp.concatenate([s.rown[0], s.rown[1]], axis=0)[:, :ROPE])

    def half_values():
        with jax.named_scope('half_values'):
            return half_values_()

    def half_values_():
        s.oout[...] = s.ol[pl.ds(pl.multiple_of((1 - c) * 64, 64), 64), :].astype(BF)
        swap(3, s.oout, s.oin)
        own = s.ol[pl.ds(pl.multiple_of(c * 64, 64), 64), :]
        c_uv(1).wait()
        swapped(3, s.oout, s.oin)
        other = s.oin[...].astype(F32)
        for h in range(HEADS // 2):
            rows = slice(h * B, (h + 1) * B)
            o = dot(jnp.concatenate([own[rows], other[rows]], axis=0).astype(BF), s.wuvb[h])
            s.os2[:, h * VH:(h + 1) * VH] = o.astype(BF)

    def half_project():
        with jax.named_scope('half_project'):
            return half_project_()

    def half_project_():
        for j in range(4):
            h_o(j).wait()
        for j in range(4):
            r = dot(s.os2[...], s.mbuf[5 + j // 2, j % 2 * 1024:(j % 2 + 1) * 1024, :])
            s.res[:, j * CB:(j + 1) * CB] = r[:B]
            s.pout[:, j * CB:(j + 1) * CB] = r[B:]
        swap(4, s.pout, s.pin)
        swapped(4, s.pout, s.pin)
        s.res[...] = s.res[...] + s.pin[...]

    def unit(what, i, k, lhs, down_groups, down, between):
        def silu(g, u):
            return (g / (1.0 + jnp.exp(-g)) * u).astype(BF)

        early = (what, i) in (('ffn', 0), ('moe', 0), ('moe', 1))
        for group in ((0, 1, 2, 3, 4, 5),) if early else ((0, 1, 2), (3, 4, 5)):
            for j in group:
                w = 256 if j < 5 else 128
                u_gu(what, i, k, j, w, 0).wait()
                u_gu(what, i, k, j, w, 1).wait()
            if early:
                for j in range(4):
                    u_wd(what, i, k, j).wait()
            for j in group:
                w = 256 if j < 5 else 128
                r = dot(lhs[...], s.gu5[k, j] if j < 5 else s.gu1[k])
                s.act[:, j * 256:j * 256 + w] = silu(r[:, :w], r[:, w:])
        between()
        for group in down_groups:
            for j in group if not early else ():
                u_wd(what, i, k, j).wait()
            down(group, lambda j: dot(s.act[...], s.wd[k, j]))

    def gather_start(buf, ss, rs, at, on_y):
        with jax.named_scope('gather_start'):
            return gather_start_(buf, ss, rs, at, on_y)

    def gather_start_(buf, ss, rs, at, on_y):
        own = at(z, e)
        for k in ALONG:
            send(buf.at[own], buf.at[own], ss.at[k - 1], rs.at[own], lax.rem(z + k, TP), e)
        send(buf.at[own], buf.at[own], ss.at[3], rs.at[own], z, pe)
        if on_y:
            send(buf.at[own], buf.at[own], ss.at[8], rs.at[own], z, ye)

    def gather_pass(buf, ss, rs, at, on_y, before_last):
        with jax.named_scope('gather_pass'):
            return gather_pass_(buf, ss, rs, at, on_y, before_last)

    def gather_pass_(buf, ss, rs, at, on_y, before_last):
        for k in ALONG:
            if k == ALONG[-1]:
                before_last()
            g = at(lax.rem(z + k, TP), e)
            rc(buf.at[g], buf.at[g], ss.at[3 + k], rs.at[g], z, pe).wait_recv()
            send(buf.at[g], buf.at[g], ss.at[3 + k], rs.at[g], z, pe)
            if on_y:
                send(buf.at[g], buf.at[g], ss.at[8 + k], rs.at[g], z, ye)

    def gather_wait(buf, ss, rs, at):
        with jax.named_scope('gather_wait'):
            return gather_wait_(buf, ss, rs, at)

    def gather_wait_(buf, ss, rs, at):
        for zz in range(TP):
            g = at(zz, pe)
            rc(buf.at[g], buf.at[g], ss.at[0], rs.at[g], z, pe).wait_recv()

    def stack(buf, at):
        with jax.named_scope('stack'):
            return stack_(buf, at)

    def stack_(buf, at):
        for i, ee in enumerate((e, pe)):
            for q in range(2):
                s.fa[i * 32 + q * 16:i * 32 + q * 16 + 16, :] = jnp.concatenate([buf[at(2 * q, ee)], buf[at(2 * q + 1, ee)]], axis=0)

    def ffn(l, k, between):
        with jax.named_scope(f'ffn{l}'):
            return ffn_(l, k, between)

    def ffn_(l, k, between):
        def down(group, product):
            for j in group:
                r = product(j)
                s.pm[j] = r[:M // 2]
                s.ps[l, j] = r[M // 2:]
            for j in group:
                rc(s.ps.at[l, j], s.pr.at[l, j], s.pss.at[l, j], s.psr.at[l, j], z, pe).start()

        unit('ffn', l, k, s.fa, ((0, 1), (2, 3)), down, between)

    def ffn_send(l):
        with jax.named_scope(f'ffn_send{l}'):
            return ffn_send_(l)

    def ffn_send_(l):
        for j in range(4):
            rc(s.ps.at[l, j], s.pr.at[l, j], s.pss.at[l, j], s.psr.at[l, j], z, pe).wait()
            tot = s.pm[j] + s.pr[l, j]
            for q in range(TP):
                s.bs[l, q, j] = tot[q * B:(q + 1) * B].astype(BF)
            for k in ALONG:
                zz = lax.rem(z + k, TP)
                send(s.bs.at[l, zz, j], s.br.at[l, z, j], s.bss.at[l, k, j], s.bsr.at[l, z, j], zz, e)
            s.br[l, z, j] = s.bs[l, z, j]

    def ffn_recv(l):
        with jax.named_scope(f'ffn_recv{l}'):
            return ffn_recv_(l)

    def ffn_recv_(l):
        for j in range(4):
            for k in ALONG:
                zz = lax.rem(z + k, TP)
                rc(s.bs.at[l, zz, j], s.br.at[l, zz, j], s.bss.at[l, k, j], s.bsr.at[l, zz, j], zz, e).wait_recv()
            acc = s.br[l, 0, j].astype(F32)
            for q in range(1, TP):
                acc = acc + s.br[l, q, j].astype(F32)
            s.res[:, j * CB:(j + 1) * CB] = acc
        return s.res[...]

    def at16(zz, ee):
        return zz * 4 + ee

    def at8(zz, ee):
        return zz * 2 + lax.rem(ee, 2)

    def send_ids():
        with jax.named_scope('send_ids'):
            return send_ids_()

    def send_ids_():
        s.idall[me] = jnp.full((B, 128), -1, I32)
        s.idall[me, :, 0:6] = ids[...]
        pl.semaphore_wait(barrier, N - 1)
        for i, g, zz, ee in others:
            send(s.idall.at[me], s.idall.at[me], s.ids_s.at[i], s.ids_r.at[me], zz, ee)

    def slots_here():
        with jax.named_scope('slots_here'):
            return slots_here_()

    def slots_here_():
        lane = lax.broadcasted_iota(I32, (B, 128), 1)
        mine = s.idall[me]
        dst = [jnp.broadcast_to(mine[:, j:j + 1], (B, 128)) >> 2 for j in range(6)]
        hot = [jnp.where(d == lane, 1.0, 0.0) for d in dst]
        cnt = functools.reduce(jnp.add, hot)
        row = lax.broadcasted_iota(I32, (B, 128), 0)
        run = jnp.zeros((B, 128), F32)
        for t in range(B - 1):
            run = run + jnp.where(row > t, jnp.broadcast_to(cnt[t:t + 1], (B, 128)), 0.0)
        left, right = [], []
        for j in range(6):
            pos = jnp.sum(hot[j] * run, axis=1, keepdims=True)
            run = run + hot[j]
            col = dst[j].astype(F32) * B + pos
            left.append(jnp.where(col == lane.astype(F32), 1.0, 0.0))
            right.append(jnp.where(col + 4.0 == lane.astype(F32), 1.0, 0.0))
        s.gsel[...] = jnp.concatenate(left + right, axis=0).astype(BF)

    def slots_there():
        with jax.named_scope('slots_there'):
            return slots_there_()

    def slots_there_():
        for i, g, zz, ee in others:
            rc(s.idall.at[g], s.idall.at[g], s.ids_s.at[i], s.ids_r.at[g], z, pe).wait_recv()
        T = N * B
        idt = jnp.concatenate([s.idall[d] for d in range(N)], axis=0)
        lane = lax.broadcasted_iota(I32, (T, 128), 1)
        tok = lax.broadcasted_iota(I32, (T, 128), 0)
        col = [jnp.broadcast_to(idt[:, j:j + 1], (T, 128)) for j in range(6)]
        hit = [jnp.where((v >> 2) == me, 1.0, 0.0) for v in col]
        before = jnp.where((tok >> 3 == lane >> 3) & (lane < tok), 1.0, 0.0)
        run = dot(before.astype(BF), functools.reduce(jnp.add, hit).astype(BF)) + ((tok >> 3) * 4).astype(F32)
        pt = jnp.zeros((T, 128), F32)
        ex = jnp.zeros((T, 128), F32)
        for j in range(6):
            at = jnp.where(run == lane.astype(F32), hit[j], 0.0)
            pt = pt + at
            ex = ex + at * (col[j] & 3).astype(F32)
            run = run + hit[j]
        s.ptk[...] = pt[:, :M].astype(BF)
        s.el[...] = lax.dot_general(ex[:, :M].astype(BF), jnp.ones((T, 128), BF), (((0,), (0,)), ((), ())),
                                    preferred_element_type=F32)

    def expert(i, k, between):
        with jax.named_scope(f'expert{i}'):
            return expert_(i, k, between)

    def expert_(i, k, between):
        def down(group, product):
            for j in group:
                cols = pl.ds(j * CB, CB)
                r = product(j).astype(BF).astype(F32)
                if i == 0:
                    s.racc[:, cols] = r
                else:
                    keep = jnp.broadcast_to(s.el[:, 0:1], (M, CB)) == float(i)
                    s.racc[:, cols] = jnp.where(keep, r, s.racc[:, cols])

        unit('moe', i, k, s.ea, ((0, 1, 2, 3),), down, between)

    def give_back():
        with jax.named_scope('give_back'):
            return give_back_()

    def give_back_():
        for d in range(N):
            a = s.racc[4 * d:4 * d + 4, :]
            s.rs[d] = jnp.concatenate([a[:, :H // 2], a[:, H // 2:]], axis=0).astype(BF)
        for i, g, zz, ee in others:
            send(s.rs.at[g], s.rr.at[me], s.ret_s.at[i], s.ret_r.at[me], zz, ee)
        s.rr[me] = s.rs[me]

    def take_back():
        with jax.named_scope('take_back'):
            return take_back_()

    def take_back_():
        for i, g, zz, ee in others:
            rc(s.rs.at[g], s.rr.at[g], s.ret_s.at[i], s.ret_r.at[g], z, pe).wait_recv()
        for d in range(N // 2):
            s.rk[d * 16:(d + 1) * 16, :] = jnp.concatenate([s.rr[2 * d], s.rr[2 * d + 1]], axis=0)
        got = dot(s.gsel[...], s.rk[...])
        for half in range(2):
            acc = None
            for j in range(6):
                o = (half * 6 + j) * B
                term = wts[:, j:j + 1] * got[o:o + B]
                acc = term if acc is None else acc + term
            s.mm[:, half * (H // 2):(half + 1) * (H // 2)] = acc

    nothing = lambda: None

    s.an[...] = rms(x[...])

    def two0():
        m_o(0, 2).start()
        m_o(0, 3).start()
        positions()

    def q0():
        u_start('ffn', 0, 0)

    def kv0_done():
        u_start('moe', 0, 1)
        for j in range(3):
            h_q(j).start()
        c_uk(1).start()
        for t in range(B):
            c_kv(1, t).start()
        h_o(0).start()
        h_o(1).start()

    def uk0():
        send_ids()

    mla(0, two0, q0, uk0, kv0_done, lambda: c_uv(1).start())
    h_o(2).start()
    h_o(3).start()
    h0 = (x[...].astype(F32) + s.res[...]).astype(BF)
    s.h0[...] = h0
    s.uall[me] = rms(h0)
    gather_start(s.uall, s.us, s.ur, at16, True)
    slots_here()
    gather_pass(s.uall, s.us, s.ur, at16, True, slots_there)
    gather_wait(s.uall, s.us, s.ur, at16)
    stack(s.uall, at16)
    ffn(0, 0, nothing)
    u_start('moe', 1, 0)
    for zz in range(TP):
        g = at16(zz, ye)
        rc(s.uall.at[g], s.uall.at[g], s.us.at[12 + zz], s.ur.at[g], z, pe).wait_recv()
        send(s.uall.at[g], s.uall.at[g], s.us.at[12 + zz], s.ur.at[g], z, pe)
    ffn_send(0)
    for zz in range(TP):
        g = at16(zz, ype)
        rc(s.uall.at[g], s.uall.at[g], s.us.at[12 + zz], s.ur.at[g], z, pe).wait_recv()
    for half in range(2):
        cols = pl.ds(half * (H // 2), H // 2)
        for d in range(N // 2):
            s.rk[d * 16:(d + 1) * 16, :] = jnp.concatenate([s.uall[2 * d, :, cols], s.uall[2 * d + 1, :, cols]], axis=0)
        s.ea[:, cols] = lax.dot_general(s.ptk[...], s.rk[...], (((0,), (0,)), ((), ())),
                                        preferred_element_type=F32).astype(BF)
    expert(0, 1, nothing)
    u_start('moe', 2, 1)
    f0 = (s.h0[...].astype(F32) + ffn_recv(0)).astype(BF)
    s.f0[...] = f0
    s.an2[c] = rms(f0)
    half_q()
    attend(1)
    half_values()
    half_project()
    h1 = (s.f0[...].astype(F32) + s.res[...]).astype(BF)
    s.h1[...] = h1
    s.vall[at8(z, e)] = rms(h1)
    gather_start(s.vall, s.vs, s.vr, at8, False)
    expert(1, 0, nothing)
    u_start('moe', 3, 0)
    expert(2, 1, lambda: gather_pass(s.vall, s.vs, s.vr, at8, False, nothing))
    u_start('ffn', 1, 1)
    expert(3, 0, nothing)
    give_back()
    gather_wait(s.vall, s.vs, s.vr, at8)
    stack(s.vall, at8)
    ffn(1, 1, nothing)
    ffn_send(1)
    take_back()
    y[...] = (s.h1[...].astype(F32) + ffn_recv(1) + s.mm[...]).astype(BF)
    for d in sends:
        d.wait_send()


def rope_table():
    half = ROPE // 2
    f = np.float32(10000.0) ** (np.float32(-2.0) * np.arange(half, dtype=np.float32) / np.float32(ROPE))
    ang = np.arange(1, L + 1, dtype=np.float32)[:, None] * f.astype(np.float32)
    cs, sn = np.cos(ang.astype(np.float64)), np.sin(ang.astype(np.float64))
    left = np.concatenate([cs, cs, -sn, sn], axis=1).astype(np.float32)
    parts = []
    for _ in range(3):
        part = left.astype(jnp.bfloat16)
        parts.append(part)
        left = left - part.astype(np.float32)
    return jnp.asarray(np.concatenate(parts, axis=1))


def layer(x, kv0, kv1, lens, ids, wts, wq, wuk, wuv, wo, w_in, w_out, e_in, e_out):
    table = rope_table()
    sc = scratch()
    vm = pl.BlockSpec(memory_space=pltpu.VMEM)
    hbm = pl.BlockSpec(memory_space=pl.ANY)
    return pl.pallas_call(
        functools.partial(kernel, tuple(sc)),
        out_shape=jax.ShapeDtypeStruct((B, H), BF),
        in_specs=[hbm] * 15,
        out_specs=vm,
        scratch_shapes=list(sc.values()),
        compiler_params=pltpu.CompilerParams(collective_id=0, has_side_effects=True, vmem_limit_bytes=67043328),
    )(x, lens, ids, wts, table, jnp.swapaxes(kv0, 1, 2), jnp.swapaxes(kv1, 1, 2), wq, wuk, wuv, wo, w_in, w_out, e_in, e_out)


def solution(mesh):
    in_specs = (P(BATCH, None), P(BATCH, None, None), P(BATCH, None, None), P(BATCH), P(BATCH, None), P(BATCH, None),
                P(), P(), P(), P(), P(None, None, None, 'tp'), P(None, 'tp', None), P(GROUP, None, None), P(GROUP, None, None))
    return jax.shard_map(layer, mesh=mesh, in_specs=in_specs, out_specs=P(BATCH, None), check_vma=False)
```

```python
import functools
import types

import jax
import jax.numpy as jnp
import numpy as np
from jax import lax
from jax.experimental import pallas as pl
from jax.experimental.pallas import tpu as pltpu
from jax.sharding import PartitionSpec as P

BATCH = ('dp', 'tp', 'ep')
GROUP = ('tp', 'ep')
MESH = pl.DeviceIdType.MESH
BF = jnp.bfloat16
F32 = jnp.float32
I32 = jnp.int32

B = 8
H = 2048
HEADS = 16
NOPE = 128
ROPE = 64
LAT = 512
VH = 128
L = 256
FH = 1408
TP = 4
N = 16
R = HEADS * B
M = 64
CB = 512
SCALE = (NOPE + ROPE) ** -0.5

ALONG = (1, 3, 2)


def scratch():
    dma = pltpu.SemaphoreType.DMA
    v = pltpu.VMEM
    return dict(
        x=v((B, H), BF), lens=v((B,), I32), ids=v((B, 6), I32), wts=v((B, 6), F32), table=v((L, 384), BF), s_in=dma((5,)),
        mbuf=v((8, H, CB), BF), wukb=v((HEADS, NOPE, LAT), BF), wuvb=v((HEADS, LAT, VH), BF), kvb=v((B, LAT + ROPE, L), BF),
        gu5=v((2, 5, H, CB), BF), gu1=v((2, H, CB // 2), BF), wd=v((2, 4, FH, CB), BF),
        qs=v((B, HEADS * (NOPE + ROPE)), F32), qc=v((R, LAT + ROPE), BF), sc=v((R, L), F32),
        ol=v((R, LAT), F32), os=v((B, HEADS * VH), BF), res=v((B, H), F32), an=v((B, H), BF),
        an2=v((2, B, H), BF), q2=v((2 * B, HEADS // 2 * (NOPE + ROPE)), F32), qown=v((2, R // 2, LAT), BF), qout=v((R // 2, LAT), BF),
        rown=v((2, R // 2, 128), F32), rout=v((R // 2, 128), F32), oout=v((R // 2, LAT), BF), oin=v((R // 2, LAT), BF),
        os2=v((2 * B, HEADS // 2 * VH), BF), pout=v((B, H), F32), pin=v((B, H), F32), xs=dma((5,)), xr=dma((5,)),
        h0=v((B, H), BF), f0=v((B, H), BF), h1=v((B, H), BF),
        cs=v((R, ROPE), F32), sn=v((R, ROPE), F32), lm=v((R, L), F32),
        uall=v((N, B, H), BF), vall=v((N // 2, B, H), BF), fa=v((M, H), BF), ea=v((M, H), BF), act=v((M, FH), BF),
        pm=v((4, M // 2, CB), F32), ps=v((2, 4, M // 2, CB), F32), pr=v((2, 4, M // 2, CB), F32),
        bs=v((2, TP, 4, B, CB), BF), br=v((2, TP, 4, B, CB), BF),
        idall=v((N, B, 128), I32), ptk=v((N * B, M), BF), el=v((M, 128), F32), gsel=v((2 * 6 * B, 128), BF),
        racc=v((M, H), F32), rs=v((N, B, H // 2), BF), rr=v((N, B, H // 2), BF), rk=v((N * B, H // 2), BF), mm=v((B, H), F32),
        s_m=dma((8,)), s_h=dma((4,)), s_kv=dma((B,)), s_uk=dma((2,)), s_gu=dma((2, 6, 2)), s_wd=dma((2, 4)),
        us=dma((16,)), ur=dma((N,)), vs=dma((8,)), vr=dma((N // 2,)),
        pss=dma((2, 4)), psr=dma((2, 4)), bss=dma((2, TP, 4)), bsr=dma((2, TP, 4)),
        ids_s=dma((N,)), ids_r=dma((N,)), ret_s=dma((N,)), ret_r=dma((N,)),
    )


def rms(v):
    vf = v.astype(F32)
    return (vf * lax.rsqrt(jnp.mean(vf * vf, axis=-1, keepdims=True) + 1e-6)).astype(BF)


def dot(a, b):
    return jnp.dot(a, b, preferred_element_type=F32)


def kernel(names, x_in, lens_in, ids_in, wts_in, table_in, kv0, kv1, wq, wuk, wuv, wo, w_in, w_out, e_in, e_out, y, *scr):
    s = types.SimpleNamespace(**dict(zip(names, scr)))
    z = lax.axis_index('tp')
    e = lax.axis_index('ep')
    me = z * 4 + e
    c = lax.rem(e, 2)
    pe = e + 1 - 2 * c
    ye = lax.rem(e + 2, 4)
    ype = lax.rem(pe + 2, 4)
    kvs = (kv0, kv1)
    x, lens, ids, wts, table = s.x, s.lens, s.ids, s.wts, s.table
    small = [pltpu.make_async_copy(a, b, s.s_in.at[i]) for i, (a, b) in enumerate(
        ((x_in, x), (lens_in, lens), (table_in, table), (ids_in, ids), (wts_in, wts)))]
    sends = []

    barrier = pltpu.get_barrier_semaphore()
    others = []
    for i in range(1, N):
        zz, ee = lax.rem(z + i // 4, 4), lax.rem(e + i % 4, 4)
        others.append((i, zz * 4 + ee, zz, ee))
    for i, g, zz, ee in others:
        pl.semaphore_signal(barrier, inc=1, device_id=(lax.axis_index('dp'), zz, ee), device_id_type=MESH)

    def cp(src, dst, sem):
        return pltpu.make_async_copy(src, dst, sem)

    def m_q(l, j):
        k = 2 * l + j
        return cp(wq.at[l, :, pl.ds(j * CB, CB)], s.mbuf.at[k], s.s_m.at[k])

    def m_o(l, j):
        k = (2 * l + 6 + j) % 8
        return cp(wo.at[l, :, pl.ds(j * CB, CB)], s.mbuf.at[k], s.s_m.at[k])

    def c_kv(l, t):
        return cp(kvs[l].at[t], s.kvb.at[t], s.s_kv.at[t])

    def c_uk(l):
        if l:
            return cp(wuk.at[1, pl.ds(c * 8, 8)], s.wukb.at[pl.ds(0, 8)], s.s_uk.at[0])
        return cp(wuk.at[0], s.wukb, s.s_uk.at[0])

    def c_uv(l):
        if l:
            return cp(wuv.at[1, pl.ds(c * 8, 8)], s.wuvb.at[pl.ds(0, 8)], s.s_uk.at[1])
        return cp(wuv.at[0], s.wuvb, s.s_uk.at[1])

    def h_q(j):
        cols = pl.ds(pl.multiple_of(c * 1536 + j * CB, CB), CB)
        return cp(wq.at[1, :, cols], s.mbuf.at[2 + j], s.s_m.at[2 + j])

    def h_o(j):
        rows = pl.ds(pl.multiple_of(c * 1024, 1024), 1024)
        return cp(wo.at[1, rows, pl.ds(j * CB, CB)], s.mbuf.at[5 + j // 2, pl.ds(j % 2 * 1024, 1024)], s.s_h.at[j])

    def u_gu(what, i, k, j, w, half):
        o = pl.multiple_of(j * 256, 128)
        if what == 'ffn':
            src = w_in.at[i, half, :, pl.ds(pl.multiple_of(c * FH + o, 128), w)]
        else:
            src = e_in.at[i, :, pl.ds(pl.multiple_of(half * FH + o, 128), w)]
        dst = s.gu5.at[k, j, :, pl.ds(half * w, w)] if w == 256 else s.gu1.at[k, :, pl.ds(half * w, w)]
        return cp(src, dst, s.s_gu.at[k, j, half])

    def u_wd(what, i, k, j):
        cols = pl.ds(pl.multiple_of(j * CB, CB), CB)
        if what == 'ffn':
            src = w_out.at[i, pl.ds(pl.multiple_of(c * FH, 128), FH), cols]
        else:
            src = e_out.at[i, :, cols]
        return cp(src, s.wd.at[k, j], s.s_wd.at[k, j])

    def u_start_gu(what, i, k):
        def gu(j, _):
            u_gu(what, i, k, j, 256, 0).start()
            u_gu(what, i, k, j, 256, 1).start()
            return 0

        lax.fori_loop(0, 5, gu, 0)
        u_gu(what, i, k, 5, 128, 0).start()
        u_gu(what, i, k, 5, 128, 1).start()

    def u_start_wd(what, i, k):
        def dn(j, _):
            u_wd(what, i, k, j).start()
            return 0

        lax.fori_loop(0, 4, dn, 0)

    def u_start(what, i, k):
        u_start_gu(what, i, k)
        u_start_wd(what, i, k)

    def rc(src, dst, ss, rs, tp, ep):
        return pltpu.make_async_remote_copy(src_ref=src, dst_ref=dst, send_sem=ss, recv_sem=rs,
                                            device_id=(lax.axis_index('dp'), tp, ep), device_id_type=MESH)

    def send(*a):
        d = rc(*a)
        d.start()
        sends.append(d)

    for d in small:
        d.start()
    m_q(0, 0).start()
    m_q(0, 1).start()
    for d in small:
        d.wait()
    for j in range(2, 6):
        m_q(0, j).start()
    for t in range(B):
        c_kv(0, t).start()
    c_uk(0).start()
    c_uv(0).start()
    m_o(0, 0).start()
    m_o(0, 1).start()

    def positions():
        with jax.named_scope('positions'):
            return positions_()

    def positions_():
        diag = lax.broadcasted_iota(I32, (B, B), 0) == lax.broadcasted_iota(I32, (B, B), 1)
        lrow = jnp.broadcast_to(lens[...].astype(F32).reshape(1, B), (B, B))
        lv = jnp.broadcast_to(jnp.sum(jnp.where(diag, lrow, 0.0), axis=1, keepdims=True), (B, L))
        at = jnp.where(lax.broadcasted_iota(I32, (B, L), 1).astype(F32) == lv - 1.0, 1.0, 0.0).astype(BF)
        tb = dot(at, table[...])
        tb = tb[:, :128] + tb[:, 128:256] + tb[:, 256:]
        s.cs[...] = jnp.concatenate([tb[:, :ROPE]] * HEADS, axis=0)
        s.sn[...] = jnp.concatenate([tb[:, ROPE:]] * HEADS, axis=0)
        s.lm[...] = jnp.concatenate([lv] * HEADS, axis=0)

    rowt = lax.broadcasted_iota(I32, (R, L), 0) & (B - 1)

    def q_steps(l, lo, hi):
        with jax.named_scope(f'q_steps{l}'):
            return q_steps_(l, lo, hi)

    def q_steps_(l, lo, hi):
        for j in range(lo, hi):
            m_q(l, j).wait()
        for j in range(lo, hi):
            s.qs[:, j * CB:(j + 1) * CB] = dot(s.an[...], s.mbuf[2 * l + j])

    def mla(l, after_two, after_q, after_uk, after_kv, after_uv):
        q_steps(l, 0, 2)
        after_two()
        if l == 0:
            q_steps(l, 2, 4)
            q_steps(l, 4, 6)
        else:
            q_steps(l, 2, 6)
        after_q()
        latent_q(l)
        after_uk()
        attend(l)
        after_kv()
        values(l)
        after_uv()
        project(l)

    def latent_q(l):
        with jax.named_scope(f'latent_q{l}'):
            return latent_q_(l)

    def latent_q_(l):
        c_uk(l).wait()
        D = NOPE + ROPE
        rope = []
        for hp in range(HEADS // 2):
            pair = []
            for k in range(2):
                h = 2 * hp + k
                qn = s.qs[:, h * D:h * D + NOPE].astype(BF)
                pair.append(dot(qn, s.wukb[h]))
                rope.append(s.qs[:, h * D + NOPE:(h + 1) * D])
            s.qc[hp * 16:(hp + 1) * 16, :LAT] = jnp.concatenate(pair, axis=0).astype(BF)
        rotate(jnp.concatenate(rope, axis=0))

    def rotate(r):
        rot = jnp.concatenate([r[:, ROPE // 2:], r[:, :ROPE // 2]], axis=1)
        s.qc[:, LAT:] = (r * s.cs[...] + rot * s.sn[...]).astype(BF)

    def attend(l):
        with jax.named_scope(f'attend{l}'):
            return attend_(l)

    def attend_(l):
        for t in range(B):
            c_kv(l, t).wait()
        for t in range(B):
            st = dot(s.qc[...], s.kvb[t])
            if t == 0:
                s.sc[...] = st
            else:
                s.sc[...] = jnp.where(rowt == t, st, s.sc[...])
        sc = jnp.where(lax.broadcasted_iota(I32, (R, L), 1).astype(F32) < s.lm[...], s.sc[...] * SCALE, -1e30)
        ex = jnp.exp(sc - jnp.max(sc, axis=-1, keepdims=True))
        p = ex / jnp.sum(ex, axis=-1, keepdims=True)
        ol = None
        for t in range(B):
            pt = jnp.where(rowt == t, p, 0.0).astype(BF)
            ot = lax.dot_general(pt, s.kvb[t, :LAT, :], (((1,), (1,)), ((), ())), preferred_element_type=F32)
            ol = ot if ol is None else ol + ot
        s.ol[...] = ol

    def values(l):
        with jax.named_scope(f'values{l}'):
            return values_(l)

    def values_(l):
        c_uv(l).wait()
        for h in range(HEADS):
            o = dot(s.ol[h * B:(h + 1) * B, :].astype(BF), s.wuvb[h])
            s.os[:, h * VH:(h + 1) * VH] = o.astype(BF)

    def project(l):
        with jax.named_scope(f'project{l}'):
            return project_(l)

    def project_(l):
        for j in range(4):
            m_o(l, j).wait()
        for j in range(4):
            s.res[:, j * CB:(j + 1) * CB] = dot(s.os[...], s.mbuf[(2 * l + 6 + j) % 8])

    def swap(i, src, dst):
        send(src, dst, s.xs.at[i], s.xr.at[i], z, pe)

    def swapped(i, src, dst):
        rc(src, dst, s.xs.at[i], s.xr.at[i], z, pe).wait_recv()

    def half_q():
        with jax.named_scope('half_q'):
            return half_q_()

    def half_q_():
        swap(0, s.an2.at[c], s.an2.at[c])
        swapped(0, s.an2.at[1 - c], s.an2.at[1 - c])
        a = jnp.concatenate([s.an2[c], s.an2[1 - c]], axis=0)
        for j in range(3):
            h_q(j).wait()
        for j in range(3):
            s.q2[:, j * CB:(j + 1) * CB] = dot(a, s.mbuf[2 + j])
        c_uk(1).wait()
        D = NOPE + ROPE
        zero = jnp.zeros((B, 128 - ROPE), F32)
        for hp in range(HEADS // 4):
            pair = []
            for h in (2 * hp, 2 * hp + 1):
                pair.append(dot(s.q2[:, h * D:h * D + NOPE].astype(BF), s.wukb[h]))
                r = s.q2[:, h * D + NOPE:(h + 1) * D]
                s.rown[c, h * B:(h + 1) * B, :] = jnp.concatenate([r[:B], zero], axis=1)
                s.rout[h * B:(h + 1) * B, :] = jnp.concatenate([r[B:], zero], axis=1)
            s.qown[c, hp * 16:(hp + 1) * 16, :] = jnp.concatenate([pair[0][:B], pair[1][:B]], axis=0).astype(BF)
            s.qout[hp * 16:(hp + 1) * 16, :] = jnp.concatenate([pair[0][B:], pair[1][B:]], axis=0).astype(BF)
        swap(1, s.qout, s.qown.at[c])
        swap(2, s.rout, s.rown.at[c])
        swapped(1, s.qout, s.qown.at[1 - c])
        swapped(2, s.rout, s.rown.at[1 - c])
        for i in range(2):
            s.qc[i * 64:(i + 1) * 64, :LAT] = s.qown[i]
        rotate(jnp.concatenate([s.rown[0], s.rown[1]], axis=0)[:, :ROPE])

    def half_values_send():
        s.oout[...] = s.ol[pl.ds(pl.multiple_of((1 - c) * 64, 64), 64), :].astype(BF)
        swap(3, s.oout, s.oin)

    def half_values():
        with jax.named_scope('half_values'):
            return half_values_()

    def half_values_():
        own = s.ol[pl.ds(pl.multiple_of(c * 64, 64), 64), :]
        c_uv(1).wait()
        swapped(3, s.oout, s.oin)
        other = s.oin[...].astype(F32)
        for h in range(HEADS // 2):
            rows = slice(h * B, (h + 1) * B)
            o = dot(jnp.concatenate([own[rows], other[rows]], axis=0).astype(BF), s.wuvb[h])
            s.os2[:, h * VH:(h + 1) * VH] = o.astype(BF)

    def half_project():
        with jax.named_scope('half_project'):
            return half_project_()

    def half_project_():
        for j in range(4):
            h_o(j).wait()
        for j in range(4):
            r = dot(s.os2[...], s.mbuf[5 + j // 2, j % 2 * 1024:(j % 2 + 1) * 1024, :])
            s.res[:, j * CB:(j + 1) * CB] = r[:B]
            s.pout[:, j * CB:(j + 1) * CB] = r[B:]
        swap(4, s.pout, s.pin)
        swapped(4, s.pout, s.pin)
        s.res[...] = s.res[...] + s.pin[...]

    def unit(what, i, k, lhs, down_groups, down, between):
        def silu(g, u):
            return (g / (1.0 + jnp.exp(-g)) * u).astype(BF)

        early = (what, i) in (('ffn', 0), ('moe', 0), ('moe', 1))
        for group in ((0, 1, 2, 3, 4, 5),) if early else ((0, 1, 2), (3, 4, 5)):
            for j in group:
                w = 256 if j < 5 else 128
                u_gu(what, i, k, j, w, 0).wait()
                u_gu(what, i, k, j, w, 1).wait()
            if early:
                for j in range(4):
                    u_wd(what, i, k, j).wait()
            for j in group:
                w = 256 if j < 5 else 128
                r = dot(lhs[...], s.gu5[k, j] if j < 5 else s.gu1[k])
                s.act[:, j * 256:j * 256 + w] = silu(r[:, :w], r[:, w:])
        between()
        for group in down_groups:
            for j in group if not early else ():
                u_wd(what, i, k, j).wait()
            down(group, lambda j: dot(s.act[...], s.wd[k, j]))

    def gather_start(buf, ss, rs, at, on_y):
        with jax.named_scope('gather_start'):
            return gather_start_(buf, ss, rs, at, on_y)

    def gather_start_(buf, ss, rs, at, on_y):
        own = at(z, e)
        for k in ALONG:
            send(buf.at[own], buf.at[own], ss.at[k - 1], rs.at[own], lax.rem(z + k, TP), e)
        send(buf.at[own], buf.at[own], ss.at[3], rs.at[own], z, pe)
        if on_y:
            send(buf.at[own], buf.at[own], ss.at[8], rs.at[own], z, ye)

    def gather_pass(buf, ss, rs, at, on_y, before_last):
        with jax.named_scope('gather_pass'):
            return gather_pass_(buf, ss, rs, at, on_y, before_last)

    def gather_pass_(buf, ss, rs, at, on_y, before_last):
        for k in ALONG:
            if k == ALONG[-1]:
                before_last()
            g = at(lax.rem(z + k, TP), e)
            rc(buf.at[g], buf.at[g], ss.at[3 + k], rs.at[g], z, pe).wait_recv()
            send(buf.at[g], buf.at[g], ss.at[3 + k], rs.at[g], z, pe)
            if on_y:
                send(buf.at[g], buf.at[g], ss.at[8 + k], rs.at[g], z, ye)

    def gather_wait(buf, ss, rs, at):
        with jax.named_scope('gather_wait'):
            return gather_wait_(buf, ss, rs, at)

    def gather_wait_(buf, ss, rs, at):
        for zz in range(TP):
            g = at(zz, pe)
            rc(buf.at[g], buf.at[g], ss.at[0], rs.at[g], z, pe).wait_recv()

    def stack(buf, at):
        with jax.named_scope('stack'):
            return stack_(buf, at)

    def stack_(buf, at):
        for i, ee in enumerate((e, pe)):
            for q in range(2):
                s.fa[i * 32 + q * 16:i * 32 + q * 16 + 16, :] = jnp.concatenate([buf[at(2 * q, ee)], buf[at(2 * q + 1, ee)]], axis=0)

    def ffn(l, k, between):
        with jax.named_scope(f'ffn{l}'):
            return ffn_(l, k, between)

    def ffn_(l, k, between):
        def down(group, product):
            for j in group:
                r = product(j)
                s.pm[j] = r[:M // 2]
                s.ps[l, j] = r[M // 2:]
            for j in group:
                rc(s.ps.at[l, j], s.pr.at[l, j], s.pss.at[l, j], s.psr.at[l, j], z, pe).start()

        unit('ffn', l, k, s.fa, ((0, 1), (2, 3)), down, between)

    def ffn_send(l):
        with jax.named_scope(f'ffn_send{l}'):
            return ffn_send_(l)

    def ffn_send_(l):
        for j in range(4):
            rc(s.ps.at[l, j], s.pr.at[l, j], s.pss.at[l, j], s.psr.at[l, j], z, pe).wait()
            tot = s.pm[j] + s.pr[l, j]
            for q in range(TP):
                s.bs[l, q, j] = tot[q * B:(q + 1) * B].astype(BF)
            for k in ALONG:
                zz = lax.rem(z + k, TP)
                send(s.bs.at[l, zz, j], s.br.at[l, z, j], s.bss.at[l, k, j], s.bsr.at[l, z, j], zz, e)
            s.br[l, z, j] = s.bs[l, z, j]

    def ffn_recv(l):
        with jax.named_scope(f'ffn_recv{l}'):
            return ffn_recv_(l)

    def ffn_recv_(l):
        for j in range(4):
            for k in ALONG:
                zz = lax.rem(z + k, TP)
                rc(s.bs.at[l, zz, j], s.br.at[l, zz, j], s.bss.at[l, k, j], s.bsr.at[l, zz, j], zz, e).wait_recv()
            acc = s.br[l, 0, j].astype(F32)
            for q in range(1, TP):
                acc = acc + s.br[l, q, j].astype(F32)
            s.res[:, j * CB:(j + 1) * CB] = acc
        return s.res[...]

    def at16(zz, ee):
        return zz * 4 + ee

    def at8(zz, ee):
        return zz * 2 + lax.rem(ee, 2)

    def send_ids():
        with jax.named_scope('send_ids'):
            return send_ids_()

    def send_ids_():
        s.idall[me] = jnp.full((B, 128), -1, I32)
        s.idall[me, :, 0:6] = ids[...]
        pl.semaphore_wait(barrier, N - 1)
        for i, g, zz, ee in others:
            send(s.idall.at[me], s.idall.at[me], s.ids_s.at[i], s.ids_r.at[me], zz, ee)

    def slots_here():
        with jax.named_scope('slots_here'):
            return slots_here_()

    def slots_here_():
        lane = lax.broadcasted_iota(I32, (B, 128), 1)
        mine = s.idall[me]
        dst = [jnp.broadcast_to(mine[:, j:j + 1], (B, 128)) >> 2 for j in range(6)]
        hot = [jnp.where(d == lane, 1.0, 0.0) for d in dst]
        cnt = functools.reduce(jnp.add, hot)
        row = lax.broadcasted_iota(I32, (B, 128), 0)
        run = jnp.zeros((B, 128), F32)
        for t in range(B - 1):
            run = run + jnp.where(row > t, jnp.broadcast_to(cnt[t:t + 1], (B, 128)), 0.0)
        left, right = [], []
        for j in range(6):
            pos = jnp.sum(hot[j] * run, axis=1, keepdims=True)
            run = run + hot[j]
            col = dst[j].astype(F32) * B + pos
            left.append(jnp.where(col == lane.astype(F32), 1.0, 0.0))
            right.append(jnp.where(col + 4.0 == lane.astype(F32), 1.0, 0.0))
        s.gsel[...] = jnp.concatenate(left + right, axis=0).astype(BF)

    def slots_there():
        with jax.named_scope('slots_there'):
            return slots_there_()

    def slots_there_():
        for i, g, zz, ee in others:
            rc(s.idall.at[g], s.idall.at[g], s.ids_s.at[i], s.ids_r.at[g], z, pe).wait_recv()
        T = N * B
        idt = jnp.concatenate([s.idall[d] for d in range(N)], axis=0)
        lane = lax.broadcasted_iota(I32, (T, 128), 1)
        tok = lax.broadcasted_iota(I32, (T, 128), 0)
        col = [jnp.broadcast_to(idt[:, j:j + 1], (T, 128)) for j in range(6)]
        hit = [jnp.where((v >> 2) == me, 1.0, 0.0) for v in col]
        before = jnp.where((tok >> 3 == lane >> 3) & (lane < tok), 1.0, 0.0)
        run = dot(before.astype(BF), functools.reduce(jnp.add, hit).astype(BF)) + ((tok >> 3) * 4).astype(F32)
        pt = jnp.zeros((T, 128), F32)
        ex = jnp.zeros((T, 128), F32)
        for j in range(6):
            at = jnp.where(run == lane.astype(F32), hit[j], 0.0)
            pt = pt + at
            ex = ex + at * (col[j] & 3).astype(F32)
            run = run + hit[j]
        s.ptk[...] = pt[:, :M].astype(BF)
        s.el[...] = lax.dot_general(ex[:, :M].astype(BF), jnp.ones((T, 128), BF), (((0,), (0,)), ((), ())),
                                    preferred_element_type=F32)

    def expert(i, k, between):
        with jax.named_scope(f'expert{i}'):
            return expert_(i, k, between)

    def expert_(i, k, between):
        def down(group, product):
            for j in group:
                cols = pl.ds(j * CB, CB)
                r = product(j).astype(BF).astype(F32)
                if i == 0:
                    s.racc[:, cols] = r
                else:
                    keep = jnp.broadcast_to(s.el[:, 0:1], (M, CB)) == float(i)
                    s.racc[:, cols] = jnp.where(keep, r, s.racc[:, cols])

        unit('moe', i, k, s.ea, ((0, 1, 2, 3),), down, between)

    def give_back():
        with jax.named_scope('give_back'):
            return give_back_()

    def give_back_():
        for d in range(N):
            a = s.racc[4 * d:4 * d + 4, :]
            s.rs[d] = jnp.concatenate([a[:, :H // 2], a[:, H // 2:]], axis=0).astype(BF)
        for i, g, zz, ee in others:
            send(s.rs.at[g], s.rr.at[me], s.ret_s.at[i], s.ret_r.at[me], zz, ee)
        s.rr[me] = s.rs[me]

    def take_back():
        with jax.named_scope('take_back'):
            return take_back_()

    def take_back_():
        for i, g, zz, ee in others:
            rc(s.rs.at[g], s.rr.at[g], s.ret_s.at[i], s.ret_r.at[g], z, pe).wait_recv()
        for d in range(N // 2):
            s.rk[d * 16:(d + 1) * 16, :] = jnp.concatenate([s.rr[2 * d], s.rr[2 * d + 1]], axis=0)
        got = dot(s.gsel[...], s.rk[...])
        for half in range(2):
            acc = None
            for j in range(6):
                o = (half * 6 + j) * B
                term = wts[:, j:j + 1] * got[o:o + B]
                acc = term if acc is None else acc + term
            s.mm[:, half * (H // 2):(half + 1) * (H // 2)] = acc

    nothing = lambda: None

    s.an[...] = rms(x[...])

    def two0():
        m_o(0, 2).start()
        m_o(0, 3).start()
        positions()

    def q0():
        u_start('ffn', 0, 0)

    def kv0_done():
        u_start('moe', 0, 1)
        for j in range(3):
            h_q(j).start()
        c_uk(1).start()
        for t in range(B):
            c_kv(1, t).start()
        h_o(0).start()
        h_o(1).start()

    def uk0():
        send_ids()

    mla(0, two0, q0, uk0, kv0_done, lambda: c_uv(1).start())
    h_o(2).start()
    h_o(3).start()
    h0 = (x[...].astype(F32) + s.res[...]).astype(BF)
    s.h0[...] = h0
    s.uall[me] = rms(h0)
    gather_start(s.uall, s.us, s.ur, at16, True)
    slots_here()
    gather_pass(s.uall, s.us, s.ur, at16, True, slots_there)
    gather_wait(s.uall, s.us, s.ur, at16)
    stack(s.uall, at16)
    ffn(0, 0, lambda: u_start_gu('moe', 1, 0))
    u_start_wd('moe', 1, 0)
    for zz in range(TP):
        g = at16(zz, ye)
        rc(s.uall.at[g], s.uall.at[g], s.us.at[12 + zz], s.ur.at[g], z, pe).wait_recv()
        send(s.uall.at[g], s.uall.at[g], s.us.at[12 + zz], s.ur.at[g], z, pe)
    ffn_send(0)
    for zz in range(TP):
        g = at16(zz, ype)
        rc(s.uall.at[g], s.uall.at[g], s.us.at[12 + zz], s.ur.at[g], z, pe).wait_recv()
    for half in range(2):
        cols = pl.ds(half * (H // 2), H // 2)
        for d in range(N // 2):
            s.rk[d * 16:(d + 1) * 16, :] = jnp.concatenate([s.uall[2 * d, :, cols], s.uall[2 * d + 1, :, cols]], axis=0)
        s.ea[:, cols] = lax.dot_general(s.ptk[...], s.rk[...], (((0,), (0,)), ((), ())),
                                        preferred_element_type=F32).astype(BF)
    expert(0, 1, lambda: u_start_gu('moe', 2, 1))
    u_start_wd('moe', 2, 1)
    f0 = (s.h0[...].astype(F32) + ffn_recv(0)).astype(BF)
    s.f0[...] = f0
    s.an2[c] = rms(f0)
    half_q()
    attend(1)
    half_values_send()
    expert(1, 0, lambda: u_start_gu('moe', 3, 0))
    u_start_wd('moe', 3, 0)
    half_values()
    half_project()
    h1 = (s.f0[...].astype(F32) + s.res[...]).astype(BF)
    s.h1[...] = h1
    s.vall[at8(z, e)] = rms(h1)
    gather_start(s.vall, s.vs, s.vr, at8, False)
    expert(2, 1, lambda: u_start_gu('ffn', 1, 1))
    u_start_wd('ffn', 1, 1)
    expert(3, 0, lambda: gather_pass(s.vall, s.vs, s.vr, at8, False, nothing))
    give_back()
    gather_wait(s.vall, s.vs, s.vr, at8)
    stack(s.vall, at8)
    ffn(1, 1, nothing)
    ffn_send(1)
    take_back()
    y[...] = (s.h1[...].astype(F32) + ffn_recv(1) + s.mm[...]).astype(BF)
    for d in sends:
        d.wait_send()


def rope_table():
    half = ROPE // 2
    f = np.float32(10000.0) ** (np.float32(-2.0) * np.arange(half, dtype=np.float32) / np.float32(ROPE))
    ang = np.arange(1, L + 1, dtype=np.float32)[:, None] * f.astype(np.float32)
    cs, sn = np.cos(ang.astype(np.float64)), np.sin(ang.astype(np.float64))
    left = np.concatenate([cs, cs, -sn, sn], axis=1).astype(np.float32)
    parts = []
    for _ in range(3):
        part = left.astype(jnp.bfloat16)
        parts.append(part)
        left = left - part.astype(np.float32)
    return jnp.asarray(np.concatenate(parts, axis=1))


def layer(x, kv0, kv1, lens, ids, wts, wq, wuk, wuv, wo, w_in, w_out, e_in, e_out):
    table = rope_table()
    sc = scratch()
    vm = pl.BlockSpec(memory_space=pltpu.VMEM)
    hbm = pl.BlockSpec(memory_space=pl.ANY)
    return pl.pallas_call(
        functools.partial(kernel, tuple(sc)),
        out_shape=jax.ShapeDtypeStruct((B, H), BF),
        in_specs=[hbm] * 15,
        out_specs=vm,
        scratch_shapes=list(sc.values()),
        compiler_params=pltpu.CompilerParams(collective_id=0, has_side_effects=True, vmem_limit_bytes=67043328),
    )(x, lens, ids, wts, table, jnp.swapaxes(kv0, 1, 2), jnp.swapaxes(kv1, 1, 2), wq, wuk, wuv, wo, w_in, w_out, e_in, e_out)


def solution(mesh):
    in_specs = (P(BATCH, None), P(BATCH, None, None), P(BATCH, None, None), P(BATCH), P(BATCH, None), P(BATCH, None),
                P(), P(), P(), P(), P(None, None, None, 'tp'), P(None, 'tp', None), P(GROUP, None, None), P(GROUP, None, None))
    return jax.shard_map(layer, mesh=mesh, in_specs=in_specs, out_specs=P(BATCH, None), check_vma=False)
```

```python
import functools
import types

import jax
import jax.numpy as jnp
import numpy as np
from jax import lax
from jax.experimental import pallas as pl
from jax.experimental.pallas import tpu as pltpu
from jax.sharding import PartitionSpec as P

BATCH = ('dp', 'tp', 'ep')
GROUP = ('tp', 'ep')
MESH = pl.DeviceIdType.MESH
BF = jnp.bfloat16
F32 = jnp.float32
I32 = jnp.int32

B = 8
H = 2048
HEADS = 16
NOPE = 128
ROPE = 64
LAT = 512
VH = 128
L = 256
FH = 1408
TP = 4
N = 16
R = HEADS * B
M = 64
CB = 512
SCALE = (NOPE + ROPE) ** -0.5

ALONG = (1, 3, 2)


def scratch():
    dma = pltpu.SemaphoreType.DMA
    v = pltpu.VMEM
    return dict(
        x=v((B, H), BF), lens=v((B,), I32), ids=v((B, 6), I32), wts=v((B, 6), F32), table=v((L, 384), BF), s_in=dma((5,)),
        mbuf=v((8, H, CB), BF), wukb=v((HEADS, NOPE, LAT), BF), wuvb=v((HEADS, LAT, VH), BF), kvb=v((B, LAT + ROPE, L), BF),
        gu5=v((2, 5, H, CB), BF), gu1=v((2, H, CB // 2), BF), wd=v((2, 4, FH, CB), BF),
        qs=v((B, HEADS * (NOPE + ROPE)), F32), qc=v((R, LAT + ROPE), BF), sc=v((R, L), F32),
        ol=v((R, LAT), F32), os=v((B, HEADS * VH), BF), res=v((B, H), F32), an=v((B, H), BF),
        an2=v((2, B, H), BF), q2=v((2 * B, HEADS // 2 * (NOPE + ROPE)), F32), qown=v((2, R // 2, LAT), BF), qout=v((R // 2, LAT), BF),
        rown=v((2, R // 2, 128), F32), rout=v((R // 2, 128), F32), oout=v((R // 2, LAT), BF), oin=v((R // 2, LAT), BF),
        os2=v((2 * B, HEADS // 2 * VH), BF), pout=v((B, H), F32), pin=v((B, H), F32), xs=dma((5,)), xr=dma((5,)),
        h0=v((B, H), BF), f0=v((B, H), BF), h1=v((B, H), BF),
        cs=v((R, ROPE), F32), sn=v((R, ROPE), F32), lm=v((R, L), F32),
        uall=v((N, B, H), BF), vall=v((N // 2, B, H), BF), fa=v((M, H), BF), ea=v((M, H), BF), act=v((M, FH), BF),
        pm=v((4, M // 2, CB), F32), ps=v((2, 4, M // 2, CB), F32), pr=v((2, 4, M // 2, CB), F32),
        bs=v((2, TP, 4, B, CB), BF), br=v((2, TP, 4, B, CB), BF),
        idall=v((N, B, 128), I32), ptk=v((N * B, M), BF), el=v((M, 128), F32), gsel=v((2 * 6 * B, 128), BF),
        racc=v((M, H), F32), rs=v((N, B, H // 2), BF), rr=v((N, B, H // 2), BF), rk=v((N * B, H // 2), BF), mm=v((B, H), F32),
        s_m=dma((8,)), s_h=dma((4,)), s_kv=dma((B,)), s_uk=dma((2,)), s_gu=dma((2, 6, 2)), s_wd=dma((2, 4)),
        us=dma((16,)), ur=dma((N,)), vs=dma((8,)), vr=dma((N // 2,)),
        pss=dma((2, 4)), psr=dma((2, 4)), bss=dma((2, TP, 4)), bsr=dma((2, TP, 4)),
        ids_s=dma((N,)), ids_r=dma((N,)), ret_s=dma((N,)), ret_r=dma((N,)),
    )


def rms(v):
    vf = v.astype(F32)
    return (vf * lax.rsqrt(jnp.mean(vf * vf, axis=-1, keepdims=True) + 1e-6)).astype(BF)


def dot(a, b):
    return jnp.dot(a, b, preferred_element_type=F32)


def kernel(names, x_in, lens_in, ids_in, wts_in, table_in, kv0, kv1, wq, wuk, wuv, wo, w_in, w_out, e_in, e_out, y, *scr):
    s = types.SimpleNamespace(**dict(zip(names, scr)))
    z = lax.axis_index('tp')
    e = lax.axis_index('ep')
    me = z * 4 + e
    c = lax.rem(e, 2)
    pe = e + 1 - 2 * c
    ye = lax.rem(e + 2, 4)
    ype = lax.rem(pe + 2, 4)
    kvs = (kv0, kv1)
    x, lens, ids, wts, table = s.x, s.lens, s.ids, s.wts, s.table
    small = [pltpu.make_async_copy(a, b, s.s_in.at[i]) for i, (a, b) in enumerate(
        ((x_in, x), (lens_in, lens), (table_in, table), (ids_in, ids), (wts_in, wts)))]
    sends = []

    barrier = pltpu.get_barrier_semaphore()
    others = []
    for i in range(1, N):
        zz, ee = lax.rem(z + i // 4, 4), lax.rem(e + i % 4, 4)
        others.append((i, zz * 4 + ee, zz, ee))
    for i, g, zz, ee in others:
        pl.semaphore_signal(barrier, inc=1, device_id=(lax.axis_index('dp'), zz, ee), device_id_type=MESH)

    def cp(src, dst, sem):
        return pltpu.make_async_copy(src, dst, sem)

    def m_q(l, j):
        k = 2 * l + j
        return cp(wq.at[l, :, pl.ds(j * CB, CB)], s.mbuf.at[k], s.s_m.at[k])

    def m_o(l, j):
        k = (2 * l + 6 + j) % 8
        return cp(wo.at[l, :, pl.ds(j * CB, CB)], s.mbuf.at[k], s.s_m.at[k])

    def c_kv(l, t):
        return cp(kvs[l].at[t], s.kvb.at[t], s.s_kv.at[t])

    def c_uk(l):
        if l:
            return cp(wuk.at[1, pl.ds(c * 8, 8)], s.wukb.at[pl.ds(0, 8)], s.s_uk.at[0])
        return cp(wuk.at[0], s.wukb, s.s_uk.at[0])

    def c_uv(l):
        if l:
            return cp(wuv.at[1, pl.ds(c * 8, 8)], s.wuvb.at[pl.ds(0, 8)], s.s_uk.at[1])
        return cp(wuv.at[0], s.wuvb, s.s_uk.at[1])

    def h_q(j):
        cols = pl.ds(pl.multiple_of(c * 1536 + j * CB, CB), CB)
        return cp(wq.at[1, :, cols], s.mbuf.at[2 + j], s.s_m.at[2 + j])

    def h_o(j):
        rows = pl.ds(pl.multiple_of(c * 1024, 1024), 1024)
        return cp(wo.at[1, rows, pl.ds(j * CB, CB)], s.mbuf.at[5 + j // 2, pl.ds(j % 2 * 1024, 1024)], s.s_h.at[j])

    def u_gu(what, i, k, j, w, half):
        o = pl.multiple_of(j * 256, 128)
        if what == 'ffn':
            src = w_in.at[i, half, :, pl.ds(pl.multiple_of(c * FH + o, 128), w)]
        else:
            src = e_in.at[i, :, pl.ds(pl.multiple_of(half * FH + o, 128), w)]
        dst = s.gu5.at[k, j, :, pl.ds(half * w, w)] if w == 256 else s.gu1.at[k, :, pl.ds(half * w, w)]
        return cp(src, dst, s.s_gu.at[k, j, half])

    def u_wd(what, i, k, j):
        cols = pl.ds(pl.multiple_of(j * CB, CB), CB)
        if what == 'ffn':
            src = w_out.at[i, pl.ds(pl.multiple_of(c * FH, 128), FH), cols]
        else:
            src = e_out.at[i, :, cols]
        return cp(src, s.wd.at[k, j], s.s_wd.at[k, j])

    def u_start_gu(what, i, k):
        def gu(j, _):
            u_gu(what, i, k, j, 256, 0).start()
            u_gu(what, i, k, j, 256, 1).start()
            return 0

        lax.fori_loop(0, 5, gu, 0)
        u_gu(what, i, k, 5, 128, 0).start()
        u_gu(what, i, k, 5, 128, 1).start()

    def u_start_wd(what, i, k):
        def dn(j, _):
            u_wd(what, i, k, j).start()
            return 0

        lax.fori_loop(0, 4, dn, 0)

    def u_start(what, i, k):
        u_start_gu(what, i, k)
        u_start_wd(what, i, k)

    def rc(src, dst, ss, rs, tp, ep):
        return pltpu.make_async_remote_copy(src_ref=src, dst_ref=dst, send_sem=ss, recv_sem=rs,
                                            device_id=(lax.axis_index('dp'), tp, ep), device_id_type=MESH)

    def send(*a):
        d = rc(*a)
        d.start()
        sends.append(d)

    for d in small:
        d.start()
    m_q(0, 0).start()
    m_q(0, 1).start()
    for d in small:
        d.wait()
    for j in range(2, 6):
        m_q(0, j).start()
    for t in range(B):
        c_kv(0, t).start()
    c_uk(0).start()
    c_uv(0).start()
    m_o(0, 0).start()
    m_o(0, 1).start()

    def positions():
        diag = lax.broadcasted_iota(I32, (B, B), 0) == lax.broadcasted_iota(I32, (B, B), 1)
        lrow = jnp.broadcast_to(lens[...].astype(F32).reshape(1, B), (B, B))
        lv = jnp.broadcast_to(jnp.sum(jnp.where(diag, lrow, 0.0), axis=1, keepdims=True), (B, L))
        at = jnp.where(lax.broadcasted_iota(I32, (B, L), 1).astype(F32) == lv - 1.0, 1.0, 0.0).astype(BF)
        tb = dot(at, table[...])
        tb = tb[:, :128] + tb[:, 128:256] + tb[:, 256:]
        s.cs[...] = jnp.concatenate([tb[:, :ROPE]] * HEADS, axis=0)
        s.sn[...] = jnp.concatenate([tb[:, ROPE:]] * HEADS, axis=0)
        s.lm[...] = jnp.concatenate([lv] * HEADS, axis=0)

    rowt = lax.broadcasted_iota(I32, (R, L), 0) & (B - 1)

    def q_steps(l, lo, hi):
        for j in range(lo, hi):
            m_q(l, j).wait()
        for j in range(lo, hi):
            s.qs[:, j * CB:(j + 1) * CB] = dot(s.an[...], s.mbuf[2 * l + j])

    def mla(l, after_two, after_q, after_uk, after_kv, after_uv):
        q_steps(l, 0, 2)
        after_two()
        if l == 0:
            q_steps(l, 2, 4)
            q_steps(l, 4, 6)
        else:
            q_steps(l, 2, 6)
        after_q()
        latent_q(l)
        after_uk()
        attend(l)
        after_kv()
        values(l)
        after_uv()
        project(l)

    def latent_q(l):
        c_uk(l).wait()
        D = NOPE + ROPE
        rope = []
        for hp in range(HEADS // 2):
            pair = []
            for k in range(2):
                h = 2 * hp + k
                qn = s.qs[:, h * D:h * D + NOPE].astype(BF)
                pair.append(dot(qn, s.wukb[h]))
                rope.append(s.qs[:, h * D + NOPE:(h + 1) * D])
            s.qc[hp * 16:(hp + 1) * 16, :LAT] = jnp.concatenate(pair, axis=0).astype(BF)
        rotate(jnp.concatenate(rope, axis=0))

    def rotate(r):
        rot = jnp.concatenate([r[:, ROPE // 2:], r[:, :ROPE // 2]], axis=1)
        s.qc[:, LAT:] = (r * s.cs[...] + rot * s.sn[...]).astype(BF)

    def attend(l):
        for t in range(B):
            c_kv(l, t).wait()
        for t in range(B):
            st = dot(s.qc[...], s.kvb[t])
            if t == 0:
                s.sc[...] = st
            else:
                s.sc[...] = jnp.where(rowt == t, st, s.sc[...])
        sc = jnp.where(lax.broadcasted_iota(I32, (R, L), 1).astype(F32) < s.lm[...], s.sc[...] * SCALE, -1e30)
        ex = jnp.exp(sc - jnp.max(sc, axis=-1, keepdims=True))
        p = ex / jnp.sum(ex, axis=-1, keepdims=True)
        ol = None
        for t in range(B):
            pt = jnp.where(rowt == t, p, 0.0).astype(BF)
            ot = lax.dot_general(pt, s.kvb[t, :LAT, :], (((1,), (1,)), ((), ())), preferred_element_type=F32)
            ol = ot if ol is None else ol + ot
        s.ol[...] = ol

    def values(l):
        c_uv(l).wait()
        for h in range(HEADS):
            o = dot(s.ol[h * B:(h + 1) * B, :].astype(BF), s.wuvb[h])
            s.os[:, h * VH:(h + 1) * VH] = o.astype(BF)

    def project(l):
        for j in range(4):
            m_o(l, j).wait()
        for j in range(4):
            s.res[:, j * CB:(j + 1) * CB] = dot(s.os[...], s.mbuf[(2 * l + 6 + j) % 8])

    def swap(i, src, dst):
        send(src, dst, s.xs.at[i], s.xr.at[i], z, pe)

    def swapped(i, src, dst):
        rc(src, dst, s.xs.at[i], s.xr.at[i], z, pe).wait_recv()

    def half_q():
        swap(0, s.an2.at[c], s.an2.at[c])
        swapped(0, s.an2.at[1 - c], s.an2.at[1 - c])
        a = jnp.concatenate([s.an2[c], s.an2[1 - c]], axis=0)
        for j in range(3):
            h_q(j).wait()
        for j in range(3):
            s.q2[:, j * CB:(j + 1) * CB] = dot(a, s.mbuf[2 + j])
        c_uk(1).wait()
        D = NOPE + ROPE
        zero = jnp.zeros((B, 128 - ROPE), F32)
        for hp in range(HEADS // 4):
            pair = []
            for h in (2 * hp, 2 * hp + 1):
                pair.append(dot(s.q2[:, h * D:h * D + NOPE].astype(BF), s.wukb[h]))
                r = s.q2[:, h * D + NOPE:(h + 1) * D]
                s.rown[c, h * B:(h + 1) * B, :] = jnp.concatenate([r[:B], zero], axis=1)
                s.rout[h * B:(h + 1) * B, :] = jnp.concatenate([r[B:], zero], axis=1)
            s.qown[c, hp * 16:(hp + 1) * 16, :] = jnp.concatenate([pair[0][:B], pair[1][:B]], axis=0).astype(BF)
            s.qout[hp * 16:(hp + 1) * 16, :] = jnp.concatenate([pair[0][B:], pair[1][B:]], axis=0).astype(BF)
        swap(1, s.qout, s.qown.at[c])
        swap(2, s.rout, s.rown.at[c])
        swapped(1, s.qout, s.qown.at[1 - c])
        swapped(2, s.rout, s.rown.at[1 - c])
        for i in range(2):
            s.qc[i * 64:(i + 1) * 64, :LAT] = s.qown[i]
        rotate(jnp.concatenate([s.rown[0], s.rown[1]], axis=0)[:, :ROPE])

    def half_values_send():
        s.oout[...] = s.ol[pl.ds(pl.multiple_of((1 - c) * 64, 64), 64), :].astype(BF)
        swap(3, s.oout, s.oin)

    def half_values():
        own = s.ol[pl.ds(pl.multiple_of(c * 64, 64), 64), :]
        c_uv(1).wait()
        swapped(3, s.oout, s.oin)
        other = s.oin[...].astype(F32)
        for h in range(HEADS // 2):
            rows = slice(h * B, (h + 1) * B)
            o = dot(jnp.concatenate([own[rows], other[rows]], axis=0).astype(BF), s.wuvb[h])
            s.os2[:, h * VH:(h + 1) * VH] = o.astype(BF)

    def half_project():
        for j in range(4):
            h_o(j).wait()
        for j in range(4):
            r = dot(s.os2[...], s.mbuf[5 + j // 2, j % 2 * 1024:(j % 2 + 1) * 1024, :])
            s.res[:, j * CB:(j + 1) * CB] = r[:B]
            s.pout[:, j * CB:(j + 1) * CB] = r[B:]
        swap(4, s.pout, s.pin)
        swapped(4, s.pout, s.pin)
        s.res[...] = s.res[...] + s.pin[...]

    def unit(what, i, k, lhs, down_groups, down, between):
        def silu(g, u):
            return (g / (1.0 + jnp.exp(-g)) * u).astype(BF)

        early = (what, i) in (('ffn', 0), ('moe', 0), ('moe', 1))
        for group in ((0, 1, 2, 3, 4, 5),) if early else ((0, 1, 2), (3, 4, 5)):
            for j in group:
                w = 256 if j < 5 else 128
                u_gu(what, i, k, j, w, 0).wait()
                u_gu(what, i, k, j, w, 1).wait()
            if early:
                for j in range(4):
                    u_wd(what, i, k, j).wait()
            for j in group:
                w = 256 if j < 5 else 128
                r = dot(lhs[...], s.gu5[k, j] if j < 5 else s.gu1[k])
                s.act[:, j * 256:j * 256 + w] = silu(r[:, :w], r[:, w:])
        between()
        for group in down_groups:
            for j in group if not early else ():
                u_wd(what, i, k, j).wait()
            down(group, lambda j: dot(s.act[...], s.wd[k, j]))

    def gather_start(buf, ss, rs, at, on_y):
        own = at(z, e)
        for k in ALONG:
            send(buf.at[own], buf.at[own], ss.at[k - 1], rs.at[own], lax.rem(z + k, TP), e)
        send(buf.at[own], buf.at[own], ss.at[3], rs.at[own], z, pe)
        if on_y:
            send(buf.at[own], buf.at[own], ss.at[8], rs.at[own], z, ye)

    def gather_pass(buf, ss, rs, at, on_y, before_last):
        for k in ALONG:
            if k == ALONG[-1]:
                before_last()
            g = at(lax.rem(z + k, TP), e)
            rc(buf.at[g], buf.at[g], ss.at[3 + k], rs.at[g], z, pe).wait_recv()
            send(buf.at[g], buf.at[g], ss.at[3 + k], rs.at[g], z, pe)
            if on_y:
                send(buf.at[g], buf.at[g], ss.at[8 + k], rs.at[g], z, ye)

    def gather_wait(buf, ss, rs, at):
        for zz in range(TP):
            g = at(zz, pe)
            rc(buf.at[g], buf.at[g], ss.at[0], rs.at[g], z, pe).wait_recv()

    def stack(buf, at):
        for i, ee in enumerate((e, pe)):
            for q in range(2):
                s.fa[i * 32 + q * 16:i * 32 + q * 16 + 16, :] = jnp.concatenate([buf[at(2 * q, ee)], buf[at(2 * q + 1, ee)]], axis=0)

    def ffn(l, k, between):
        def down(group, product):
            for j in group:
                r = product(j)
                s.pm[j] = r[:M // 2]
                s.ps[l, j] = r[M // 2:]
            for j in group:
                rc(s.ps.at[l, j], s.pr.at[l, j], s.pss.at[l, j], s.psr.at[l, j], z, pe).start()

        unit('ffn', l, k, s.fa, ((0, 1), (2, 3)), down, between)

    def ffn_send(l):
        for j in range(4):
            rc(s.ps.at[l, j], s.pr.at[l, j], s.pss.at[l, j], s.psr.at[l, j], z, pe).wait()
            tot = s.pm[j] + s.pr[l, j]
            for q in range(TP):
                s.bs[l, q, j] = tot[q * B:(q + 1) * B].astype(BF)
            for k in ALONG:
                zz = lax.rem(z + k, TP)
                send(s.bs.at[l, zz, j], s.br.at[l, z, j], s.bss.at[l, k, j], s.bsr.at[l, z, j], zz, e)
            s.br[l, z, j] = s.bs[l, z, j]

    def ffn_recv(l):
        for j in range(4):
            for k in ALONG:
                zz = lax.rem(z + k, TP)
                rc(s.bs.at[l, zz, j], s.br.at[l, zz, j], s.bss.at[l, k, j], s.bsr.at[l, zz, j], zz, e).wait_recv()
            acc = s.br[l, 0, j].astype(F32)
            for q in range(1, TP):
                acc = acc + s.br[l, q, j].astype(F32)
            s.res[:, j * CB:(j + 1) * CB] = acc
        return s.res[...]

    def at16(zz, ee):
        return zz * 4 + ee

    def at8(zz, ee):
        return zz * 2 + lax.rem(ee, 2)

    def send_ids():
        s.idall[me] = jnp.full((B, 128), -1, I32)
        s.idall[me, :, 0:6] = ids[...]
        pl.semaphore_wait(barrier, N - 1)
        for i, g, zz, ee in others:
            send(s.idall.at[me], s.idall.at[me], s.ids_s.at[i], s.ids_r.at[me], zz, ee)

    def slots_here():
        lane = lax.broadcasted_iota(I32, (B, 128), 1)
        mine = s.idall[me]
        dst = [jnp.broadcast_to(mine[:, j:j + 1], (B, 128)) >> 2 for j in range(6)]
        hot = [jnp.where(d == lane, 1.0, 0.0) for d in dst]
        cnt = functools.reduce(jnp.add, hot)
        row = lax.broadcasted_iota(I32, (B, 128), 0)
        run = jnp.zeros((B, 128), F32)
        for t in range(B - 1):
            run = run + jnp.where(row > t, jnp.broadcast_to(cnt[t:t + 1], (B, 128)), 0.0)
        left, right = [], []
        for j in range(6):
            pos = jnp.sum(hot[j] * run, axis=1, keepdims=True)
            run = run + hot[j]
            col = dst[j].astype(F32) * B + pos
            left.append(jnp.where(col == lane.astype(F32), 1.0, 0.0))
            right.append(jnp.where(col + 4.0 == lane.astype(F32), 1.0, 0.0))
        s.gsel[...] = jnp.concatenate(left + right, axis=0).astype(BF)

    def slots_there():
        for i, g, zz, ee in others:
            rc(s.idall.at[g], s.idall.at[g], s.ids_s.at[i], s.ids_r.at[g], z, pe).wait_recv()
        T = N * B
        idt = jnp.concatenate([s.idall[d] for d in range(N)], axis=0)
        lane = lax.broadcasted_iota(I32, (T, 128), 1)
        tok = lax.broadcasted_iota(I32, (T, 128), 0)
        col = [jnp.broadcast_to(idt[:, j:j + 1], (T, 128)) for j in range(6)]
        hit = [jnp.where((v >> 2) == me, 1.0, 0.0) for v in col]
        before = jnp.where((tok >> 3 == lane >> 3) & (lane < tok), 1.0, 0.0)
        run = dot(before.astype(BF), functools.reduce(jnp.add, hit).astype(BF)) + ((tok >> 3) * 4).astype(F32)
        pt = jnp.zeros((T, 128), F32)
        ex = jnp.zeros((T, 128), F32)
        for j in range(6):
            at = jnp.where(run == lane.astype(F32), hit[j], 0.0)
            pt = pt + at
            ex = ex + at * (col[j] & 3).astype(F32)
            run = run + hit[j]
        s.ptk[...] = pt[:, :M].astype(BF)
        s.el[...] = lax.dot_general(ex[:, :M].astype(BF), jnp.ones((T, 128), BF), (((0,), (0,)), ((), ())),
                                    preferred_element_type=F32)

    def expert(i, k, between):
        def down(group, product):
            for j in group:
                cols = pl.ds(j * CB, CB)
                r = product(j).astype(BF).astype(F32)
                if i == 0:
                    s.racc[:, cols] = r
                else:
                    keep = jnp.broadcast_to(s.el[:, 0:1], (M, CB)) == float(i)
                    s.racc[:, cols] = jnp.where(keep, r, s.racc[:, cols])

        unit('moe', i, k, s.ea, ((0, 1, 2, 3),), down, between)

    def give_back():
        for d in range(N):
            a = s.racc[4 * d:4 * d + 4, :]
            s.rs[d] = jnp.concatenate([a[:, :H // 2], a[:, H // 2:]], axis=0).astype(BF)
        for i, g, zz, ee in others:
            send(s.rs.at[g], s.rr.at[me], s.ret_s.at[i], s.ret_r.at[me], zz, ee)
        s.rr[me] = s.rs[me]

    def take_back():
        for i, g, zz, ee in others:
            rc(s.rs.at[g], s.rr.at[g], s.ret_s.at[i], s.ret_r.at[g], z, pe).wait_recv()
        for d in range(N // 2):
            s.rk[d * 16:(d + 1) * 16, :] = jnp.concatenate([s.rr[2 * d], s.rr[2 * d + 1]], axis=0)
        got = dot(s.gsel[...], s.rk[...])
        for half in range(2):
            acc = None
            for j in range(6):
                o = (half * 6 + j) * B
                term = wts[:, j:j + 1] * got[o:o + B]
                acc = term if acc is None else acc + term
            s.mm[:, half * (H // 2):(half + 1) * (H // 2)] = acc

    nothing = lambda: None

    s.an[...] = rms(x[...])

    def two0():
        m_o(0, 2).start()
        m_o(0, 3).start()
        positions()

    def q0():
        u_start('ffn', 0, 0)

    def kv0_done():
        u_start('moe', 0, 1)
        for j in range(3):
            h_q(j).start()
        c_uk(1).start()
        for t in range(B):
            c_kv(1, t).start()
        h_o(0).start()
        h_o(1).start()

    def uk0():
        send_ids()

    mla(0, two0, q0, uk0, kv0_done, lambda: c_uv(1).start())
    h_o(2).start()
    h_o(3).start()
    h0 = (x[...].astype(F32) + s.res[...]).astype(BF)
    s.h0[...] = h0
    s.uall[me] = rms(h0)
    gather_start(s.uall, s.us, s.ur, at16, True)
    slots_here()
    gather_pass(s.uall, s.us, s.ur, at16, True, slots_there)
    gather_wait(s.uall, s.us, s.ur, at16)
    stack(s.uall, at16)
    ffn(0, 0, lambda: u_start_gu('moe', 1, 0))
    u_start_wd('moe', 1, 0)
    for zz in range(TP):
        g = at16(zz, ye)
        rc(s.uall.at[g], s.uall.at[g], s.us.at[12 + zz], s.ur.at[g], z, pe).wait_recv()
        send(s.uall.at[g], s.uall.at[g], s.us.at[12 + zz], s.ur.at[g], z, pe)
    ffn_send(0)
    for zz in range(TP):
        g = at16(zz, ype)
        rc(s.uall.at[g], s.uall.at[g], s.us.at[12 + zz], s.ur.at[g], z, pe).wait_recv()
    for half in range(2):
        cols = pl.ds(half * (H // 2), H // 2)
        for d in range(N // 2):
            s.rk[d * 16:(d + 1) * 16, :] = jnp.concatenate([s.uall[2 * d, :, cols], s.uall[2 * d + 1, :, cols]], axis=0)
        s.ea[:, cols] = lax.dot_general(s.ptk[...], s.rk[...], (((0,), (0,)), ((), ())),
                                        preferred_element_type=F32).astype(BF)
    expert(0, 1, lambda: u_start_gu('moe', 2, 1))
    u_start_wd('moe', 2, 1)
    f0 = (s.h0[...].astype(F32) + ffn_recv(0)).astype(BF)
    s.f0[...] = f0
    s.an2[c] = rms(f0)
    half_q()
    attend(1)
    half_values_send()
    expert(1, 0, lambda: u_start_gu('moe', 3, 0))
    u_start_wd('moe', 3, 0)
    half_values()
    half_project()
    h1 = (s.f0[...].astype(F32) + s.res[...]).astype(BF)
    s.h1[...] = h1
    s.vall[at8(z, e)] = rms(h1)
    gather_start(s.vall, s.vs, s.vr, at8, False)
    expert(2, 1, lambda: u_start_gu('ffn', 1, 1))
    u_start_wd('ffn', 1, 1)
    expert(3, 0, lambda: gather_pass(s.vall, s.vs, s.vr, at8, False, nothing))
    give_back()
    gather_wait(s.vall, s.vs, s.vr, at8)
    stack(s.vall, at8)
    ffn(1, 1, nothing)
    early = len(sends)
    ffn_send(1)
    for d in sends[:early]:
        d.wait_send()
    take_back()
    y[...] = (s.h1[...].astype(F32) + ffn_recv(1) + s.mm[...]).astype(BF)
    for d in sends[early:]:
        d.wait_send()


def rope_table():
    half = ROPE // 2
    f = np.float32(10000.0) ** (np.float32(-2.0) * np.arange(half, dtype=np.float32) / np.float32(ROPE))
    ang = np.arange(1, L + 1, dtype=np.float32)[:, None] * f.astype(np.float32)
    cs, sn = np.cos(ang.astype(np.float64)), np.sin(ang.astype(np.float64))
    left = np.concatenate([cs, cs, -sn, sn], axis=1).astype(np.float32)
    parts = []
    for _ in range(3):
        part = left.astype(jnp.bfloat16)
        parts.append(part)
        left = left - part.astype(np.float32)
    return jnp.asarray(np.concatenate(parts, axis=1))


def layer(x, kv0, kv1, lens, ids, wts, wq, wuk, wuv, wo, w_in, w_out, e_in, e_out):
    table = rope_table()
    sc = scratch()
    vm = pl.BlockSpec(memory_space=pltpu.VMEM)
    hbm = pl.BlockSpec(memory_space=pl.ANY)
    return pl.pallas_call(
        functools.partial(kernel, tuple(sc)),
        out_shape=jax.ShapeDtypeStruct((B, H), BF),
        in_specs=[hbm] * 15,
        out_specs=vm,
        scratch_shapes=list(sc.values()),
        compiler_params=pltpu.CompilerParams(collective_id=0, has_side_effects=True, vmem_limit_bytes=67043328),
    )(x, lens, ids, wts, table, jnp.swapaxes(kv0, 1, 2), jnp.swapaxes(kv1, 1, 2), wq, wuk, wuv, wo, w_in, w_out, e_in, e_out)


def solution(mesh):
    in_specs = (P(BATCH, None), P(BATCH, None, None), P(BATCH, None, None), P(BATCH), P(BATCH, None), P(BATCH, None),
                P(), P(), P(), P(), P(None, None, None, 'tp'), P(None, 'tp', None), P(GROUP, None, None), P(GROUP, None, None))
    return jax.shard_map(layer, mesh=mesh, in_specs=in_specs, out_specs=P(BATCH, None), check_vma=False)
```
